256 devices in a mesh: grp: 2 (over z), ma: 128 (over x, y, core).
Axes of the slice: x: 8, y: 8, z: 2, core: 2. Of those that a mesh axis runs over, the one named last changes fastest.
The devices are a block of a 8x8x16 slice.
Arguments:
- tbar_alm: bfloat16 [1024, 8, 2, 2049], P('ma', 'grp'), parts along dimension 1, may hold values from -6 to 6
- twf_alm: bfloat16 [1024, 8, 2, 2049], P('ma', 'grp'), parts along dimension 1, may hold values from -6 to 6
- legendre: bfloat16 [1024, 2049, 128], P('ma'), may hold values from -0.125 to 0.125
- m_slots: int32 [1024], replicated, may hold values from 0 to 1023, each once
- cycle_order: int32 [128], replicated, may hold values from 0 to 127, each once
- colatitude: float32 [128], replicated, may hold values from 0.35 to 2.79
- cycle_weight: float32 [128], replicated, may hold values from 0.25 to 1
- pixel_mask: int32 [128, 4096], P('ma'), may hold values from 0 to 3
Outputs:
- gradient: float32 [1024, 8, 2, 2049], P('ma', 'grp'), parts along dimension 1
- curl: float32 [1024, 8, 2, 2049], P('ma', 'grp'), parts along dimension 1
The draws below stay inside these ranges and needn't reach their ends.
There are 2 independent parts, one for each index of `grp`. The reference program is written for one: setup_inputs(seed, part) draws one part's arguments, and reference() takes and returns one part's arrays. A program takes and returns all parts, laid end to end along the dimension named above; an argument that names none is the same for every part. Nothing has to cross between parts.
Inputs may be any that keep to these rules, and one draw needn't show every extreme that they name: Pair p holds the orders m_slots[p] and 2047 - m_slots[p]; each value appears once. Cycle slot i holds cycle cycle_order[i]; each value appears once.
All inputs are finite; a program needn't handle non-finite values.
Results may differ from the reference program's by a relative error of at most 0.017.
Values may be sent and summed in bfloat16 or wider, within the bound.
No kernel may reach another device: no remote copies, remote signals or barrier semaphores. Data moves between devices by JAX's collectives and lax.ppermute only.
A program may use at most 128 MiB of HBM per device.

```python
import math
import jax
import jax.numpy as jnp
from jax import lax

MODES = 2048
PAIRS = 1024
ROWS = 2049
CYCLES = 128
NPHI = 4096
SIMS = 4


def touch_ends(drawn, stream_key, smallest, high):
    extent = drawn.shape
    spot = [jax.random.randint(jax.random.fold_in(stream_key, axis), (), 0, extent[axis]) for axis in range(len(extent))]
    drawn = drawn.at[tuple(spot)].set(smallest)
    longest = extent.index(max(extent))
    spot[longest] = (spot[longest] + 1) % extent[longest]
    return drawn.at[tuple(spot)].set(high)


def levels(stream_key, extent, split, low, largest):
    level, own = 1.0, jax.random.fold_in(stream_key, 6)
    for position, parts in split:
        steps = jnp.exp(jax.random.uniform(jax.random.fold_in(own, position), (parts,), jnp.float32, low / len(split), largest / len(split)))
        level = level * jnp.repeat(steps, extent[position] // parts).reshape([-1 if axis == position else 1 for axis in range(len(extent))])
    return level


def scatter_about(stream_key, extent, deviation, reach, split=(), dtype=jnp.bfloat16):
    drawn = deviation * jax.random.normal(stream_key, extent, jnp.float32)
    if split:
        drawn = drawn * levels(stream_key, extent, split, -0.22, 0.18)
    return jnp.clip(drawn, -reach, reach).astype(dtype)


def setup_inputs(seed: int = 0, part: int = 0) -> dict:
    seeds = jax.random.split(jax.random.key(seed), 9)
    part_splits = jax.random.split(jax.random.fold_in(seeds[8], part), 9)
    tbar_alm = scatter_about(part_splits[0], (PAIRS, SIMS, 2, ROWS), 1.0, 6.0, ((0, 128),))
    twf_alm = scatter_about(part_splits[1], (PAIRS, SIMS, 2, ROWS), 1.0, 6.0, ((0, 128),))
    legendre = scatter_about(seeds[2], (PAIRS, ROWS, CYCLES), ROWS ** -0.5, 0.125, ((0, 128),))
    m_slots = jax.random.permutation(seeds[3], PAIRS).astype(jnp.int32)
    cycle_order = jax.random.permutation(seeds[4], CYCLES).astype(jnp.int32)
    colatitude = jnp.clip(jax.random.uniform(seeds[5], (CYCLES,), jnp.float32, 0.35, 2.79), 0.35, 2.79)
    cycle_weight = jnp.clip(jnp.exp(jax.random.uniform(seeds[6], (CYCLES,), jnp.float32, math.log(0.25), math.log(1.0))), 0.25, 1.0)
    pixel_mask = touch_ends(jax.random.randint(seeds[7], (CYCLES, NPHI), 0, 4), jax.random.fold_in(seeds[7], 1), 0, 3).astype(jnp.int32)
    return {"tbar_alm": tbar_alm, "twf_alm": twf_alm, "legendre": legendre, "m_slots": m_slots, "cycle_order": cycle_order, "colatitude": colatitude, "cycle_weight": cycle_weight, "pixel_mask": pixel_mask}


def rounded(values):
    return lax.optimization_barrier(values.astype(jnp.bfloat16)).astype(jnp.float32)

def pair_layout(small_orders, mode_count):
    row_index = lax.broadcasted_iota(jnp.int32, (small_orders.shape[0], mode_count + 1), 1)
    smaller = small_orders[:, None]
    upper_half = row_index >= mode_count - smaller
    degree = jnp.where(upper_half, row_index - 1, smaller + row_index)
    orders = jnp.where(upper_half, mode_count - 1 - smaller, smaller + 0 * row_index)
    return (upper_half, degree.astype(jnp.float32), orders.astype(jnp.float32))

def raising(degree, orders):
    square = (degree * degree - orders * orders) * (2.0 * degree + 1.0) / jnp.maximum(2.0 * degree - 1.0, 1.0)
    return jnp.where(degree > orders, jnp.sqrt(jnp.where(degree > orders, square, 0.0)), 0.0)

def synthesis_sets(tbar_alm, twf_alm, degree, raising_factor, mode_count):
    wiener = twf_alm.astype(jnp.float32)
    scaled = (raising_factor / mode_count)[:, None, None, :] * wiener
    raised = jnp.concatenate([scaled[..., 1:], jnp.zeros_like(scaled[..., :1])], axis=-1)
    stacked = jnp.stack([tbar_alm.astype(jnp.float32), wiener, (degree / mode_count)[:, None, None, :] * wiener, raised], axis=2)
    return stacked.reshape(stacked.shape[0], stacked.shape[1], 8, stacked.shape[4]).astype(jnp.bfloat16)

def mode_columns(small_orders, mode_count):
    return jnp.stack([small_orders, mode_count - 1 - small_orders], axis=1).reshape(-1)

def fourier_table(orders_int, pixel_count):
    pixel_index = lax.broadcasted_iota(jnp.int32, (orders_int.shape[0], pixel_count), 1)
    turns = orders_int[:, None] * pixel_index % pixel_count
    radians = turns.astype(jnp.float32) * (2.0 * math.pi / pixel_count)
    return jnp.stack([jnp.cos(radians), -jnp.sin(radians)], axis=0).astype(jnp.bfloat16)

def combine_modes(legendre_sums, orders_int, cos_cycle, sin_cycle, mode_count):
    orders_real = orders_int.astype(jnp.float32)
    inv_sin = 1.0 / sin_cycle
    ratio = (orders_real / mode_count)[:, None]
    theta_real = (cos_cycle * legendre_sums[:, 4] - legendre_sums[:, 6]) * inv_sin
    theta_imag = (cos_cycle * legendre_sums[:, 5] - legendre_sums[:, 7]) * inv_sin
    phi_real = -ratio * legendre_sums[:, 3] * inv_sin
    phi_imag = ratio * legendre_sums[:, 2] * inv_sin
    weight = (jnp.where(orders_int == 0, 1.0, 2.0) * mode_count ** (-0.5))[:, None]
    stacked = jnp.stack([legendre_sums[:, 0], legendre_sums[:, 1], theta_real, theta_imag, phi_real, phi_imag], axis=1)
    return (stacked * weight).astype(jnp.bfloat16)

def analysis_sets(spectra, colatitude, cycle_weight):
    with_cos = cycle_weight * jnp.cos(colatitude) / jnp.sin(colatitude)
    with_sin = cycle_weight / jnp.sin(colatitude)
    stacked = jnp.stack([spectra[:, 0] * with_cos, spectra[:, 0] * with_sin, spectra[:, 1] * with_cos, spectra[:, 1] * with_sin], axis=1)
    return stacked.reshape(spectra.shape[0], 8, spectra.shape[3], spectra.shape[4]).astype(jnp.bfloat16)

def estimate(merged, degree, orders, raising_factor, mode_count, cycle_count):
    level = degree[:, None, :]
    azimuth = orders[:, None, :]
    factor = raising_factor[:, None, :]

    def previous(values):
        return jnp.concatenate([jnp.zeros_like(values[..., :1]), values[..., :-1]], axis=-1)
    grad_real = level * merged[:, :, 0] - factor * previous(merged[:, :, 2]) + azimuth * merged[:, :, 7]
    grad_imag = level * merged[:, :, 1] - factor * previous(merged[:, :, 3]) - azimuth * merged[:, :, 6]
    curl_real = level * merged[:, :, 4] - factor * previous(merged[:, :, 6]) - azimuth * merged[:, :, 3]
    curl_imag = level * merged[:, :, 5] - factor * previous(merged[:, :, 7]) + azimuth * merged[:, :, 2]
    scale = (mode_count / cycle_count) ** 0.5 / jnp.sqrt(jnp.maximum(level * (level + 1.0), 1.0))
    scale = scale[:, :, None, :]
    return (jnp.stack([grad_real, grad_imag], axis=2) * scale, jnp.stack([curl_real, curl_imag], axis=2) * scale)

def reference(tbar_alm, twf_alm, legendre, m_slots, cycle_order, colatitude, cycle_weight, pixel_mask):
    upper_half, degree, orders = pair_layout(m_slots, MODES)
    raising_factor = raising(degree, orders)
    coeff_sets = rounded(synthesis_sets(tbar_alm, twf_alm, degree, raising_factor, MODES))
    halves = jnp.stack([jnp.logical_not(upper_half), upper_half], axis=1).astype(jnp.float32)
    blocks = PAIRS // 8

    def synth_block(block_items):
        block_sets, block_halves, block_table = block_items
        masked = block_sets[:, None] * block_halves[:, :, None, None, :]
        return jnp.einsum('phsck,pkr->scphr', masked, block_table.astype(jnp.float32))
    legendre_sums = lax.map(synth_block, (coeff_sets.reshape(blocks, 8, SIMS, 8, ROWS), halves.reshape(blocks, 8, 2, ROWS), legendre.reshape(blocks, 8, ROWS, CYCLES)))
    legendre_sums = jnp.transpose(legendre_sums, (1, 2, 0, 3, 4, 5)).reshape(SIMS, 8, MODES, CYCLES)
    legendre_sums = jnp.take(legendre_sums, cycle_order, axis=3)
    slot_theta = jnp.take(colatitude, cycle_order)
    orders_all = mode_columns(m_slots, MODES)
    fourier = combine_modes(legendre_sums, orders_all, jnp.cos(slot_theta), jnp.sin(slot_theta), MODES)
    fourier = rounded(fourier).reshape(SIMS, 3, 2, MODES, CYCLES)
    dft_table = rounded(fourier_table(orders_all, NPHI))
    cycle_maps = jnp.einsum('sqemr,emj->sqrj', fourier, dft_table)
    products = rounded(pixel_mask.astype(jnp.float32) * cycle_maps[:, 0:1] * cycle_maps[:, 1:3])
    spectra = rounded(jnp.einsum('sqrj,emj->sqemr', products, dft_table) * NPHI ** (-0.5))
    inverse = jnp.zeros((CYCLES,), jnp.int32).at[cycle_order].set(lax.iota(jnp.int32, CYCLES))
    spectra = jnp.take(spectra, inverse, axis=4)
    weighted = rounded(analysis_sets(spectra, colatitude, cycle_weight))
    weighted = jnp.moveaxis(weighted.reshape(SIMS, 8, blocks, 8, 2, CYCLES), 2, 0)

    def analysis_block(block_items):
        block_weighted, block_table, block_halves, block_degree, block_orders, block_raising = block_items
        projected = jnp.einsum('scphr,pkr->phsck', block_weighted, block_table.astype(jnp.float32))
        merged = lax.optimization_barrier(jnp.sum(projected * block_halves[:, :, None, None, :], axis=1))
        return estimate(merged, block_degree, block_orders, block_raising, MODES, CYCLES)
    gradient, curl = lax.map(analysis_block, (weighted, legendre.reshape(blocks, 8, ROWS, CYCLES), halves.reshape(blocks, 8, 2, ROWS), degree.reshape(blocks, 8, ROWS), orders.reshape(blocks, 8, ROWS), raising_factor.reshape(blocks, 8, ROWS)))
    return (gradient.reshape(PAIRS, SIMS, 2, ROWS), curl.reshape(PAIRS, SIMS, 2, ROWS))
```

```python
import math

import jax
import jax.numpy as jnp
from jax import lax
from jax.sharding import Mesh
from jax.sharding import PartitionSpec as P

MA = ("ma_0", "ma_1", "ma_2")


def pair_layout(small_orders, mode_count):
    row_index = lax.broadcasted_iota(jnp.int32, (small_orders.shape[0], mode_count + 1), 1)
    smaller = small_orders[:, None]
    upper_half = row_index >= mode_count - smaller
    degree = jnp.where(upper_half, row_index - 1, smaller + row_index)
    orders = jnp.where(upper_half, mode_count - 1 - smaller, smaller + 0 * row_index)
    return (upper_half, degree.astype(jnp.float32), orders.astype(jnp.float32))


def raising(degree, orders):
    square = (
        (degree * degree - orders * orders)
        * (2.0 * degree + 1.0)
        / jnp.maximum(2.0 * degree - 1.0, 1.0)
    )
    return jnp.where(degree > orders, jnp.sqrt(jnp.where(degree > orders, square, 0.0)), 0.0)


def synthesis_sets(tbar_alm, twf_alm, degree, raising_factor, mode_count):
    wiener = twf_alm.astype(jnp.float32)
    scaled = (raising_factor / mode_count)[:, None, None, :] * wiener
    raised = jnp.concatenate([scaled[..., 1:], jnp.zeros_like(scaled[..., :1])], axis=-1)
    stacked = jnp.stack(
        [
            tbar_alm.astype(jnp.float32),
            wiener,
            (degree / mode_count)[:, None, None, :] * wiener,
            raised,
        ],
        axis=2,
    )
    return stacked.reshape(stacked.shape[0], stacked.shape[1], 8, stacked.shape[4]).astype(
        jnp.bfloat16
    )


def mode_columns(small_orders, mode_count):
    return jnp.stack([small_orders, mode_count - 1 - small_orders], axis=1).reshape(-1)


def phases(rows, columns, period):
    turns = lax.broadcasted_iota(jnp.int32, (rows, columns), 0) * lax.broadcasted_iota(
        jnp.int32, (rows, columns), 1
    )
    radians = (turns % period).astype(jnp.float32) * (2.0 * math.pi / period)
    return jnp.cos(radians), jnp.sin(radians)


def bf(x):
    return x.astype(jnp.bfloat16)


def dot(spec, a, b):
    return jnp.einsum(spec, bf(a), bf(b), preferred_element_type=jnp.float32)


def to_pixels(values, pixel_count):
    s, q, _, mode_count = values.shape
    v = values.reshape(s, q, 2, mode_count // 64, 64)
    c, d = phases(mode_count // 64, 64, 64)
    re = dot("sqak,aj->sqkj", v[:, :, 0], c) - dot("sqak,aj->sqkj", v[:, :, 1], d)
    im = dot("sqak,aj->sqkj", v[:, :, 0], d) + dot("sqak,aj->sqkj", v[:, :, 1], c)
    tc, td = phases(64, 64, pixel_count)
    hr = re * tc - im * td
    hi = re * td + im * tc
    c, d = phases(64, pixel_count // 64, 64)
    return dot("sqkj,kl->sqjl", hr, c) - dot("sqkj,kl->sqjl", hi, d)


def to_modes(values, mode_count):
    s, q, j2, j1 = values.shape
    c, d = phases(64, j1, 64)
    re = dot("sqjl,kl->sqjk", values, c)
    im = -dot("sqjl,kl->sqjk", values, d)
    tc, td = phases(64, 64, j1 * j2)
    rr = re * tc + im * td
    ri = im * tc - re * td
    c, d = phases(mode_count // 64, 64, 64)
    zr = dot("sqjk,aj->sqak", rr, c) + dot("sqjk,aj->sqak", ri, d)
    zi = dot("sqjk,aj->sqak", ri, c) - dot("sqjk,aj->sqak", rr, d)
    return jnp.stack([zr, zi], axis=2).reshape(s, q, 2, mode_count)


def combine_modes(legendre_sums, orders_int, cos_cycle, sin_cycle, mode_count):
    orders_real = orders_int.astype(jnp.float32)
    inv_sin = 1.0 / sin_cycle
    ratio = (orders_real / mode_count)[:, None]
    theta_real = (cos_cycle * legendre_sums[:, 4] - legendre_sums[:, 6]) * inv_sin
    theta_imag = (cos_cycle * legendre_sums[:, 5] - legendre_sums[:, 7]) * inv_sin
    phi_real = -ratio * legendre_sums[:, 3] * inv_sin
    phi_imag = ratio * legendre_sums[:, 2] * inv_sin
    weight = (jnp.where(orders_int == 0, 1.0, 2.0) * mode_count ** (-0.5))[:, None]
    stacked = jnp.stack(
        [legendre_sums[:, 0], legendre_sums[:, 1], theta_real, theta_imag, phi_real, phi_imag],
        axis=1,
    )
    return (stacked * weight).astype(jnp.bfloat16)


def analysis_sets(spectra, colatitude, cycle_weight):
    with_cos = cycle_weight * jnp.cos(colatitude) / jnp.sin(colatitude)
    with_sin = cycle_weight / jnp.sin(colatitude)
    stacked = jnp.stack(
        [
            spectra[:, 0] * with_cos,
            spectra[:, 0] * with_sin,
            spectra[:, 1] * with_cos,
            spectra[:, 1] * with_sin,
        ],
        axis=1,
    )
    return stacked.reshape(spectra.shape[0], 8, spectra.shape[3], spectra.shape[4]).astype(
        jnp.bfloat16
    )


def estimate(merged, degree, orders, raising_factor, mode_count, cycle_count):
    level = degree[:, None, :]
    azimuth = orders[:, None, :]
    factor = raising_factor[:, None, :]

    def previous(values):
        return jnp.concatenate([jnp.zeros_like(values[..., :1]), values[..., :-1]], axis=-1)

    grad_real = (
        level * merged[:, :, 0] - factor * previous(merged[:, :, 2]) + azimuth * merged[:, :, 7]
    )
    grad_imag = (
        level * merged[:, :, 1] - factor * previous(merged[:, :, 3]) - azimuth * merged[:, :, 6]
    )
    curl_real = (
        level * merged[:, :, 4] - factor * previous(merged[:, :, 6]) - azimuth * merged[:, :, 3]
    )
    curl_imag = (
        level * merged[:, :, 5] - factor * previous(merged[:, :, 7]) + azimuth * merged[:, :, 2]
    )
    scale = (mode_count / cycle_count) ** 0.5 / jnp.sqrt(jnp.maximum(level * (level + 1.0), 1.0))
    scale = scale[:, :, None, :]
    return (
        jnp.stack([grad_real, grad_imag], axis=2) * scale,
        jnp.stack([curl_real, curl_imag], axis=2) * scale,
    )


def shards(tbar_alm, twf_alm, legendre, m_slots, cycle_order, colatitude, cycle_weight, pixel_mask):
    pairs_dev = tbar_alm.shape[0]
    row_count = tbar_alm.shape[3]
    mode_count = row_count - 1
    cycle_count = legendre.shape[2]
    cycle_dev = pixel_mask.shape[0]
    pixel_count = pixel_mask.shape[1]
    device_slot = lax.axis_index(MA)
    local_small = lax.dynamic_slice_in_dim(m_slots, device_slot * pairs_dev, pairs_dev)
    upper_half, degree, orders = pair_layout(local_small, mode_count)
    raising_factor = raising(degree, orders)
    coeff_sets = synthesis_sets(tbar_alm, twf_alm, degree, raising_factor, mode_count)
    halves = jnp.stack([jnp.logical_not(upper_half), upper_half], axis=1)
    masked = coeff_sets[:, None] * halves.astype(jnp.bfloat16)[:, :, None, None, :]
    legendre_sums = jnp.einsum(
        "phsck,pkr->scphr", masked, legendre, preferred_element_type=jnp.float32
    )
    legendre_sums = jnp.take(legendre_sums, cycle_order, axis=4)
    legendre_sums = legendre_sums.reshape(legendre_sums.shape[0], 8, 2 * pairs_dev, cycle_count)
    all_orders = mode_columns(m_slots, mode_count)
    pixel_weights = pixel_mask.astype(jnp.float32).reshape(pixel_count // 64, 64).T
    slot_theta = jnp.take(colatitude, cycle_order)
    local_orders = mode_columns(local_small, mode_count)
    outgoing = combine_modes(
        legendre_sums, local_orders, jnp.cos(slot_theta), jnp.sin(slot_theta), mode_count
    )
    fourier = lax.all_to_all(outgoing, MA, split_axis=3, concat_axis=2, tiled=True)
    fourier = fourier.reshape(fourier.shape[0], 3, 2, mode_count)
    place = (
        jnp.zeros((mode_count,), jnp.int32).at[all_orders].set(lax.iota(jnp.int32, mode_count))
    )
    cycle_maps = to_pixels(jnp.take(fourier, place, axis=3), pixel_count)
    products = (pixel_weights * cycle_maps[:, 0:1] * cycle_maps[:, 1:3]).astype(jnp.bfloat16)
    spectra = to_modes(products, mode_count)
    received = (spectra * pixel_count ** (-0.5)).astype(jnp.bfloat16)
    received = jnp.take(received, all_orders, axis=3)[..., None]
    returned = lax.all_to_all(received, MA, split_axis=3, concat_axis=4, tiled=True)
    inverse = (
        jnp.zeros((cycle_count,), jnp.int32).at[cycle_order].set(lax.iota(jnp.int32, cycle_count))
    )
    spectra = jnp.take(returned, inverse, axis=4).astype(jnp.float32)
    weighted = analysis_sets(spectra, colatitude, cycle_weight)
    weighted = weighted.reshape(weighted.shape[0], 8, pairs_dev, 2, cycle_count)
    projected = jnp.einsum(
        "scphr,pkr->phsck", weighted, legendre, preferred_element_type=jnp.float32
    )
    merged = jnp.sum(projected * halves.astype(jnp.float32)[:, :, None, None, :], axis=1)
    return estimate(merged, degree, orders, raising_factor, mode_count, cycle_count)


def solution(mesh):
    finer = Mesh(mesh.devices.reshape(mesh.shape["grp"], 8, 8, 2), ("grp", "ma_0", "ma_1", "ma_2"))
    in_specs = (
        P(MA, "grp", None, None),
        P(MA, "grp", None, None),
        P(MA, None, None),
        P(),
        P(),
        P(),
        P(),
        P(MA, None),
    )
    out_specs = (P(MA, "grp", None, None), P(MA, "grp", None, None))
    return jax.shard_map(
        shards, mesh=finer, in_specs=in_specs, out_specs=out_specs, check_vma=False
    )
```

```python
import functools
import math

import jax
import jax.numpy as jnp
import numpy as np
from jax import lax
from jax.experimental import pallas as pl
from jax.experimental.pallas import tpu as pltpu
from jax.sharding import PartitionSpec as P

F32 = jnp.float32
BF16 = jnp.bfloat16
FOLD = 64
NT = (((1,), (1,)), ((), ()))
NN = (((1,), (0,)), ((), ()))


def dot(a, b, dims=NN):
    return lax.dot_general(a, b, dims, preferred_element_type=F32)


def iota(shape, dim):
    return lax.broadcasted_iota(jnp.int32, shape, dim)


def small_column(m_ref, first, pairs):
    row = iota((pairs, 1), 0)
    column = jnp.zeros((pairs, 1), jnp.int32)
    for p in range(pairs):
        column = jnp.where(row == p, m_ref[first + p], column)
    return column


def layout_rows(small, modes):
    k = iota((small.shape[0], modes), 1)
    upper = k >= modes - small
    degree = jnp.where(upper, k - 1, small + k).astype(F32)
    orders = jnp.where(upper, modes - 1 - small, small).astype(F32)
    last_degree = jnp.full(small.shape, modes - 1, F32)
    last_orders = (modes - 1 - small).astype(F32)
    return (
        (degree, orders, raising(degree, orders)),
        (last_degree, last_orders, raising(last_degree, last_orders)),
    )


def raising(degree, orders):
    square = (
        (degree * degree - orders * orders)
        * (2.0 * degree + 1.0)
        / jnp.maximum(2.0 * degree - 1.0, 1.0)
    )
    return jnp.where(degree > orders, jnp.sqrt(jnp.where(degree > orders, square, 0.0)), 0.0)


def slot_of_cycle(order_ref):
    n = order_ref.shape[1]
    return jnp.where(iota((n, n), 0) == order_ref[...], 1.0, 0.0)


def turn(values):
    rows = values.shape[0]
    real = iota(values.shape, 0) % 2 == 0
    return jnp.where(real, -pltpu.roll(values, rows - 1, 0), pltpu.roll(values, 1, 0))


def rows_of(ref, p):
    return jnp.concatenate([ref[p, s].astype(F32) for s in range(ref.shape[1])], axis=0)


def synth_kernel(
    axis, m_ref, order_ref, colat_ref, t_ref, w_ref, l_ref, tail_ref, out_ref, lr_ref, ltail_ref,
    c_ref, s_ref, f_ref, deg_ref, eps_ref,
):
    step = pl.program_id(0)
    pairs, sims = t_ref.shape[0], t_ref.shape[1]
    modes = t_ref.shape[3] - 1
    lines = 2 * sims
    chunk = l_ref.shape[0]
    first = lax.axis_index(axis) * pairs
    wide = out_ref.shape[1] // pairs

    @pl.when(step == 0)
    def _():
        small = small_column(m_ref, first, pairs)
        (degree, _, eps), (_, _, last_eps) = layout_rows(small, modes)
        deg_ref[...] = degree * (1.0 / modes)
        eps_ref[...] = eps * (1.0 / modes)
        k = iota((lines, modes), 1)
        tail_rows = tail_ref[0].astype(F32)
        for p in range(pairs):
            tbar, wiener = rows_of(t_ref, p), rows_of(w_ref, p)
            main, last = wiener[:, :modes], wiener[:, modes:]
            scaled = eps_ref[p : p + 1, :] * main
            raised = pltpu.roll(scaled, modes - 1, 1)
            last_scaled = (last_eps[p : p + 1, :] * (1.0 / modes)) * last
            raised = jnp.where(k == modes - 1, last_scaled, raised)
            sets = (tbar[:, :modes], main, deg_ref[p : p + 1, :] * main, raised)
            upper = k >= modes - m_ref[first + p]
            for q, values in enumerate(sets):
                c_ref[p, q * lines : (q + 1) * lines, :] = jnp.where(upper, 0.0, values).astype(BF16)
                c_ref[p, (4 + q) * lines : (5 + q) * lines, :] = jnp.where(upper, values, 0.0).astype(BF16)
            lasts = (tbar[:, modes:], last, ((modes - 1.0) / modes) * last)
            s_ref[p] = jnp.zeros(s_ref.shape[1:], F32)
            for q, values in enumerate(lasts):
                s_ref[p, (4 + q) * lines : (5 + q) * lines, :] = (
                    values.astype(BF16).astype(F32) * tail_rows[p : p + 1, :]
                )
        ltail_ref[...] = tail_rows

    f_ref[...] = l_ref[...].astype(F32).reshape(chunk * pairs, l_ref.shape[2])
    for p in range(pairs):
        table = f_ref[pl.ds(p, chunk, stride=pairs), :].astype(BF16)
        lr_ref[p] = table
        at = pl.multiple_of(step * chunk, chunk)
        s_ref[p] += dot(c_ref[p, :, pl.ds(at, chunk)], table)

    @pl.when(step == pl.num_programs(0) - 1)
    def _():
        theta = colat_ref[...]
        cos, inv_sin = jnp.cos(theta), 1.0 / jnp.sin(theta)
        blocks = []
        for p in range(pairs):
            small = m_ref[first + p]
            for half, order in enumerate((small, modes - 1 - small)):
                at = 4 * lines * half
                s0, s1, s2, s3 = (s_ref[p, at + q * lines : at + (q + 1) * lines, :] for q in range(4))
                weight = jnp.where(order == 0, 1.0, 2.0) * modes ** (-0.5)
                ratio = order.astype(F32) * (1.0 / modes)
                blocks.append(s0 * weight)
                blocks.append((cos * s2 - s3) * inv_sin * weight)
                blocks.append(turn(s1) * ratio * inv_sin * weight)
            row = iota((wide - 6 * lines, s_ref.shape[2]), 0)
            low, high = (small % FOLD).astype(F32), (small // FOLD).astype(F32)
            blocks.append(jnp.where(row == 0, low, jnp.where(row == 1, high, 0.0)))
        fourier = jnp.concatenate(blocks, axis=0).astype(BF16)
        cycle_of_slot = slot_of_cycle(order_ref).T.astype(BF16)
        out_ref[...] = dot(cycle_of_slot, fourier, NT).astype(BF16)


def synth(tbar_alm, twf_alm, table, m_slots, cycle_order, colatitude, axis):
    pairs, sims, _, rows = tbar_alm.shape
    modes = rows - 1
    cycles = table.shape[2]
    steps = 8
    chunk = modes // steps
    lines = 2 * sims
    wide = 8 * lines
    vmem = pl.BlockSpec(memory_space=pltpu.VMEM)
    return pl.pallas_call(
        functools.partial(synth_kernel, axis),
        grid=(steps,),
        in_specs=[
            pl.BlockSpec(memory_space=pltpu.SMEM), vmem, vmem, vmem, vmem,
            pl.BlockSpec((chunk, pairs, cycles), lambda j: (j, 0, 0)),
            pl.BlockSpec((1, pairs, cycles), lambda j: (modes, 0, 0)),
        ],
        out_specs=[
            pl.BlockSpec((cycles, pairs * wide), lambda j: (0, 0)),
            pl.BlockSpec((pairs, chunk, cycles), lambda j: (0, j, 0)),
            pl.BlockSpec((pairs, cycles), lambda j: (0, 0)),
        ],
        out_shape=[
            jax.ShapeDtypeStruct((cycles, pairs * wide), BF16),
            jax.ShapeDtypeStruct((pairs, modes, cycles), BF16),
            jax.ShapeDtypeStruct((pairs, cycles), F32),
        ],
        scratch_shapes=[
            pltpu.VMEM((pairs, 8 * lines, modes), BF16),
            pltpu.VMEM((pairs, 8 * lines, cycles), F32),
            pltpu.VMEM((chunk * pairs, cycles), F32),
            pltpu.VMEM((pairs, modes), F32),
            pltpu.VMEM((pairs, modes), F32),
        ],
        name="synth",
    )(m_slots, cycle_order.reshape(1, -1), colatitude.reshape(1, -1), tbar_alm, twf_alm, table, table)


def angles(left, right, period):
    return 2.0 * np.pi * (np.outer(left, right) % period) / period


def split(table):
    high = table.astype(np.float32).astype(jnp.bfloat16)
    return high, (table - high.astype(np.float64)).astype(np.float32).astype(jnp.bfloat16)


def sky_tables(modes, pixels):
    m1, j2, m2 = np.arange(FOLD), np.arange(FOLD), np.arange(modes // FOLD)
    j1 = np.arange(pixels // FOLD).reshape(-1, 2).T.reshape(-1)
    th = angles(j2, m2, FOLD).reshape(FOLD, 2, -1)
    c, s = np.cos(th), np.sin(th)
    first = np.stack([np.stack([c, -s], 2), np.stack([s, c], 2)], 0).reshape(2 * FOLD, -1)
    th = angles(j2, m1, pixels)
    twist = np.stack([np.tile(np.cos(th), (1, 2)), np.tile(np.sin(th), (1, 2))])
    th = angles(m1, j1, FOLD)
    two = np.eye(2)
    second = np.concatenate([np.kron(two, np.cos(th)), np.kron(two, -np.sin(th))], 0)
    third = np.concatenate([np.kron(two, np.cos(th.T)), np.kron(two, -np.sin(th.T))], 1)
    th = angles(m2, j2, FOLD).reshape(2, -1, FOLD)
    c, s = np.cos(th), np.sin(th)
    fourth = np.stack([np.concatenate([c, s], 2), np.concatenate([-s, c], 2)], 1)
    fourth = fourth.reshape(2 * modes // FOLD, -1)
    return (
        np.concatenate(split(first), 1), twist.astype(np.float32), np.concatenate(split(second), 0),
        np.concatenate(split(third), 0), np.concatenate(split(fourth), 1),
    )


def sky_kernel(
    pairs, sims, x_ref, mask_ref, first_ref, twist_ref, second_ref, third_ref, fourth_ref, out_ref,
    xt_ref, lhs_ref, hot_ref,
):
    devices, width = x_ref.shape
    wide = width // pairs
    lines = 2 * sims
    half_sims = sims // 2
    fold2 = 2 * FOLD
    tall = fourth_ref.shape[0] // 4
    xt_ref[...] = x_ref[...].astype(F32).T
    groups = [(q, a) for q in range(3) for a in range(half_sims)]

    def key(p, half):
        low = xt_ref[p * wide + 6 * lines : p * wide + 6 * lines + 1, :].astype(jnp.int32)
        high = xt_ref[p * wide + 6 * lines + 1 : p * wide + 6 * lines + 2, :].astype(jnp.int32)
        return (FOLD - 1 - low, tall - 1 - high) if half else (low, high)

    sorted_halves, places = [], []
    for half in range(2):
        place = []
        for p in range(pairs):
            low, high = key(p, half)
            place.append(iota((tall, devices), 0) == high)
            for e in range(2):
                at = (e * pairs + p) * devices
                hot_ref[half, :, at : at + devices] = jnp.where(
                    iota((fold2, devices), 0) == low + e * FOLD, 1.0, 0.0
                ).astype(BF16)
                parts = []
                for q, a in groups:
                    for c in range(2):
                        row = p * wide + (half * 3 + q) * lines + (e * half_sims + a) * 2 + c
                        parts.append(jnp.where(place[p], xt_ref[row : row + 1, :], 0.0))
                lhs_ref[:, at : at + devices] = jnp.concatenate(parts, axis=0).astype(BF16)
        places.append(place)
        sorted_halves.append(dot(lhs_ref[...], hot_ref[half], NT).astype(BF16))

    n = 2 * tall
    spread = jnp.concatenate(
        [
            jnp.concatenate([s[g * n : (g + 1) * n] for s in sorted_halves], axis=0)
            for g in range(len(groups))
        ],
        axis=1,
    )
    stage = dot(first_ref[...], jnp.concatenate([spread, spread], axis=0))
    cos, sin = twist_ref[0], twist_ref[1]
    twisted = []
    for g in range(len(groups)):
        re, im = (stage[i * FOLD : (i + 1) * FOLD, g * fold2 : (g + 1) * fold2] for i in range(2))
        twisted.append(jnp.concatenate([re * cos - im * sin, re * sin + im * cos], axis=1))
    twisted = jnp.concatenate(twisted, axis=0).astype(BF16)
    maps = dot(twisted, second_ref[: 2 * fold2]) + dot(twisted, second_ref[2 * fold2 :])

    mask = mask_ref[...].astype(F32).T
    mask = jnp.concatenate([mask[:FOLD], mask[FOLD:]] * 2, axis=1)
    products = []
    for q in range(1, 3):
        for a in range(half_sims):
            one = maps[a * FOLD : (a + 1) * FOLD]
            at = (q * half_sims + a) * FOLD
            products.append(mask * one * maps[at : at + FOLD])
    products = jnp.concatenate(products, axis=0).astype(BF16)
    stage = dot(products, third_ref[:fold2]) + dot(products, third_ref[fold2:])
    twisted = []
    for g in range(2 * half_sims):
        re, im = (stage[g * FOLD : (g + 1) * FOLD, i * fold2 : (i + 1) * fold2] for i in range(2))
        twisted.append(jnp.concatenate([re * cos + im * sin, im * cos - re * sin], axis=0))
    twisted = jnp.concatenate(twisted, axis=1).astype(BF16)
    pixels = mask_ref.shape[0] * mask_ref.shape[1]
    spectra = dot(fourth_ref[...], jnp.concatenate([twisted, twisted], axis=0)) * pixels ** (-0.5)
    spectra = spectra.astype(BF16)

    groups = 2 * half_sims
    add = jnp.where(
        iota((2 * groups, 2 * groups * tall), 1) // tall == iota((2 * groups, 2 * groups * tall), 0), 1.0, 0.0
    ).astype(BF16)
    found = []
    for half in range(2):
        rows = jnp.concatenate(
            [spectra[half * n : (half + 1) * n, g * fold2 : (g + 1) * fold2] for g in range(groups)], axis=0
        )
        for e in range(2):
            for p in range(pairs):
                at = (e * pairs + p) * devices
                values = dot(rows, hot_ref[half, :, at : at + devices])
                keep = jnp.concatenate([places[half][p]] * (2 * groups), axis=0)
                lhs_ref[: values.shape[0], at : at + devices] = jnp.where(keep, values, 0.0).astype(BF16)
        found.append(dot(add, lhs_ref[: 2 * groups * tall, :]))
    blocks = []
    upper = iota((lines, devices), 0) >= lines // 2
    for p in range(pairs):
        for half in range(2):
            a, b = (
                found[half][:, (e * pairs + p) * devices : (e * pairs + p + 1) * devices] for e in range(2)
            )
            blocks.append(jnp.where(upper, pltpu.roll(b, lines // 2, 0), a))
            blocks.append(jnp.where(upper, b, pltpu.roll(a, lines // 2, 0)))
    out_ref[...] = jnp.concatenate(blocks, axis=0).T.astype(BF16)


def sky(received, pixel_mask, pairs, sims, modes):
    devices = received.shape[0]
    pixels = pixel_mask.shape[1]
    tables = sky_tables(modes, pixels)
    vmem = pl.BlockSpec(memory_space=pltpu.VMEM)
    tall = modes // FOLD // 2
    return pl.pallas_call(
        functools.partial(sky_kernel, pairs, sims),
        in_specs=[vmem] * 7,
        out_specs=vmem,
        out_shape=jax.ShapeDtypeStruct((devices, pairs * 8 * sims), BF16),
        scratch_shapes=[
            pltpu.VMEM(received.shape[::-1], F32),
            pltpu.VMEM((3 * sims * tall, 2 * pairs * devices), BF16),
            pltpu.VMEM((2, 2 * FOLD, 2 * pairs * devices), BF16),
        ],
        name="sky",
    )(received, pixel_mask.reshape(-1, 2 * FOLD), *(jnp.asarray(t) for t in tables))


def analyse_kernel(
    axis, m_ref, order_ref, colat_ref, weight_ref, r_ref, l_ref, tail_ref, grad_ref, curl_ref,
    w_ref, deg_ref, eps_ref, ord_ref,
):
    p = pl.program_id(0)
    pairs, lines2, cycles = w_ref.shape
    lines = lines2 // 8
    modes = l_ref.shape[1]
    first = lax.axis_index(axis) * pairs
    factor = (modes / cycles) ** 0.5

    def scale_of(degree):
        return factor / jnp.sqrt(jnp.maximum(degree * (degree + 1.0), 1.0))

    @pl.when(p == 0)
    def _():
        small = small_column(m_ref, first, pairs)
        (degree, orders, eps), _ = layout_rows(small, modes)
        scale = scale_of(degree)
        deg_ref[...] = degree * scale
        eps_ref[...] = eps * scale
        ord_ref[...] = orders * scale
        spectra = dot(r_ref[...].astype(F32).T.astype(BF16), slot_of_cycle(order_ref).astype(BF16), NT)
        theta, weight = colat_ref[...], weight_ref[...]
        with_cos = weight * jnp.cos(theta) / jnp.sin(theta)
        with_sin = weight / jnp.sin(theta)
        for i in range(pairs):
            for half in range(2):
                for q in range(2):
                    at = ((i * 2 + half) * 2 + q) * lines
                    values = spectra[at : at + lines]
                    at = (half * 4 + q * 2) * lines
                    w_ref[i, at : at + lines] = (values * with_cos).astype(BF16)
                    w_ref[i, at + lines : at + 2 * lines] = (values * with_sin).astype(BF16)

    small = m_ref[first + p]
    level, raised, azimuth = (ref[pl.ds(p, 1), :] for ref in (deg_ref, eps_ref, ord_ref))
    weighted = w_ref[p]
    sums = dot(weighted, l_ref[0], NT)
    k = iota((lines, modes), 1)
    upper = k >= modes - small
    a0, a1, a2, a3 = (
        jnp.where(upper, sums[(4 + q) * lines : (5 + q) * lines], sums[q * lines : (q + 1) * lines])
        for q in range(4)
    )

    def previous(values):
        return jnp.where(k == 0, 0.0, pltpu.roll(values, 1, 1))

    grad = level * a0 - raised * previous(a1) - azimuth * turn(a3)
    curl = level * a2 - raised * previous(a3) + azimuth * turn(a1)
    last = jnp.sum(
        weighted[4 * lines :].astype(F32) * tail_ref[pl.ds(p, 1), :], axis=1, keepdims=True
    )
    degree = jnp.full((1, 1), modes - 1, F32)
    order = jnp.full((1, 1), modes - 1 - small, jnp.int32).astype(F32)
    scale = scale_of(degree)
    level, raised, azimuth = degree * scale, raising(degree, order) * scale, order * scale
    b0, b1, b2, b3 = (last[q * lines : (q + 1) * lines] for q in range(4))
    last_grad = level * b0 - raised * a1[:, modes - 1 :] - azimuth * turn(b3)
    last_curl = level * b2 - raised * a3[:, modes - 1 :] + azimuth * turn(b1)
    for s in range(lines // 2):
        rows = slice(2 * s, 2 * s + 2)
        grad_ref[0, s, :, :modes] = grad[rows]
        grad_ref[0, s, :, modes:] = last_grad[rows]
        curl_ref[0, s, :, :modes] = curl[rows]
        curl_ref[0, s, :, modes:] = last_curl[rows]


def analyse(returned, table, tail, m_slots, cycle_order, colatitude, cycle_weight, sims, axis):
    pairs, modes, cycles = table.shape
    vmem = pl.BlockSpec(memory_space=pltpu.VMEM)
    out = jax.ShapeDtypeStruct((pairs, sims, 2, modes + 1), F32)
    out_spec = pl.BlockSpec((1, sims, 2, modes + 1), lambda p: (p, 0, 0, 0))
    return pl.pallas_call(
        functools.partial(analyse_kernel, axis),
        grid=(pairs,),
        in_specs=[
            pl.BlockSpec(memory_space=pltpu.SMEM), vmem, vmem, vmem, vmem,
            pl.BlockSpec((1, modes, cycles), lambda p: (p, 0, 0)), vmem,
        ],
        out_specs=[out_spec, out_spec],
        out_shape=[out, out],
        scratch_shapes=[
            pltpu.VMEM((pairs, 16 * sims, cycles), BF16),
            pltpu.VMEM((pairs, modes), F32),
            pltpu.VMEM((pairs, modes), F32),
            pltpu.VMEM((pairs, modes), F32),
        ],
        name="analyse",
    )(m_slots, cycle_order.reshape(1, -1), colatitude.reshape(1, -1), cycle_weight.reshape(1, -1), returned, table, tail)


def shards(axis, tbar_alm, twf_alm, legendre, m_slots, cycle_order, colatitude, cycle_weight, pixel_mask):
    pairs, sims, _, rows = tbar_alm.shape
    by_row = jnp.transpose(legendre, (1, 0, 2))
    outgoing, table, tail = synth(tbar_alm, twf_alm, by_row, m_slots, cycle_order, colatitude, axis)
    received = lax.all_to_all(outgoing, axis, 0, 0, tiled=True)
    spectra = sky(received, pixel_mask, pairs, sims, rows - 1)
    returned = lax.all_to_all(spectra, axis, 0, 0, tiled=True)
    return analyse(returned, table, tail, m_slots, cycle_order, colatitude, cycle_weight, sims, axis)


def solution(mesh):
    coefficients = P("ma", "grp", None, None)
    return jax.shard_map(
        functools.partial(shards, "ma"),
        mesh=mesh,
        in_specs=(coefficients, coefficients, P("ma", None, None), P(), P(), P(), P(), P("ma", None)),
        out_specs=(coefficients, coefficients),
        check_vma=False,
    )
```

```python
import functools
import math

import jax
import jax.numpy as jnp
import numpy as np
from jax import lax
from jax.experimental import pallas as pl
from jax.experimental.pallas import tpu as pltpu
from jax.sharding import PartitionSpec as P

F32 = jnp.float32
BF16 = jnp.bfloat16
LANES = 128
FOLD = 64
GRANT = 24 * 2**20
NT = (((1,), (1,)), ((), ()))
NN = (((1,), (0,)), ((), ()))


def dot(a, b, dims=NN):
    return lax.dot_general(a, b, dims, preferred_element_type=F32)


def iota(shape, dim):
    return lax.broadcasted_iota(jnp.int32, shape, dim)


def small_column(m_ref, first, pairs):
    row = iota((pairs, 1), 0)
    column = jnp.zeros((pairs, 1), jnp.int32)
    for p in range(pairs):
        column = jnp.where(row == p, m_ref[first + p], column)
    return column


def layout_rows(small, modes):
    k = iota((small.shape[0], modes), 1)
    upper = k >= modes - small
    degree = jnp.where(upper, k - 1, small + k).astype(F32)
    orders = jnp.where(upper, modes - 1 - small, small).astype(F32)
    last_degree = jnp.full(small.shape, modes - 1, F32)
    last_orders = (modes - 1 - small).astype(F32)
    return (
        (degree, orders, raising(degree, orders)),
        (last_degree, last_orders, raising(last_degree, last_orders)),
    )


def raising(degree, orders):
    square = (
        (degree * degree - orders * orders)
        * (2.0 * degree + 1.0)
        / jnp.maximum(2.0 * degree - 1.0, 1.0)
    )
    return jnp.where(degree > orders, jnp.sqrt(jnp.where(degree > orders, square, 0.0)), 0.0)


def slot_of_cycle(order_ref):
    n = order_ref.shape[1]
    return jnp.where(iota((n, n), 0) == order_ref[...], 1.0, 0.0)


def turn(values):
    rows = values.shape[0]
    real = iota(values.shape, 0) % 2 == 0
    return jnp.where(real, -pltpu.roll(values, rows - 1, 0), pltpu.roll(values, 1, 0))


def synth_kernel(
    axis, m_hbm, order_hbm, colat_hbm, t_hbm, w_hbm, l_hbm, out_ref, lr_ref, ltail_ref,
    m_ref, order_ref, colat_ref, t_ref, w_ref, l_ref, c_ref, s_ref, deg_ref, eps_ref, sems,
):
    pairs, sims = t_ref.shape[0], t_ref.shape[1]
    modes = t_ref.shape[3] - 1
    lines = 2 * sims
    steps = sems.shape[0] - 6
    chunk = modes // steps
    first = lax.axis_index(axis) * pairs
    wide = out_ref.shape[1] * out_ref.shape[2] // pairs

    pieces = [(m_hbm, m_ref), (order_hbm, order_ref), (colat_hbm, colat_ref), (w_hbm, w_ref), (t_hbm, t_ref)]
    for j in range(steps + 1):
        part = pl.ds(j * chunk, chunk if j < steps else 1)
        pieces.append((l_hbm.at[part], l_ref.at[part]))
    copies = [pltpu.make_async_copy(*piece, sems.at[i]) for i, piece in enumerate(pieces)]
    for copy in copies:
        copy.start()
    for copy in copies[:3]:
        copy.wait()

    small = small_column(m_ref, first, pairs)
    (degree, _, eps), (_, _, last_eps) = layout_rows(small, modes)
    deg_ref[...] = degree * (1.0 / modes)
    eps_ref[...] = eps * (1.0 / modes)
    last_eps = last_eps * (1.0 / modes)
    theta = colat_ref[...]
    cos, inv_sin = jnp.cos(theta), 1.0 / jnp.sin(theta)
    cycle_of_slot = slot_of_cycle(order_ref).T.astype(BF16)
    k = iota((1, modes), 1)
    ends = iota((lines, modes), 1) == modes - 1

    copies[3].wait()
    copies[4].wait()
    lasts = []
    for p in range(pairs):
        tbar = t_ref[p].reshape(lines, modes + 1)
        wiener = w_ref[p].reshape(lines, modes + 1).astype(F32)
        main, last = wiener[:, :modes], wiener[:, modes:]
        raised = pltpu.roll(eps_ref[p : p + 1, :] * main, modes - 1, 1)
        raised = jnp.where(ends, last_eps[p : p + 1, :] * last, raised)
        sets = jnp.concatenate(
            [
                jnp.concatenate([tbar[:, :modes].astype(F32), main], axis=0).astype(BF16),
                jnp.concatenate([deg_ref[p : p + 1, :] * main, raised], axis=0).astype(BF16),
            ],
            axis=0,
        )
        upper = jnp.where(k >= modes - m_ref[first + p], 1.0, 0.0)
        upper = jnp.broadcast_to(upper, (4 * lines, modes)).astype(BF16)
        above = sets * upper
        c_ref[p, : 4 * lines, :] = sets - above
        c_ref[p, 4 * lines :, :] = above
        lasts.append(
            jnp.concatenate(
                [tbar[:, modes:].astype(F32), last, ((modes - 1.0) / modes) * last, 0.0 * last], axis=0
            )
            .astype(BF16)
            .astype(F32)
        )

    copies[-1].wait()
    tail_rows = l_ref[modes].astype(F32)
    ltail_ref[...] = tail_rows
    for p in range(pairs):
        s_ref[p, : 4 * lines] = jnp.zeros((4 * lines, s_ref.shape[2]), F32)
        s_ref[p, 4 * lines :] = lasts[p] * tail_rows[p : p + 1, :]
    for j in range(steps):
        copies[5 + j].wait()
        at = slice(j * chunk, (j + 1) * chunk)
        table = jnp.swapaxes(l_ref[at], 0, 1)
        lr_ref[:, at, :] = table
        for p in range(pairs):
            s_ref[p] += dot(c_ref[p, :, at], table[p])

    blocks = []
    for p in range(pairs):
        small = m_ref[first + p]
        for half, order in enumerate((small, modes - 1 - small)):
            at = 4 * lines * half
            s0, s1, s2, s3 = (s_ref[p, at + q * lines : at + (q + 1) * lines, :] for q in range(4))
            weight = jnp.where(order == 0, 1.0, 2.0) * modes ** (-0.5)
            ratio = order.astype(F32) * (1.0 / modes)
            blocks.append(s0 * weight)
            blocks.append((cos * s2 - s3) * inv_sin * weight)
            blocks.append(turn(s1) * ratio * inv_sin * weight)
        row = iota((wide - 6 * lines, s_ref.shape[2]), 0)
        low, high = (small % FOLD).astype(F32), (small // FOLD).astype(F32)
        blocks.append(jnp.where(row == 0, low, jnp.where(row == 1, high, 0.0)))
    fourier = jnp.concatenate(blocks, axis=0).astype(BF16)
    out_ref[...] = dot(cycle_of_slot, fourier, NT).astype(BF16).reshape(out_ref.shape)


def synth(tbar_alm, twf_alm, table, m_slots, cycle_order, colatitude, axis):
    pairs, sims, _, rows = tbar_alm.shape
    modes = rows - 1
    cycles = table.shape[2]
    lines = 2 * sims
    wide = 8 * lines
    steps = 8
    vmem = pl.BlockSpec(memory_space=pltpu.VMEM)
    hbm = pl.BlockSpec(memory_space=pltpu.HBM)
    return pl.pallas_call(
        functools.partial(synth_kernel, axis),
        in_specs=[hbm] * 6,
        out_specs=[vmem] * 3,
        out_shape=[
            pltpu.VMEM((cycles, pairs * wide // LANES, LANES), BF16),
            pltpu.VMEM((pairs, modes, cycles), BF16),
            pltpu.VMEM((pairs, cycles), F32),
        ],
        scratch_shapes=[
            pltpu.SMEM(m_slots.shape, jnp.int32),
            pltpu.VMEM((1, cycles), jnp.int32),
            pltpu.VMEM((1, cycles), F32),
            pltpu.VMEM(tbar_alm.shape, BF16),
            pltpu.VMEM(twf_alm.shape, BF16),
            pltpu.VMEM(table.shape, BF16),
            pltpu.VMEM((pairs, 8 * lines, modes), BF16),
            pltpu.VMEM((pairs, 8 * lines, cycles), F32),
            pltpu.VMEM((pairs, modes), F32),
            pltpu.VMEM((pairs, modes), F32),
            pltpu.SemaphoreType.DMA((steps + 6,)),
        ],
        compiler_params=pltpu.CompilerParams(vmem_limit_bytes=GRANT),
        name="synth",
    )(*(pltpu.with_memory_space_constraint(x, pltpu.HBM) for x in (
        m_slots, cycle_order.reshape(1, -1), colatitude.reshape(1, -1), tbar_alm, twf_alm, table
    )))


def angles(left, right, period):
    return 2.0 * np.pi * (np.outer(left, right) % period) / period


def split(table):
    high = table.astype(np.float32).astype(jnp.bfloat16)
    return high, (table - high.astype(np.float64)).astype(np.float32).astype(jnp.bfloat16)


def sky_tables(modes, pixels):
    m1, j2, m2 = np.arange(FOLD), np.arange(FOLD), np.arange(modes // FOLD)
    j1 = np.arange(pixels // FOLD).reshape(-1, 2).T.reshape(-1)
    th = angles(j2, m2, FOLD).reshape(FOLD, 2, -1)
    c, s = np.cos(th), np.sin(th)
    first = np.stack([np.stack([c, -s], 2), np.stack([s, c], 2)], 0).reshape(2 * FOLD, -1)
    th = angles(j2, m1, pixels)
    twist = np.stack([np.tile(np.cos(th), (1, 2)), np.tile(np.sin(th), (1, 2))])
    th = angles(m1, j1, FOLD)
    two = np.eye(2)
    second = np.concatenate([np.kron(two, np.cos(th)), np.kron(two, -np.sin(th))], 0)
    third = np.concatenate([np.kron(two, np.cos(th.T)), np.kron(two, -np.sin(th.T))], 1)
    th = angles(m2, j2, FOLD).reshape(2, -1, FOLD)
    c, s = np.cos(th), np.sin(th)
    fourth = np.stack([np.concatenate([c, s], 2), np.concatenate([-s, c], 2)], 1)
    fourth = fourth.reshape(2 * modes // FOLD, -1)
    return (
        np.concatenate(split(first), 1), twist.astype(np.float32), np.concatenate(split(second), 0),
        np.concatenate(split(third), 0), np.concatenate(split(fourth), 1),
    )


def sky_kernel(
    pairs, sims, x_ref, mask_ref, first_ref, twist_ref, second_ref, third_ref, fourth_ref, out_ref,
    xt_ref, lhs_ref, hot_ref,
):
    devices = x_ref.shape[0]
    width = x_ref.shape[1] * x_ref.shape[2]
    wide = width // pairs
    lines = 2 * sims
    half_sims = sims // 2
    fold2 = 2 * FOLD
    tall = fourth_ref.shape[0] // 4
    xt_ref[...] = x_ref[...].reshape(devices, width).astype(F32).T
    groups = [(q, a) for q in range(3) for a in range(half_sims)]

    def key(p, half):
        low = xt_ref[p * wide + 6 * lines : p * wide + 6 * lines + 1, :].astype(jnp.int32)
        high = xt_ref[p * wide + 6 * lines + 1 : p * wide + 6 * lines + 2, :].astype(jnp.int32)
        return (FOLD - 1 - low, tall - 1 - high) if half else (low, high)

    sorted_halves, places = [], []
    for half in range(2):
        place = []
        for p in range(pairs):
            low, high = key(p, half)
            place.append(iota((tall, devices), 0) == high)
            for e in range(2):
                at = (e * pairs + p) * devices
                hot_ref[half, :, at : at + devices] = jnp.where(
                    iota((fold2, devices), 0) == low + e * FOLD, 1.0, 0.0
                ).astype(BF16)
                parts = []
                for q, a in groups:
                    for c in range(2):
                        row = p * wide + (half * 3 + q) * lines + (e * half_sims + a) * 2 + c
                        parts.append(jnp.where(place[p], xt_ref[row : row + 1, :], 0.0))
                lhs_ref[:, at : at + devices] = jnp.concatenate(parts, axis=0).astype(BF16)
        places.append(place)
        sorted_halves.append(dot(lhs_ref[...], hot_ref[half], NT).astype(BF16))

    n = 2 * tall
    spread = jnp.concatenate(
        [
            jnp.concatenate([s[g * n : (g + 1) * n] for s in sorted_halves], axis=0)
            for g in range(len(groups))
        ],
        axis=1,
    )
    stage = dot(first_ref[...], jnp.concatenate([spread, spread], axis=0))
    cos, sin = twist_ref[0], twist_ref[1]
    twisted = []
    for g in range(len(groups)):
        re, im = (stage[i * FOLD : (i + 1) * FOLD, g * fold2 : (g + 1) * fold2] for i in range(2))
        twisted.append(jnp.concatenate([re * cos - im * sin, re * sin + im * cos], axis=1))
    twisted = jnp.concatenate(twisted, axis=0).astype(BF16)
    maps = dot(twisted, second_ref[: 2 * fold2]) + dot(twisted, second_ref[2 * fold2 :])

    mask = mask_ref[...].astype(F32).T
    mask = jnp.concatenate([mask[:FOLD], mask[FOLD:]] * 2, axis=1)
    products = []
    for q in range(1, 3):
        for a in range(half_sims):
            one = maps[a * FOLD : (a + 1) * FOLD]
            at = (q * half_sims + a) * FOLD
            products.append(mask * one * maps[at : at + FOLD])
    products = jnp.concatenate(products, axis=0).astype(BF16)
    stage = dot(products, third_ref[:fold2]) + dot(products, third_ref[fold2:])
    twisted = []
    for g in range(2 * half_sims):
        re, im = (stage[g * FOLD : (g + 1) * FOLD, i * fold2 : (i + 1) * fold2] for i in range(2))
        twisted.append(jnp.concatenate([re * cos + im * sin, im * cos - re * sin], axis=0))
    twisted = jnp.concatenate(twisted, axis=1).astype(BF16)
    pixels = mask_ref.shape[0] * mask_ref.shape[1]
    spectra = dot(fourth_ref[...], jnp.concatenate([twisted, twisted], axis=0)) * pixels ** (-0.5)
    spectra = spectra.astype(BF16)

    groups = 2 * half_sims
    add = jnp.where(
        iota((2 * groups, 2 * groups * tall), 1) // tall == iota((2 * groups, 2 * groups * tall), 0), 1.0, 0.0
    ).astype(BF16)
    found = []
    for half in range(2):
        rows = jnp.concatenate(
            [spectra[half * n : (half + 1) * n, g * fold2 : (g + 1) * fold2] for g in range(groups)], axis=0
        )
        for e in range(2):
            for p in range(pairs):
                at = (e * pairs + p) * devices
                values = dot(rows, hot_ref[half, :, at : at + devices])
                keep = jnp.concatenate([places[half][p]] * (2 * groups), axis=0)
                lhs_ref[: values.shape[0], at : at + devices] = jnp.where(keep, values, 0.0).astype(BF16)
        found.append(dot(add, lhs_ref[: 2 * groups * tall, :]))
    blocks = []
    upper = iota((lines, devices), 0) >= lines // 2
    for p in range(pairs):
        for half in range(2):
            a, b = (
                found[half][:, (e * pairs + p) * devices : (e * pairs + p + 1) * devices] for e in range(2)
            )
            blocks.append(jnp.where(upper, pltpu.roll(b, lines // 2, 0), a))
            blocks.append(jnp.where(upper, b, pltpu.roll(a, lines // 2, 0)))
    out_ref[...] = jnp.concatenate(blocks, axis=0).T.astype(BF16).reshape(out_ref.shape)


def sky(received, pixel_mask, pairs, sims, modes):
    devices = received.shape[0]
    pixels = pixel_mask.shape[1]
    tables = sky_tables(modes, pixels)
    vmem = pl.BlockSpec(memory_space=pltpu.VMEM)
    tall = modes // FOLD // 2
    return pl.pallas_call(
        functools.partial(sky_kernel, pairs, sims),
        in_specs=[vmem] * 7,
        out_specs=vmem,
        out_shape=jax.ShapeDtypeStruct((devices, pairs * 8 * sims // LANES, LANES), BF16),
        scratch_shapes=[
            pltpu.VMEM((received.shape[1] * LANES, devices), F32),
            pltpu.VMEM((3 * sims * tall, 2 * pairs * devices), BF16),
            pltpu.VMEM((2, 2 * FOLD, 2 * pairs * devices), BF16),
        ],
        compiler_params=pltpu.CompilerParams(vmem_limit_bytes=GRANT),
        name="sky",
    )(received, pixel_mask.reshape(-1, 2 * FOLD), *(jnp.asarray(t) for t in tables))


def analyse_kernel(
    axis, m_ref, order_ref, colat_ref, weight_ref, r_ref, l_ref, tail_ref, grad_hbm, curl_hbm,
    w_ref, deg_ref, eps_ref, ord_ref, grad_ref, curl_ref, sems,
):
    pairs, modes, cycles = l_ref.shape
    lines = w_ref.shape[1] // 8
    sims = lines // 2
    first = lax.axis_index(axis) * pairs
    factor = (modes / cycles) ** 0.5

    def scale_of(degree):
        return factor / jnp.sqrt(jnp.maximum(degree * (degree + 1.0), 1.0))

    small = small_column(m_ref, first, pairs)
    (degree, orders, eps), (last_degree, last_orders, last_eps) = layout_rows(small, modes)
    scale = scale_of(degree)
    deg_ref[...] = degree * scale
    eps_ref[...] = eps * scale
    ord_ref[...] = orders * scale
    scale = scale_of(last_degree)
    last_degree, last_orders, last_eps = last_degree * scale, last_orders * scale, last_eps * scale

    rows = r_ref[...].reshape(cycles, r_ref.shape[1] * r_ref.shape[2])
    spectra = dot(rows.astype(F32).T.astype(BF16), slot_of_cycle(order_ref).astype(BF16), NT)
    theta, weight = colat_ref[...], weight_ref[...]
    with_cos = weight * jnp.cos(theta) / jnp.sin(theta)
    with_sin = weight / jnp.sin(theta)
    for i in range(pairs):
        for half in range(2):
            parts = []
            for q in range(2):
                at = ((i * 2 + half) * 2 + q) * lines
                values = spectra[at : at + lines]
                parts += [values * with_cos, values * with_sin]
            w_ref[i, half * 4 * lines : (half + 1) * 4 * lines] = jnp.concatenate(parts, axis=0).astype(BF16)

    k = iota((lines, modes), 1)
    starts = k == 0

    def previous(values):
        return jnp.where(starts, 0.0, pltpu.roll(values, 1, 1))

    copies = []
    for p in range(pairs):
        weighted = w_ref[p]
        sums = dot(weighted, l_ref[p], NT)
        upper = k >= modes - m_ref[first + p]
        a0, a1, a2, a3 = (
            jnp.where(upper, sums[(4 + q) * lines : (5 + q) * lines], sums[q * lines : (q + 1) * lines])
            for q in range(4)
        )
        level, raised, azimuth = (ref[p : p + 1, :] for ref in (deg_ref, eps_ref, ord_ref))
        grad = level * a0 - raised * previous(a1) - azimuth * turn(a3)
        curl = level * a2 - raised * previous(a3) + azimuth * turn(a1)
        last = jnp.sum(weighted[4 * lines :].astype(F32) * tail_ref[p : p + 1, :], axis=1, keepdims=True)
        level, raised, azimuth = (v[p : p + 1, :] for v in (last_degree, last_eps, last_orders))
        b0, b1, b2, b3 = (last[q * lines : (q + 1) * lines] for q in range(4))
        last_grad = level * b0 - raised * a1[:, modes - 1 :] - azimuth * turn(b3)
        last_curl = level * b2 - raised * a3[:, modes - 1 :] + azimuth * turn(b1)
        for ref, hbm, main, last in ((grad_ref, grad_hbm, grad, last_grad), (curl_ref, curl_hbm, curl, last_curl)):
            ref[p, :, :, :modes] = main.reshape(sims, 2, modes)
            ref[p, :, :, modes:] = last.reshape(sims, 2, 1)
            copies.append(pltpu.make_async_copy(ref.at[p], hbm.at[p], sems.at[len(copies)]))
            copies[-1].start()
    for copy in copies:
        copy.wait()


def analyse(returned, table, tail, m_slots, cycle_order, colatitude, cycle_weight, sims, axis):
    pairs, modes, cycles = table.shape
    vmem = pl.BlockSpec(memory_space=pltpu.VMEM)
    hbm = pl.BlockSpec(memory_space=pltpu.HBM)
    shape = (pairs, sims, 2, modes + 1)
    out = jax.ShapeDtypeStruct(shape, F32)
    return pl.pallas_call(
        functools.partial(analyse_kernel, axis),
        in_specs=[pl.BlockSpec(memory_space=pltpu.SMEM)] + [vmem] * 6,
        out_specs=[hbm, hbm],
        out_shape=[out, out],
        scratch_shapes=[
            pltpu.VMEM((pairs, 16 * sims, cycles), BF16),
            pltpu.VMEM((pairs, modes), F32),
            pltpu.VMEM((pairs, modes), F32),
            pltpu.VMEM((pairs, modes), F32),
            pltpu.VMEM(shape, F32),
            pltpu.VMEM(shape, F32),
            pltpu.SemaphoreType.DMA((2 * pairs,)),
        ],
        compiler_params=pltpu.CompilerParams(vmem_limit_bytes=GRANT),
        name="analyse",
    )(m_slots, cycle_order.reshape(1, -1), colatitude.reshape(1, -1), cycle_weight.reshape(1, -1), returned, table, tail)


def exchange(values, axis):
    return lax.all_to_all(values, axis, 0, 0, tiled=True)


def shards(axis, tbar_alm, twf_alm, legendre, m_slots, cycle_order, colatitude, cycle_weight, pixel_mask):
    pairs, sims, _, rows = tbar_alm.shape
    by_row = jnp.transpose(legendre, (1, 0, 2))
    outgoing, table, tail = synth(tbar_alm, twf_alm, by_row, m_slots, cycle_order, colatitude, axis)
    received = exchange(outgoing, axis)
    spectra = sky(received, pixel_mask, pairs, sims, rows - 1)
    returned = exchange(spectra, axis)
    return analyse(returned, table, tail, m_slots, cycle_order, colatitude, cycle_weight, sims, axis)


def solution(mesh):
    coefficients = P("ma", "grp", None, None)
    return jax.shard_map(
        functools.partial(shards, "ma"),
        mesh=mesh,
        in_specs=(coefficients, coefficients, P("ma", None, None), P(), P(), P(), P(), P("ma", None)),
        out_specs=(coefficients, coefficients),
        check_vma=False,
    )
```

```python
import functools
import math

import jax
import jax.numpy as jnp
import numpy as np
from jax import lax
from jax.experimental import pallas as pl
from jax.experimental.pallas import tpu as pltpu
from jax.sharding import Mesh
from jax.sharding import PartitionSpec as P

F32 = jnp.float32
BF16 = jnp.bfloat16
LANES = 128
FOLD = 64
GRANT = 24 * 2**20
CHIP, CORE = "chip", "core"
NT = (((1,), (1,)), ((), ()))
NN = (((1,), (0,)), ((), ()))


def dot(a, b, dims=NN):
    return lax.dot_general(a, b, dims, preferred_element_type=F32)


def iota(shape, dim):
    return lax.broadcasted_iota(jnp.int32, shape, dim)


def small_column(m_ref, first, pairs):
    row = iota((pairs, 1), 0)
    column = jnp.zeros((pairs, 1), jnp.int32)
    for p in range(pairs):
        column = jnp.where(row == p, m_ref[first + p], column)
    return column


def layout_rows(small, modes):
    k = iota((small.shape[0], modes), 1)
    upper = k >= modes - small
    degree = jnp.where(upper, k - 1, small + k).astype(F32)
    orders = jnp.where(upper, modes - 1 - small, small).astype(F32)
    last_degree = jnp.full(small.shape, modes - 1, F32)
    last_orders = (modes - 1 - small).astype(F32)
    return (
        (degree, orders, raising(degree, orders)),
        (last_degree, last_orders, raising(last_degree, last_orders)),
    )


def raising(degree, orders):
    square = (
        (degree * degree - orders * orders)
        * (2.0 * degree + 1.0)
        / jnp.maximum(2.0 * degree - 1.0, 1.0)
    )
    return jnp.where(degree > orders, jnp.sqrt(jnp.where(degree > orders, square, 0.0)), 0.0)


def slot_of_cycle(order_ref):
    n = order_ref.shape[1]
    core = lax.axis_index(CORE)
    place = iota((n, n), 1)
    near = place < n // 2
    slot = 2 * (place % (n // 2)) + jnp.where(near, core, 1 - core)
    pick = jnp.where(iota((n, n), 0) == slot, 1.0, 0.0).astype(BF16)
    order = jnp.broadcast_to(order_ref[...].astype(F32), (8, n)).astype(BF16)
    return jnp.where(iota((n, n), 0).astype(F32) == dot(order, pick)[:1], 1.0, 0.0)


def first_pair(pairs):
    return (lax.axis_index(CHIP) * lax.axis_size(CORE) + lax.axis_index(CORE)) * pairs


def turn(values):
    rows = values.shape[0]
    real = iota(values.shape, 0) % 2 == 0
    return jnp.where(real, -pltpu.roll(values, rows - 1, 0), pltpu.roll(values, 1, 0))


def synth_kernel(
    m_hbm, order_hbm, colat_hbm, t_hbm, w_hbm, l_hbm, near_ref, far_ref, lr_ref, ltail_ref,
    m_ref, order_ref, colat_ref, t_ref, w_ref, last_ref, c_ref, s_ref, deg_ref, eps_ref, up_ref, end_ref, lasts_ref, sems, *l_refs,
):
    pairs, sims = t_ref.shape[0], t_ref.shape[1]
    modes = t_ref.shape[3] - 1
    lines = 2 * sims
    steps = len(l_refs)
    chunk = modes // steps
    first = first_pair(pairs)
    wide = near_ref.shape[1] * near_ref.shape[2] // pairs
    cycles = last_ref.shape[2]

    pieces = [(m_hbm, m_ref), (order_hbm, order_ref), (colat_hbm, colat_ref), (w_hbm, w_ref), (t_hbm, t_ref)]
    pieces.append((l_hbm.at[pl.ds(modes, 1)], last_ref))
    pieces += [(l_hbm.at[pl.ds(j * chunk, chunk)], l_refs[j]) for j in range(steps)]
    copies = [pltpu.make_async_copy(*piece, sems.at[i]) for i, piece in enumerate(pieces)]
    for copy in copies:
        copy.start()
    for copy in copies[:3]:
        copy.wait()

    small = small_column(m_ref, first, pairs)
    (degree, _, eps), (_, _, last_eps) = layout_rows(small, modes)
    deg_ref[...] = degree * (1.0 / modes)
    eps_ref[...] = eps * (1.0 / modes)
    last_eps = last_eps * (1.0 / modes)
    theta = colat_ref[...]
    cos, inv_sin = jnp.cos(theta), 1.0 / jnp.sin(theta)
    cycle_of_slot = slot_of_cycle(order_ref).T.astype(BF16)
    up_ref[...] = jnp.where(iota((pairs, modes), 1) >= modes - small, 1.0, 0.0)
    ends = iota((lines, modes), 1) == modes - 1

    copies[3].wait()
    copies[4].wait()
    def coefficients(p, _):
        tbar = t_ref[p].reshape(lines, modes + 1)
        wiener = w_ref[p].reshape(lines, modes + 1)
        main, last = wiener[:, :modes].astype(F32), wiener[:, modes:].astype(F32)
        raised = pltpu.roll(eps_ref[pl.ds(p, 1), :] * main, modes - 1, 1)
        raised = jnp.where(ends, end_ref[pl.ds(p, 1), :][:, :1] * last, raised)
        raised = jnp.concatenate([deg_ref[pl.ds(p, 1), :] * main, raised], axis=0).astype(BF16)
        upper = jnp.broadcast_to(up_ref[pl.ds(p, 1), :], (2 * lines, modes)).astype(BF16)
        for i, sets in enumerate((jnp.concatenate([tbar[:, :modes], wiener[:, :modes]], axis=0), raised)):
            c_ref[p, 2 * i * lines : 2 * (i + 1) * lines, :] = sets
            c_ref[p, 2 * (i + 2) * lines : 2 * (i + 3) * lines, :] = sets * upper
        lasts = jnp.concatenate(
            [tbar[:, modes:].astype(F32), last, ((modes - 1.0) / modes) * last, 0.0 * last], axis=0
        )
        lasts_ref[p] = jnp.broadcast_to(lasts.astype(BF16).astype(F32), lasts_ref.shape[1:])
        return 0

    end_ref[...] = jnp.broadcast_to(last_eps, end_ref.shape)
    lax.fori_loop(0, pairs, coefficients, 0)

    copies[5].wait()
    tail_rows = last_ref[0].astype(F32)
    ltail_ref[...] = tail_rows
    for j in range(steps + 1):
        if j < steps:
            copies[6 + j].wait()
            lr_ref[:, j * chunk : (j + 1) * chunk, :] = jnp.swapaxes(l_refs[j][...], 0, 1)
        if j == 0:
            continue
        at = slice((j - 1) * chunk, j * chunk)
        for p in range(0, pairs, 2):
            both = jnp.concatenate([c_ref[p, :, at], c_ref[p + 1, :, at]], axis=0)
            sums = dot(both, jnp.concatenate([lr_ref[p, at, :], lr_ref[p + 1, at, :]], axis=1))
            for i in range(2):
                part = sums[i * 8 * lines : (i + 1) * 8 * lines, i * cycles : (i + 1) * cycles]
                s_ref[p + i] = part if j == 1 else s_ref[p + i] + part

    blocks = []
    for p in range(pairs):
        small = m_ref[first + p]
        for half, order in enumerate((small, modes - 1 - small)):
            above = s_ref[p, 4 * lines :, :]
            sums = above + lasts_ref[p] * tail_rows[p : p + 1, :] if half else s_ref[p, : 4 * lines, :] - above
            s0, s1, s2, s3 = (sums[q * lines : (q + 1) * lines] for q in range(4))
            weight = jnp.where(order == 0, 1.0, 2.0) * modes ** (-0.5)
            ratio = order.astype(F32) * (1.0 / modes)
            blocks.append(s0 * weight)
            blocks.append((cos * s2 - s3) * inv_sin * weight)
            blocks.append(turn(s1) * ratio * inv_sin * weight)
        row = iota((wide - 6 * lines, s_ref.shape[2]), 0)
        low, high = (small % FOLD).astype(F32), (small // FOLD).astype(F32)
        blocks.append(jnp.where(row == 0, low, jnp.where(row == 1, high, 0.0)))
    fourier = jnp.concatenate(blocks, axis=0).astype(BF16)
    out = dot(cycle_of_slot, fourier, NT).astype(BF16)
    near_ref[...] = out[: cycles // 2].reshape(near_ref.shape)
    far_ref[...] = out[cycles // 2 :].reshape(far_ref.shape)


def synth(tbar_alm, twf_alm, table, m_slots, cycle_order, colatitude):
    pairs, sims, _, rows = tbar_alm.shape
    modes = rows - 1
    cycles = table.shape[2]
    lines = 2 * sims
    wide = 8 * lines
    steps = 4
    vmem = pl.BlockSpec(memory_space=pltpu.VMEM)
    hbm = pl.BlockSpec(memory_space=pltpu.HBM)
    return pl.pallas_call(
        synth_kernel,
        in_specs=[hbm] * 6,
        out_specs=[vmem] * 4,
        out_shape=[
            pltpu.VMEM((cycles // 2, pairs * wide // LANES, LANES), BF16),
            pltpu.VMEM((cycles // 2, pairs * wide // LANES, LANES), BF16),
            pltpu.VMEM((pairs, modes, cycles), BF16),
            pltpu.VMEM((pairs, cycles), F32),
        ],
        scratch_shapes=[
            pltpu.SMEM(m_slots.shape, jnp.int32),
            pltpu.VMEM((1, cycles), jnp.int32),
            pltpu.VMEM((1, cycles), F32),
            pltpu.VMEM(tbar_alm.shape, BF16),
            pltpu.VMEM(twf_alm.shape, BF16),
            pltpu.VMEM((1, pairs, cycles), BF16),
            pltpu.VMEM((pairs, 8 * lines, modes), BF16),
            pltpu.VMEM((pairs, 8 * lines, cycles), F32),
            pltpu.VMEM((pairs, modes), F32),
            pltpu.VMEM((pairs, modes), F32),
            pltpu.VMEM((pairs, modes), F32),
            pltpu.VMEM((pairs, LANES), F32),
            pltpu.VMEM((pairs, 4 * lines, cycles), F32),
            pltpu.SemaphoreType.DMA((steps + 6,)),
        ]
        + [pltpu.VMEM((modes // steps, pairs, cycles), BF16)] * steps,
        compiler_params=pltpu.CompilerParams(vmem_limit_bytes=GRANT),
        name="synth",
    )(*(pltpu.with_memory_space_constraint(x, pltpu.HBM) for x in (
        m_slots, cycle_order.reshape(1, -1), colatitude.reshape(1, -1), tbar_alm, twf_alm, table
    )))


def angles(left, right, period):
    return 2.0 * np.pi * (np.outer(left, right) % period) / period


def split(table):
    high = table.astype(np.float32).astype(jnp.bfloat16)
    return high, (table - high.astype(np.float64)).astype(np.float32).astype(jnp.bfloat16)


def sky_tables(modes, pixels):
    m1, j2, m2 = np.arange(FOLD), np.arange(FOLD), np.arange(modes // FOLD)
    j1 = np.arange(pixels // FOLD).reshape(-1, 2).T.reshape(-1)
    th = angles(j2, m2, FOLD).reshape(FOLD, 2, -1)
    c, s = np.cos(th), np.sin(th)
    first = np.stack([np.stack([c, -s], 2), np.stack([s, c], 2)], 0).reshape(2 * FOLD, -1)
    th = angles(j2, m1, pixels)
    twist = np.stack([np.tile(np.cos(th), (1, 2)), np.tile(np.sin(th), (1, 2))])
    th = angles(m1, j1, FOLD)
    two = np.eye(2)
    second = np.concatenate([np.kron(two, np.cos(th)), np.kron(two, -np.sin(th))], 0)
    third = np.concatenate([np.kron(two, np.cos(th.T)), np.kron(two, -np.sin(th.T))], 1)
    th = angles(m2, j2, FOLD).reshape(2, -1, FOLD)
    c, s = np.cos(th), np.sin(th)
    fourth = np.stack([np.concatenate([c, s], 2), np.concatenate([-s, c], 2)], 1)
    fourth = fourth.reshape(2 * modes // FOLD, -1)
    return (
        np.concatenate(split(first), 1), twist.astype(np.float32), np.concatenate(split(second), 0),
        np.concatenate(split(third), 0), np.concatenate(split(fourth), 1),
    )


def near_then_far(ref):
    chips, parts, lanes = ref.shape
    halves = (ref[:, : parts // 2], ref[:, parts // 2 :])
    return jnp.concatenate([h.reshape(chips, parts // 2 * lanes) for h in halves], axis=0)


def sky_kernel(
    pairs, sims, x_ref, mask_ref, first_ref, twist_ref, second_ref, third_ref, fourth_ref, near_ref, far_ref,
    xt_ref, lhs_ref, hot_ref,
):
    devices = 2 * x_ref.shape[0]
    width = x_ref.shape[1] * x_ref.shape[2] // 2
    wide = width // pairs
    lines = 2 * sims
    half_sims = sims // 2
    fold2 = 2 * FOLD
    tall = fourth_ref.shape[0] // 4
    xt_ref[...] = near_then_far(x_ref).astype(F32).T
    groups = [(q, a) for q in range(3) for a in range(half_sims)]

    def key(p, half):
        low = xt_ref[p * wide + 6 * lines : p * wide + 6 * lines + 1, :].astype(jnp.int32)
        high = xt_ref[p * wide + 6 * lines + 1 : p * wide + 6 * lines + 2, :].astype(jnp.int32)
        return (FOLD - 1 - low, tall - 1 - high) if half else (low, high)

    sorted_halves, places = [], []
    for half in range(2):
        place = []
        for p in range(pairs):
            low, high = key(p, half)
            place.append(iota((tall, devices), 0) == high)
            for e in range(2):
                at = (e * pairs + p) * devices
                hot_ref[half, :, at : at + devices] = jnp.where(
                    iota((fold2, devices), 0) == low + e * FOLD, 1.0, 0.0
                ).astype(BF16)
                parts = []
                for q, a in groups:
                    for c in range(2):
                        row = p * wide + (half * 3 + q) * lines + (e * half_sims + a) * 2 + c
                        parts.append(jnp.where(place[p], xt_ref[row : row + 1, :], 0.0))
                lhs_ref[:, at : at + devices] = jnp.concatenate(parts, axis=0).astype(BF16)
        places.append(place)
        sorted_halves.append(dot(lhs_ref[...], hot_ref[half], NT).astype(BF16))

    n = 2 * tall
    spread = jnp.concatenate(
        [
            jnp.concatenate([s[g * n : (g + 1) * n] for s in sorted_halves], axis=0)
            for g in range(len(groups))
        ],
        axis=1,
    )
    stage = dot(first_ref[...], jnp.concatenate([spread, spread], axis=0))
    cos, sin = twist_ref[0], twist_ref[1]
    twisted = []
    for g in range(len(groups)):
        re, im = (stage[i * FOLD : (i + 1) * FOLD, g * fold2 : (g + 1) * fold2] for i in range(2))
        twisted.append(jnp.concatenate([re * cos - im * sin, re * sin + im * cos], axis=1))
    twisted = jnp.concatenate(twisted, axis=0).astype(BF16)
    maps = dot(twisted, second_ref[: 2 * fold2]) + dot(twisted, second_ref[2 * fold2 :])

    mask = mask_ref[...].astype(F32).T
    mask = jnp.concatenate([mask[:FOLD], mask[FOLD:]] * 2, axis=1)
    products = []
    for q in range(1, 3):
        for a in range(half_sims):
            one = maps[a * FOLD : (a + 1) * FOLD]
            at = (q * half_sims + a) * FOLD
            products.append(mask * one * maps[at : at + FOLD])
    products = jnp.concatenate(products, axis=0).astype(BF16)
    stage = dot(products, third_ref[:fold2]) + dot(products, third_ref[fold2:])
    twisted = []
    for g in range(2 * half_sims):
        re, im = (stage[g * FOLD : (g + 1) * FOLD, i * fold2 : (i + 1) * fold2] for i in range(2))
        twisted.append(jnp.concatenate([re * cos + im * sin, im * cos - re * sin], axis=0))
    twisted = jnp.concatenate(twisted, axis=1).astype(BF16)
    pixels = mask_ref.shape[0] * mask_ref.shape[1]
    spectra = dot(fourth_ref[...], jnp.concatenate([twisted, twisted], axis=0)) * pixels ** (-0.5)
    spectra = spectra.astype(BF16)

    groups = 2 * half_sims
    add = jnp.where(
        iota((2 * groups, 2 * groups * tall), 1) // tall == iota((2 * groups, 2 * groups * tall), 0), 1.0, 0.0
    ).astype(BF16)
    found = []
    for half in range(2):
        rows = jnp.concatenate(
            [spectra[half * n : (half + 1) * n, g * fold2 : (g + 1) * fold2] for g in range(groups)], axis=0
        )
        for e in range(2):
            for p in range(pairs):
                at = (e * pairs + p) * devices
                values = dot(rows, hot_ref[half, :, at : at + devices])
                keep = jnp.concatenate([places[half][p]] * (2 * groups), axis=0)
                lhs_ref[: values.shape[0], at : at + devices] = jnp.where(keep, values, 0.0).astype(BF16)
        found.append(dot(add, lhs_ref[: 2 * groups * tall, :]))
    blocks = []
    upper = iota((lines, devices), 0) >= lines // 2
    for p in range(pairs):
        for half in range(2):
            a, b = (
                found[half][:, (e * pairs + p) * devices : (e * pairs + p + 1) * devices] for e in range(2)
            )
            blocks.append(jnp.where(upper, pltpu.roll(b, lines // 2, 0), a))
            blocks.append(jnp.where(upper, b, pltpu.roll(a, lines // 2, 0)))
    out = jnp.concatenate(blocks, axis=0).T.astype(BF16)
    near_ref[...] = out[: devices // 2].reshape(near_ref.shape)
    far_ref[...] = out[devices // 2 :].reshape(far_ref.shape)


def sky(received, pixel_mask, pairs, sims, modes):
    devices = 2 * received.shape[0]
    pixels = pixel_mask.shape[1]
    tables = sky_tables(modes, pixels)
    vmem = pl.BlockSpec(memory_space=pltpu.VMEM)
    tall = modes // FOLD // 2
    return pl.pallas_call(
        functools.partial(sky_kernel, pairs, sims),
        in_specs=[vmem] * 7,
        out_specs=[vmem] * 2,
        out_shape=[pltpu.VMEM((devices // 2, pairs * 8 * sims // LANES, LANES), BF16)] * 2,
        scratch_shapes=[
            pltpu.VMEM((received.shape[1] // 2 * LANES, devices), F32),
            pltpu.VMEM((3 * sims * tall, 2 * pairs * devices), BF16),
            pltpu.VMEM((2, 2 * FOLD, 2 * pairs * devices), BF16),
        ],
        compiler_params=pltpu.CompilerParams(vmem_limit_bytes=GRANT),
        name="sky",
    )(received, pixel_mask.reshape(-1, 2 * FOLD), *(jnp.asarray(t) for t in tables))


def analyse_kernel(
    m_ref, order_ref, colat_ref, weight_ref, r_ref, l_ref, tail_ref, grad_hbm, curl_hbm,
    w_ref, deg_ref, eps_ref, ord_ref, grad_ref, curl_ref, sems,
):
    pairs, modes, cycles = l_ref.shape
    lines = w_ref.shape[1] // 16
    sims = lines // 2
    first = first_pair(pairs)
    factor = (modes / cycles) ** 0.5

    def scale_of(degree):
        return factor / jnp.sqrt(jnp.maximum(degree * (degree + 1.0), 1.0))

    small = small_column(m_ref, first, pairs)
    (degree, orders, eps), (last_degree, last_orders, last_eps) = layout_rows(small, modes)
    scale = scale_of(degree)
    deg_ref[...] = degree * scale
    eps_ref[...] = eps * scale
    ord_ref[...] = orders * scale
    scale = scale_of(last_degree)
    last_degree, last_orders, last_eps = last_degree * scale, last_orders * scale, last_eps * scale

    spectra = dot(near_then_far(r_ref).astype(F32).T.astype(BF16), slot_of_cycle(order_ref).astype(BF16), NT)
    theta, weight = colat_ref[...], weight_ref[...]
    with_cos = weight * jnp.cos(theta) / jnp.sin(theta)
    with_sin = weight / jnp.sin(theta)
    blank = jnp.zeros((4 * lines, cycles), F32)
    for i in range(pairs):
        for half in range(2):
            parts = []
            for q in range(2):
                at = ((i * 2 + half) * 2 + q) * lines
                values = spectra[at : at + lines]
                parts += [values * with_cos, values * with_sin]
            parts = jnp.concatenate(parts, axis=0)
            at = ((i % 2) * 2 + half) * 4 * lines
            w_ref[i // 2, at : at + 4 * lines] = jnp.concatenate(
                [blank, parts] if i % 2 else [parts, blank], axis=1
            ).astype(BF16)

    k = iota((lines, modes), 1)
    starts = k == 0

    def previous(values):
        return jnp.where(starts, 0.0, pltpu.roll(values, 1, 1))

    copies = []
    for p in range(pairs):
        odd = p % 2
        weighted = w_ref[p // 2, odd * 8 * lines : (odd + 1) * 8 * lines, odd * cycles : (odd + 1) * cycles]
        if not odd:
            tables = jnp.concatenate([l_ref[p], l_ref[p + 1]], axis=1)
            both = dot(w_ref[p // 2], tables, NT)
        sums = both[odd * 8 * lines : (odd + 1) * 8 * lines]
        upper = k >= modes - m_ref[first + p]
        a0, a1, a2, a3 = (
            jnp.where(upper, sums[(4 + q) * lines : (5 + q) * lines], sums[q * lines : (q + 1) * lines])
            for q in range(4)
        )
        level, raised, azimuth = (ref[p : p + 1, :] for ref in (deg_ref, eps_ref, ord_ref))
        grad = level * a0 - raised * previous(a1) - azimuth * turn(a3)
        curl = level * a2 - raised * previous(a3) + azimuth * turn(a1)
        last = jnp.sum(weighted[4 * lines :].astype(F32) * tail_ref[p : p + 1, :], axis=1, keepdims=True)
        level, raised, azimuth = (v[p : p + 1, :] for v in (last_degree, last_eps, last_orders))
        b0, b1, b2, b3 = (last[q * lines : (q + 1) * lines] for q in range(4))
        last_grad = level * b0 - raised * a1[:, modes - 1 :] - azimuth * turn(b3)
        last_curl = level * b2 - raised * a3[:, modes - 1 :] + azimuth * turn(b1)
        for ref, hbm, main, last in ((grad_ref, grad_hbm, grad, last_grad), (curl_ref, curl_hbm, curl, last_curl)):
            ref[p, :, :, :modes] = main.reshape(sims, 2, modes)
            ref[p, :, :, modes:] = last.reshape(sims, 2, 1)
            copies.append(pltpu.make_async_copy(ref.at[p], hbm.at[p], sems.at[len(copies)]))
            copies[-1].start()
    for copy in copies:
        copy.wait()


def analyse(returned, table, tail, m_slots, cycle_order, colatitude, cycle_weight, sims):
    pairs, modes, cycles = table.shape
    vmem = pl.BlockSpec(memory_space=pltpu.VMEM)
    hbm = pl.BlockSpec(memory_space=pltpu.HBM)
    shape = (pairs, sims, 2, modes + 1)
    out = jax.ShapeDtypeStruct(shape, F32)
    return pl.pallas_call(
        analyse_kernel,
        in_specs=[pl.BlockSpec(memory_space=pltpu.SMEM)] + [vmem] * 6,
        out_specs=[hbm, hbm],
        out_shape=[out, out],
        scratch_shapes=[
            pltpu.VMEM((pairs // 2, 32 * sims, 2 * cycles), BF16),
            pltpu.VMEM((pairs, modes), F32),
            pltpu.VMEM((pairs, modes), F32),
            pltpu.VMEM((pairs, modes), F32),
            pltpu.VMEM(shape, F32),
            pltpu.VMEM(shape, F32),
            pltpu.SemaphoreType.DMA((2 * pairs,)),
        ],
        compiler_params=pltpu.CompilerParams(vmem_limit_bytes=GRANT),
        name="analyse",
    )(m_slots, cycle_order.reshape(1, -1), colatitude.reshape(1, -1), cycle_weight.reshape(1, -1), returned, table, tail)


def merge_kernel(near_ref, far_ref, out_ref):
    parts = near_ref.shape[1]
    out_ref[:, :parts] = near_ref[...]
    out_ref[:, parts:] = far_ref[...]


def exchange(near, far):
    vmem = pl.BlockSpec(memory_space=pltpu.VMEM)
    swapped = lax.ppermute(far, CORE, [(0, 1), (1, 0)])
    chips, parts, lanes = near.shape
    both = pl.pallas_call(
        merge_kernel,
        in_specs=[vmem] * 2,
        out_specs=vmem,
        out_shape=pltpu.VMEM((chips, 2 * parts, lanes), near.dtype),
        compiler_params=pltpu.CompilerParams(vmem_limit_bytes=GRANT),
        name="merge",
    )(near, swapped)
    return lax.all_to_all(both, CHIP, 0, 0, tiled=True)


def shards(tbar_alm, twf_alm, legendre, m_slots, cycle_order, colatitude, cycle_weight, pixel_mask):
    pairs, sims, _, rows = tbar_alm.shape
    by_row = jnp.transpose(legendre, (1, 0, 2))
    near, far, table, tail = synth(tbar_alm, twf_alm, by_row, m_slots, cycle_order, colatitude)
    near, far = sky(exchange(near, far), pixel_mask, pairs, sims, rows - 1)
    returned = exchange(near, far)
    return analyse(returned, table, tail, m_slots, cycle_order, colatitude, cycle_weight, sims)


def solution(mesh):
    devices = mesh.devices.reshape(mesh.shape["grp"], -1, 2)
    finer = Mesh(devices, ("grp", CHIP, CORE))
    ma = (CHIP, CORE)
    coefficients = P(ma, "grp", None, None)
    return jax.shard_map(
        shards,
        mesh=finer,
        in_specs=(coefficients, coefficients, P(ma, None, None), P(), P(), P(), P(), P(ma, None)),
        out_specs=(coefficients, coefficients),
        check_vma=False,
    )
```

```python
import functools
import math

import jax
import jax.numpy as jnp
import numpy as np
from jax import lax
from jax.experimental import pallas as pl
from jax.experimental.pallas import tpu as pltpu
from jax.sharding import Mesh
from jax.sharding import PartitionSpec as P

F32 = jnp.float32
BF16 = jnp.bfloat16
LANES = 128
GRANT = 24 * 2**20
CHIP, CORE = "chip", "core"
NT = (((1,), (1,)), ((), ()))
NN = (((1,), (0,)), ((), ()))


def dot(a, b, dims=NN):
    return lax.dot_general(a, b, dims, preferred_element_type=F32)


def iota(shape, dim):
    return lax.broadcasted_iota(jnp.int32, shape, dim)


def small_column(m_ref, first, pairs):
    row = iota((pairs, 1), 0)
    column = jnp.zeros((pairs, 1), jnp.int32)
    for p in range(pairs):
        column = jnp.where(row == p, m_ref[first + p], column)
    return column


def layout_rows(small, modes):
    k = iota((small.shape[0], modes), 1)
    upper = k >= modes - small
    degree = jnp.where(upper, k - 1, small + k).astype(F32)
    orders = jnp.where(upper, modes - 1 - small, small).astype(F32)
    last_degree = jnp.full(small.shape, modes - 1, F32)
    last_orders = (modes - 1 - small).astype(F32)
    return (
        (degree, orders, raising(degree, orders)),
        (last_degree, last_orders, raising(last_degree, last_orders)),
    )


def raising(degree, orders):
    square = (
        (degree * degree - orders * orders)
        * (2.0 * degree + 1.0)
        / jnp.maximum(2.0 * degree - 1.0, 1.0)
    )
    return jnp.where(degree > orders, jnp.sqrt(jnp.where(degree > orders, square, 0.0)), 0.0)


def slot_of_cycle(order_ref):
    n = order_ref.shape[1]
    core = lax.axis_index(CORE)
    place = iota((n, n), 1)
    near = place < n // 2
    slot = 2 * (place % (n // 2)) + jnp.where(near, core, 1 - core)
    pick = jnp.where(iota((n, n), 0) == slot, 1.0, 0.0).astype(BF16)
    order = jnp.broadcast_to(order_ref[...].astype(F32), (8, n)).astype(BF16)
    return jnp.where(iota((n, n), 0).astype(F32) == dot(order, pick)[:1], 1.0, 0.0)


def first_pair(pairs):
    return (lax.axis_index(CHIP) * lax.axis_size(CORE) + lax.axis_index(CORE)) * pairs


def turn(values):
    rows = values.shape[0]
    real = iota(values.shape, 0) % 2 == 0
    return jnp.where(real, -pltpu.roll(values, rows - 1, 0), pltpu.roll(values, 1, 0))


def synth_kernel(
    m_hbm, order_hbm, colat_hbm, t_hbm, w_hbm, l_hbm, near_ref, far_ref, lr_ref, ltail_ref, small_ref,
    m_ref, order_ref, colat_ref, t_ref, w_ref, last_ref, c_ref, s_ref, deg_ref, eps_ref, up_ref, end_ref, lasts_ref, sems, *l_refs,
):
    pairs, sims = t_ref.shape[0], t_ref.shape[1]
    modes = t_ref.shape[3] - 1
    lines = 2 * sims
    steps = len(l_refs)
    chunk = modes // steps
    first = first_pair(pairs)
    wide = near_ref.shape[1] * near_ref.shape[2] // pairs
    cycles = last_ref.shape[2]

    pieces = [(m_hbm, m_ref), (order_hbm, order_ref), (colat_hbm, colat_ref), (w_hbm, w_ref), (t_hbm, t_ref)]
    pieces.append((l_hbm.at[pl.ds(modes, 1)], last_ref))
    pieces += [(l_hbm.at[pl.ds(j * chunk, chunk)], l_refs[j]) for j in range(steps)]
    copies = [pltpu.make_async_copy(*piece, sems.at[i]) for i, piece in enumerate(pieces)]
    for copy in copies:
        copy.start()
    for copy in copies[:3]:
        copy.wait()

    small = small_column(m_ref, first, pairs)
    (degree, _, eps), (_, _, last_eps) = layout_rows(small, modes)
    small_ref[...] = jnp.broadcast_to(small.astype(F32), small_ref.shape)
    deg_ref[...] = degree * (1.0 / modes)
    eps_ref[...] = eps * (1.0 / modes)
    last_eps = last_eps * (1.0 / modes)
    theta = colat_ref[...]
    cos, inv_sin = jnp.cos(theta), 1.0 / jnp.sin(theta)
    cycle_of_slot = slot_of_cycle(order_ref).T.astype(BF16)
    up_ref[...] = jnp.where(iota((pairs, modes), 1) >= modes - small, 1.0, 0.0)
    ends = iota((lines, modes), 1) == modes - 1

    copies[3].wait()
    copies[4].wait()
    def coefficients(p, _):
        tbar = t_ref[p].reshape(lines, modes + 1)
        wiener = w_ref[p].reshape(lines, modes + 1)
        main, last = wiener[:, :modes].astype(F32), wiener[:, modes:].astype(F32)
        raised = pltpu.roll(eps_ref[pl.ds(p, 1), :] * main, modes - 1, 1)
        raised = jnp.where(ends, end_ref[pl.ds(p, 1), :][:, :1] * last, raised)
        raised = jnp.concatenate([deg_ref[pl.ds(p, 1), :] * main, raised], axis=0).astype(BF16)
        upper = jnp.broadcast_to(up_ref[pl.ds(p, 1), :], (2 * lines, modes)).astype(BF16)
        for i, sets in enumerate((jnp.concatenate([tbar[:, :modes], wiener[:, :modes]], axis=0), raised)):
            c_ref[p, 2 * i * lines : 2 * (i + 1) * lines, :] = sets
            c_ref[p, 2 * (i + 2) * lines : 2 * (i + 3) * lines, :] = sets * upper
        lasts = jnp.concatenate(
            [tbar[:, modes:].astype(F32), last, ((modes - 1.0) / modes) * last, 0.0 * last], axis=0
        )
        lasts_ref[p] = jnp.broadcast_to(lasts.astype(BF16).astype(F32), lasts_ref.shape[1:])
        return 0

    end_ref[...] = jnp.broadcast_to(last_eps, end_ref.shape)
    lax.fori_loop(0, pairs, coefficients, 0, unroll=2)

    copies[5].wait()
    tail_rows = last_ref[0].astype(F32)
    ltail_ref[...] = tail_rows
    for j in range(steps + 1):
        if j < steps:
            copies[6 + j].wait()
            lr_ref[:, j * chunk : (j + 1) * chunk, :] = jnp.swapaxes(l_refs[j][...], 0, 1)
        if j == 0:
            continue
        at = slice((j - 1) * chunk, j * chunk)
        for p in range(0, pairs, 2):
            both = jnp.concatenate([c_ref[p, :, at], c_ref[p + 1, :, at]], axis=0)
            sums = dot(both, jnp.concatenate([lr_ref[p, at, :], lr_ref[p + 1, at, :]], axis=1))
            for i in range(2):
                part = sums[i * 8 * lines : (i + 1) * 8 * lines, i * cycles : (i + 1) * cycles]
                s_ref[p + i] = part if j == 1 else s_ref[p + i] + part

    blocks = []
    for p in range(pairs):
        small = m_ref[first + p]
        for half, order in enumerate((small, modes - 1 - small)):
            above = s_ref[p, 4 * lines :, :]
            sums = above + lasts_ref[p] * tail_rows[p : p + 1, :] if half else s_ref[p, : 4 * lines, :] - above
            s0, s1, s2, s3 = (sums[q * lines : (q + 1) * lines] for q in range(4))
            weight = jnp.where(order == 0, 1.0, 2.0) * modes ** (-0.5)
            ratio = order.astype(F32) * (1.0 / modes)
            blocks.append(s0 * weight)
            blocks.append((cos * s2 - s3) * inv_sin * weight)
            blocks.append(turn(s1) * ratio * inv_sin * weight)
        row = iota((wide - 6 * lines, s_ref.shape[2]), 0)
        low, high = (small % LANES).astype(F32), (small // LANES).astype(F32)
        blocks.append(jnp.where(row == 0, low, jnp.where(row == 1, high, 0.0)))
    fourier = jnp.concatenate(blocks, axis=0).astype(BF16)
    out = dot(cycle_of_slot, fourier, NT).astype(BF16)
    near_ref[...] = out[: cycles // 2].reshape(near_ref.shape)
    far_ref[...] = out[cycles // 2 :].reshape(far_ref.shape)


def synth(tbar_alm, twf_alm, table, m_slots, cycle_order, colatitude):
    pairs, sims, _, rows = tbar_alm.shape
    modes = rows - 1
    cycles = table.shape[2]
    lines = 2 * sims
    wide = 8 * lines
    steps = 4
    vmem = pl.BlockSpec(memory_space=pltpu.VMEM)
    hbm = pl.BlockSpec(memory_space=pltpu.HBM)
    return pl.pallas_call(
        synth_kernel,
        in_specs=[hbm] * 6,
        out_specs=[vmem] * 5,
        out_shape=[
            pltpu.VMEM((cycles // 2, pairs * wide // LANES, LANES), BF16),
            pltpu.VMEM((cycles // 2, pairs * wide // LANES, LANES), BF16),
            pltpu.VMEM((pairs, modes, cycles), BF16),
            pltpu.VMEM((pairs, cycles), F32),
            pltpu.VMEM((pairs, LANES), F32),
        ],
        scratch_shapes=[
            pltpu.SMEM(m_slots.shape, jnp.int32),
            pltpu.VMEM((1, cycles), jnp.int32),
            pltpu.VMEM((1, cycles), F32),
            pltpu.VMEM(tbar_alm.shape, BF16),
            pltpu.VMEM(twf_alm.shape, BF16),
            pltpu.VMEM((1, pairs, cycles), BF16),
            pltpu.VMEM((pairs, 8 * lines, modes), BF16),
            pltpu.VMEM((pairs, 8 * lines, cycles), F32),
            pltpu.VMEM((pairs, modes), F32),
            pltpu.VMEM((pairs, modes), F32),
            pltpu.VMEM((pairs, modes), F32),
            pltpu.VMEM((pairs, LANES), F32),
            pltpu.VMEM((pairs, 4 * lines, cycles), F32),
            pltpu.SemaphoreType.DMA((steps + 6,)),
        ]
        + [pltpu.VMEM((modes // steps, pairs, cycles), BF16)] * steps,
        compiler_params=pltpu.CompilerParams(vmem_limit_bytes=GRANT),
        name="synth",
    )(*(pltpu.with_memory_space_constraint(x, pltpu.HBM) for x in (
        m_slots, cycle_order.reshape(1, -1), colatitude.reshape(1, -1), tbar_alm, twf_alm, table
    )))


def angles(left, right, period):
    return 2.0 * np.pi * (np.outer(left, right) % period) / period


def split(table):
    high = table.astype(np.float32).astype(jnp.bfloat16)
    return high, (table - high.astype(np.float64)).astype(np.float32).astype(jnp.bfloat16)


def sky_tables(modes, pixels):
    small = pixels // LANES
    m1, j2, m2 = np.arange(LANES), np.arange(small), np.arange(modes // LANES)
    j1 = np.arange(LANES).reshape(-1, LANES // small).T.reshape(-1)
    th = angles(j2, m2, small).reshape(small, 2, -1)
    c, s = np.cos(th), np.sin(th)
    first = np.stack([np.stack([c, -s], 2), np.stack([s, c], 2)], 0).reshape(2 * small, -1)
    th = angles(j2, m1, pixels)
    twist = np.stack([np.cos(th), np.sin(th)])
    th = angles(m1, j1, LANES)
    second = np.concatenate([np.cos(th), -np.sin(th)], 0)
    third = np.concatenate([np.cos(th.T), -np.sin(th.T)], 1)
    th = angles(m2, j2, small).reshape(2, -1, small)
    c, s = np.cos(th), np.sin(th)
    fourth = np.stack([np.concatenate([c, s], 2), np.concatenate([-s, c], 2)], 1)
    fourth = fourth.reshape(2 * modes // LANES, -1)
    return (
        np.concatenate(split(first), 1), twist.astype(np.float32), np.concatenate(split(second), 0),
        np.concatenate(split(third), 0), np.concatenate(split(fourth), 1),
    )


def near_then_far(ref):
    chips, parts, lanes = ref.shape
    halves = (ref[:, : parts // 2], ref[:, parts // 2 :])
    return jnp.concatenate([h.reshape(chips, parts // 2 * lanes) for h in halves], axis=0)


def sky_kernel(
    pairs, sims, x_ref, mask_ref, first_ref, twist_ref, second_ref, third_ref, fourth_ref, near_ref, far_ref,
    xt_ref, lhs_ref, hot_ref,
):
    devices = 2 * x_ref.shape[0]
    wide = x_ref.shape[1] * x_ref.shape[2] // 2 // pairs
    lines = 2 * sims
    small = twist_ref.shape[1]
    pixels = small * LANES
    tall = fourth_ref.shape[0] // 4
    xt_ref[...] = near_then_far(x_ref).astype(F32).T

    n = 2 * tall
    groups = 3 * sims
    sorted_halves, places = [], []
    for half in range(2):
        place = []
        for p in range(pairs):
            at = p * wide + 6 * lines
            low, high = (xt_ref[at + i : at + i + 1, :].astype(jnp.int32) for i in range(2))
            if half:
                low, high = LANES - 1 - low, tall - 1 - high
            place.append(iota((tall, devices), 0) == high)
            tile = slice(p * devices, (p + 1) * devices)
            hot_ref[half, :, tile] = jnp.where(iota((LANES, devices), 0) == low, 1.0, 0.0).astype(BF16)
            parts = []
            for row in range(3 * lines):
                at = p * wide + half * 3 * lines + row
                parts.append(jnp.where(place[p], xt_ref[at : at + 1, :], 0.0))
            lhs_ref[:, tile] = jnp.concatenate(parts, axis=0).astype(BF16)
        places.append(place)
        sorted_halves.append(dot(lhs_ref[...], hot_ref[half], NT).astype(BF16))

    spread = jnp.concatenate(
        [
            jnp.concatenate([s[g * n : (g + 1) * n] for s in sorted_halves], axis=0)
            for g in range(groups)
        ],
        axis=1,
    )
    stage = dot(first_ref[...], jnp.concatenate([spread, spread], axis=0))
    cos, sin = twist_ref[0], twist_ref[1]
    twisted = []
    for g in range(groups):
        re, im = (stage[i * small : (i + 1) * small, g * LANES : (g + 1) * LANES] for i in range(2))
        twisted.append(jnp.concatenate([re * cos - im * sin, re * sin + im * cos], axis=1))
    twisted = jnp.concatenate(twisted, axis=0).astype(BF16)
    maps = dot(twisted, second_ref[: 2 * LANES]) + dot(twisted, second_ref[2 * LANES :])

    mask = mask_ref[...].astype(F32).T
    mask = jnp.concatenate([mask[i * small : (i + 1) * small] for i in range(LANES // small)], axis=1)
    products = []
    for q in range(1, 3):
        for s in range(sims):
            at = (q * sims + s) * small
            products.append(mask * maps[s * small : (s + 1) * small] * maps[at : at + small])
    products = jnp.concatenate(products, axis=0).astype(BF16)
    stage = dot(products, third_ref[:LANES]) + dot(products, third_ref[LANES:])
    groups = 2 * sims
    twisted = []
    for g in range(groups):
        re, im = (stage[g * small : (g + 1) * small, i * LANES : (i + 1) * LANES] for i in range(2))
        twisted.append(jnp.concatenate([re * cos + im * sin, im * cos - re * sin], axis=0))
    twisted = jnp.concatenate(twisted, axis=1).astype(BF16)
    spectra = dot(fourth_ref[...], jnp.concatenate([twisted, twisted], axis=0)) * pixels ** (-0.5)
    spectra = spectra.astype(BF16)

    rows, columns = 2 * groups, 2 * groups * tall
    add = jnp.where(iota((rows, columns), 1) // tall == iota((rows, columns), 0), 1.0, 0.0).astype(BF16)
    found = []
    for half in range(2):
        stacked = jnp.concatenate(
            [spectra[half * n : (half + 1) * n, g * LANES : (g + 1) * LANES] for g in range(groups)], axis=0
        )
        values = dot(stacked, hot_ref[half])
        for p in range(pairs):
            tile = slice(p * devices, (p + 1) * devices)
            keep = jnp.concatenate([places[half][p]] * rows, axis=0)
            lhs_ref[:columns, tile] = jnp.where(keep, values[:, tile], 0.0).astype(BF16)
        found.append(dot(add, lhs_ref[:columns, :]))
    blocks = [found[half][:, p * devices : (p + 1) * devices] for p in range(pairs) for half in range(2)]
    out = jnp.concatenate(blocks, axis=0).T.astype(BF16)
    near_ref[...] = out[: devices // 2].reshape(near_ref.shape)
    far_ref[...] = out[devices // 2 :].reshape(far_ref.shape)


def sky(received, pixel_mask, pairs, sims, modes):
    devices = 2 * received.shape[0]
    pixels = pixel_mask.shape[1]
    tables = sky_tables(modes, pixels)
    vmem = pl.BlockSpec(memory_space=pltpu.VMEM)
    tall = modes // LANES // 2
    return pl.pallas_call(
        functools.partial(sky_kernel, pairs, sims),
        in_specs=[vmem] * 7,
        out_specs=[vmem] * 2,
        out_shape=[pltpu.VMEM((devices // 2, pairs * 8 * sims // LANES, LANES), BF16)] * 2,
        scratch_shapes=[
            pltpu.VMEM((received.shape[1] // 2 * LANES, devices), F32),
            pltpu.VMEM((6 * sims * tall, pairs * devices), BF16),
            pltpu.VMEM((2, LANES, pairs * devices), BF16),
        ],
        compiler_params=pltpu.CompilerParams(vmem_limit_bytes=GRANT),
        name="sky",
    )(received, pixel_mask.reshape(-1, LANES), *(jnp.asarray(t) for t in tables))


def rows_kernel(
    small_ref, order_ref, colat_ref, weight_ref, table_ref, _, row_ref, end_ref, hot_ref, with_ref, flip_ref
):
    pairs, modes, cycles = row_ref.shape[1], row_ref.shape[3], end_ref.shape[2]
    small = small_ref[:, :1].astype(jnp.int32)
    main, last = layout_rows(small, modes)
    for i, ref in enumerate((row_ref, end_ref)):
        degree, orders, eps = (main, last)[i]
        scale = (modes / cycles) ** 0.5 / jnp.sqrt(jnp.maximum(degree * (degree + 1.0), 1.0))
        for j, values in enumerate((degree * scale, eps * scale, orders * scale)):
            if i:
                ref[j] = jnp.broadcast_to(values, ref.shape[1:])
            else:
                for p in range(pairs):
                    ref[j, p] = jnp.broadcast_to(values[p : p + 1], ref.shape[2:])
    late = flip_ref.shape[0]
    for p in range(late):
        flip_ref[p] = table_ref[pairs - late + p].T
    hot_ref[...] = slot_of_cycle(order_ref).astype(BF16)
    theta, weight = colat_ref[...], weight_ref[...]
    with_ref[0] = jnp.broadcast_to(weight * jnp.cos(theta) / jnp.sin(theta), with_ref.shape[1:])
    with_ref[1] = jnp.broadcast_to(weight / jnp.sin(theta), with_ref.shape[1:])


def layout(small, cycle_order, colatitude, cycle_weight, table, late, after, lines, modes):
    pairs = small.shape[0]
    cycles = cycle_order.shape[0]
    vmem = pl.BlockSpec(memory_space=pltpu.VMEM)
    return pl.pallas_call(
        rows_kernel,
        in_specs=[vmem] * 6,
        out_specs=[vmem] * 5,
        out_shape=[
            pltpu.VMEM((3, pairs, lines, modes), F32), pltpu.VMEM((3, pairs, cycles), F32),
            pltpu.VMEM((cycles, cycles), BF16), pltpu.VMEM((2, lines, cycles), F32),
            pltpu.VMEM((late, cycles, modes), BF16),
        ],
        compiler_params=pltpu.CompilerParams(vmem_limit_bytes=GRANT),
        cost_estimate=pl.CostEstimate(flops=10**9, bytes_accessed=10**6, transcendentals=10**5),
        name="layout",
    )(small, cycle_order.reshape(1, -1), colatitude.reshape(1, -1), cycle_weight.reshape(1, -1), table, after)


def flip_kernel(table_ref, _, out_ref):
    for p in range(out_ref.shape[0]):
        out_ref[p] = table_ref[p].T


def flip(table, pairs, after):
    _, modes, cycles = table.shape
    vmem = pl.BlockSpec(memory_space=pltpu.VMEM)
    return pl.pallas_call(
        flip_kernel,
        in_specs=[vmem] * 2,
        out_specs=vmem,
        out_shape=pltpu.VMEM((pairs, cycles, modes), BF16),
        compiler_params=pltpu.CompilerParams(vmem_limit_bytes=GRANT),
        cost_estimate=pl.CostEstimate(flops=10**9, bytes_accessed=10**6, transcendentals=0),
        name="flip",
    )(table, after)


def analyse_kernel(
    small_ref, r_ref, l_ref, l2_ref, tail_ref, row_ref, end_ref, hot_ref, with_ref, grad_hbm, curl_hbm,
    w_ref, grad_ref, curl_ref, sems,
):
    pairs, lines, modes = row_ref.shape[1:]
    cycles = l_ref.shape[1]
    sims = lines // 2
    high = 6 * lines

    spectra = dot(near_then_far(r_ref).astype(F32).T.astype(BF16), hot_ref[...], NT)
    with_cos, with_sin = with_ref[0], with_ref[1]
    blank = jnp.zeros((high, cycles), F32)
    for i in range(pairs):
        for half in range(2):
            at = (i * 2 + half) * 2 * lines
            parts, turned = [], []
            for values in (spectra[at : at + lines], spectra[at + lines : at + 2 * lines]):
                parts += [values * with_cos, values * with_sin]
                turned.append(turn(parts[-1]))
            parts = jnp.concatenate(parts + turned, axis=0)
            at = ((i % 2) * 2 + half) * high
            w_ref[i // 2, at : at + high] = jnp.concatenate(
                [blank, parts] if i % 2 else [parts, blank], axis=1
            ).astype(BF16)

    k = iota((lines, modes), 1)
    starts = k == 0

    def previous(values):
        return jnp.where(starts, 0.0, pltpu.roll(values, 1, 1))

    copies = []
    for p in range(pairs):
        odd = p % 2
        if not odd:
            ref, at = (l_ref, p) if p < l_ref.shape[0] else (l2_ref, p - l_ref.shape[0])
            tables = jnp.concatenate([ref[at], ref[at + 1]], axis=0)
            both = dot(w_ref[p // 2], tables)
        sums = both[odd * 2 * high : (odd + 1) * 2 * high]
        upper = k >= modes - small_ref[p : p + 1, :1].astype(jnp.int32)
        a0, a1, a2, a3, t1, t3 = (
            jnp.where(upper, sums[high + q * lines : high + (q + 1) * lines], sums[q * lines : (q + 1) * lines])
            for q in range(6)
        )
        level, raised, azimuth = (row_ref[i, p] for i in range(3))
        grad = level * a0 - raised * previous(a1) - azimuth * t3
        curl = level * a2 - raised * previous(a3) + azimuth * t1
        weighted = w_ref[p // 2, (2 * odd + 1) * high : (2 * odd + 2) * high, odd * cycles : (odd + 1) * cycles]
        last = jnp.sum(weighted.astype(F32) * tail_ref[p : p + 1, :], axis=1, keepdims=True)
        level, raised, azimuth = (end_ref[i, p : p + 1, :1] for i in range(3))
        b0, b1, b2, b3, u1, u3 = (last[q * lines : (q + 1) * lines] for q in range(6))
        last_grad = level * b0 - raised * a1[:, modes - 1 :] - azimuth * u3
        last_curl = level * b2 - raised * a3[:, modes - 1 :] + azimuth * u1
        for ref, hbm, main, last in ((grad_ref, grad_hbm, grad, last_grad), (curl_ref, curl_hbm, curl, last_curl)):
            ref[p, :, :, :modes] = main.reshape(sims, 2, modes)
            ref[p, :, :, modes:] = last.reshape(sims, 2, 1)
            copies.append(pltpu.make_async_copy(ref.at[p], hbm.at[p], sems.at[len(copies)]))
            copies[-1].start()
    for copy in copies:
        copy.wait()


def analyse(returned, tables, tail, small, rows, ends, hot, weights):
    _, pairs, lines, modes = rows.shape
    cycles = hot.shape[0]
    vmem = pl.BlockSpec(memory_space=pltpu.VMEM)
    hbm = pl.BlockSpec(memory_space=pltpu.HBM)
    shape = (pairs, lines // 2, 2, modes + 1)
    out = jax.ShapeDtypeStruct(shape, F32)
    return pl.pallas_call(
        analyse_kernel,
        in_specs=[vmem] * 9,
        out_specs=[hbm, hbm],
        out_shape=[out, out],
        scratch_shapes=[
            pltpu.VMEM((pairs // 2, 24 * lines, 2 * cycles), BF16),
            pltpu.VMEM(shape, F32),
            pltpu.VMEM(shape, F32),
            pltpu.SemaphoreType.DMA((2 * pairs,)),
        ],
        compiler_params=pltpu.CompilerParams(vmem_limit_bytes=GRANT),
        name="analyse",
    )(small, returned, *tables, tail, rows, ends, hot, weights)


def merge_kernel(near_ref, far_ref, *refs):
    out_ref = refs[-1]
    parts = near_ref.shape[1]
    out_ref[:, :parts] = near_ref[...]
    out_ref[:, parts:] = far_ref[...]


def exchange(near, far, *beside):
    vmem = pl.BlockSpec(memory_space=pltpu.VMEM)
    swapped = lax.ppermute(far, CORE, [(0, 1), (1, 0)])
    chips, parts, lanes = near.shape
    both = pl.pallas_call(
        merge_kernel,
        in_specs=[vmem] * (2 + len(beside)),
        out_specs=vmem,
        out_shape=pltpu.VMEM((chips, 2 * parts, lanes), near.dtype),
        compiler_params=pltpu.CompilerParams(vmem_limit_bytes=GRANT),
        name="merge",
    )(near, swapped, *beside)
    return lax.all_to_all(both, CHIP, 0, 0, tiled=True)


def shards(tbar_alm, twf_alm, legendre, m_slots, cycle_order, colatitude, cycle_weight, pixel_mask):
    pairs, sims, _, rows = tbar_alm.shape
    by_row = jnp.transpose(legendre, (1, 0, 2))
    near, far, table, tail, small = synth(tbar_alm, twf_alm, by_row, m_slots, cycle_order, colatitude)
    early = pairs // 4 * 3
    flipped = flip(table, early, near)
    near, far = sky(exchange(near, far, flipped), pixel_mask, pairs, sims, rows - 1)
    factors, ends, hot, weights, others = layout(
        small, cycle_order, colatitude, cycle_weight, table, pairs - early, near, 2 * sims, rows - 1
    )
    returned = exchange(near, far, ends)
    return analyse(returned, (flipped, others), tail, small, factors, ends, hot, weights)


def solution(mesh):
    devices = mesh.devices.reshape(mesh.shape["grp"], -1, 2)
    finer = Mesh(devices, ("grp", CHIP, CORE))
    ma = (CHIP, CORE)
    coefficients = P(ma, "grp", None, None)
    return jax.shard_map(
        shards,
        mesh=finer,
        in_specs=(coefficients, coefficients, P(ma, None, None), P(), P(), P(), P(), P(ma, None)),
        out_specs=(coefficients, coefficients),
        check_vma=False,
    )
```

```python
import functools
import math

import jax
import jax.numpy as jnp
import numpy as np
from jax import lax
from jax.experimental import pallas as pl
from jax.experimental.pallas import tpu as pltpu
from jax.sharding import Mesh
from jax.sharding import PartitionSpec as P

F32 = jnp.float32
BF16 = jnp.bfloat16
LANES = 128
GRANT = 24 * 2**20
STRIDE = 9
CHIP, CORE = "chip", "core"
NT = (((1,), (1,)), ((), ()))
NN = (((1,), (0,)), ((), ()))


def dot(a, b, dims=NN):
    return lax.dot_general(a, b, dims, preferred_element_type=F32)


def iota(shape, dim):
    return lax.broadcasted_iota(jnp.int32, shape, dim)


def across(tiles):
    return jnp.concatenate(list(tiles), axis=1)


def small_column(m_ref, first, pairs):
    row = iota((pairs, 1), 0)
    column = jnp.zeros((pairs, 1), jnp.int32)
    for p in range(pairs):
        column = jnp.where(row == p, m_ref[first + p], column)
    return column


def layout_rows(small, modes):
    k = iota((small.shape[0], modes), 1)
    upper = k >= modes - small
    degree = jnp.where(upper, k - 1, small + k).astype(F32)
    orders = jnp.where(upper, modes - 1 - small, small).astype(F32)
    last_degree = jnp.full(small.shape, modes - 1, F32)
    last_orders = (modes - 1 - small).astype(F32)
    return (
        (degree, orders, raising(degree, orders)),
        (last_degree, last_orders, raising(last_degree, last_orders)),
    )


def raising(degree, orders):
    square = (
        (degree * degree - orders * orders)
        * (2.0 * degree + 1.0)
        / jnp.maximum(2.0 * degree - 1.0, 1.0)
    )
    return jnp.where(degree > orders, jnp.sqrt(jnp.where(degree > orders, square, 0.0)), 0.0)


def slot_of_cycle(order_ref):
    n = order_ref.shape[1]
    core = lax.axis_index(CORE)
    place = iota((n, n), 1)
    near = place < n // 2
    slot = 2 * (place % (n // 2)) + jnp.where(near, core, 1 - core)
    pick = jnp.where(iota((n, n), 0) == slot, 1.0, 0.0).astype(BF16)
    order = jnp.broadcast_to(order_ref[...].astype(F32), (8, n)).astype(BF16)
    return jnp.where(iota((n, n), 0).astype(F32) == dot(order, pick)[:1], 1.0, 0.0)


def first_pair(pairs):
    return (lax.axis_index(CHIP) * lax.axis_size(CORE) + lax.axis_index(CORE)) * pairs


def turn(values):
    rows = values.shape[0]
    real = iota(values.shape, 0) % 2 == 0
    return jnp.where(real, -pltpu.roll(values, rows - 1, 0), pltpu.roll(values, 1, 0))


def synth_kernel(
    m_hbm, order_hbm, colat_hbm, t_hbm, w_hbm, l_hbm, near_ref, far_ref, lr_ref, ltail_ref, small_ref,
    m_ref, order_ref, colat_ref, t_ref, w_ref, last_ref, c_ref, s_ref, deg_ref, eps_ref, up_ref, end_ref, lasts_ref, f_ref, sems, *l_refs,
):
    pairs, sims = t_ref.shape[0], t_ref.shape[1]
    modes = t_ref.shape[3] - 1
    lines = 2 * sims
    steps = len(l_refs)
    chunk = modes // steps
    first = first_pair(pairs)
    wide = near_ref.shape[1] * near_ref.shape[2] // pairs
    cycles = last_ref.shape[2]

    pieces = [(m_hbm, m_ref), (order_hbm, order_ref), (colat_hbm, colat_ref), (w_hbm, w_ref), (t_hbm, t_ref)]
    pieces.append((l_hbm.at[pl.ds(modes, 1)], last_ref))
    pieces += [(l_hbm.at[pl.ds(j * chunk, chunk)], l_refs[j]) for j in range(steps)]
    copies = [pltpu.make_async_copy(*piece, sems.at[i]) for i, piece in enumerate(pieces)]
    for copy in copies:
        copy.start()
    for copy in copies[:3]:
        copy.wait()

    small = small_column(m_ref, first, pairs)
    (degree, _, eps), (_, _, last_eps) = layout_rows(small, modes)
    small_ref[...] = jnp.broadcast_to(small.astype(F32), small_ref.shape)
    deg_ref[...] = degree * (1.0 / modes)
    eps_ref[...] = eps * (1.0 / modes)
    last_eps = last_eps * (1.0 / modes)
    theta = colat_ref[...]
    cos, inv_sin = jnp.cos(theta), 1.0 / jnp.sin(theta)
    cycle_of_slot = slot_of_cycle(order_ref).T.astype(BF16)
    up_ref[...] = jnp.where(iota((pairs, modes), 1) >= modes - small, 1.0, 0.0)
    ends = iota((lines, modes), 1) == modes - 1

    copies[3].wait()
    copies[4].wait()
    def coefficients(p, _):
        tbar = t_ref[p].reshape(lines, modes + 1)
        wiener = w_ref[p].reshape(lines, modes + 1)
        main, last = wiener[:, :modes].astype(F32), wiener[:, modes:].astype(F32)
        raised = pltpu.roll(eps_ref[pl.ds(p, 1), :] * main, modes - 1, 1)
        raised = jnp.where(ends, end_ref[pl.ds(p, 1), :][:, :1] * last, raised)
        raised = jnp.concatenate([deg_ref[pl.ds(p, 1), :] * main, raised], axis=0).astype(BF16)
        upper = jnp.broadcast_to(up_ref[pl.ds(p, 1), :], (2 * lines, modes)).astype(BF16)
        for i, sets in enumerate((jnp.concatenate([tbar[:, :modes], wiener[:, :modes]], axis=0), raised)):
            above = sets * upper
            for t in range(modes // LANES):
                tile = slice(t * LANES, (t + 1) * LANES)
                c_ref[p, t, 2 * i * lines : 2 * (i + 1) * lines] = sets[:, tile]
                c_ref[p, t, 2 * (i + 2) * lines : 2 * (i + 3) * lines] = above[:, tile]
        lasts = jnp.concatenate(
            [tbar[:, modes:].astype(F32), last, ((modes - 1.0) / modes) * last, 0.0 * last], axis=0
        )
        lasts_ref[p] = jnp.broadcast_to(lasts.astype(BF16).astype(F32), lasts_ref.shape[1:])
        return 0

    end_ref[...] = jnp.broadcast_to(last_eps, end_ref.shape)
    lax.fori_loop(0, pairs, coefficients, 0, unroll=2)

    copies[5].wait()
    tail_rows = last_ref[0].astype(F32)
    ltail_ref[...] = tail_rows
    for j in range(steps):
        copies[6 + j].wait()
        at = slice(j * chunk, (j + 1) * chunk)
        for row in range(chunk):
            f_ref[row * STRIDE : row * STRIDE + pairs, :] = l_refs[j][row].astype(F32)
        for p in range(0, pairs, 2):
            tables = [f_ref[pl.ds(p + i, chunk, stride=STRIDE), :].astype(BF16) for i in range(2)]
            both = across(
                jnp.concatenate([c_ref[p, t], c_ref[p + 1, t]], axis=0)
                for t in range(j * chunk // LANES, (j + 1) * chunk // LANES)
            )
            sums = dot(both, jnp.concatenate(tables, axis=1))
            for i in range(2):
                lr_ref[p + i, at, :] = tables[i]
                part = sums[i * 8 * lines : (i + 1) * 8 * lines, i * cycles : (i + 1) * cycles]
                s_ref[p + i] = part if j == 0 else s_ref[p + i] + part

    blocks = []
    for p in range(pairs):
        small = m_ref[first + p]
        for half, order in enumerate((small, modes - 1 - small)):
            above = s_ref[p, 4 * lines :, :]
            sums = above + lasts_ref[p] * tail_rows[p : p + 1, :] if half else s_ref[p, : 4 * lines, :] - above
            s0, s1, s2, s3 = (sums[q * lines : (q + 1) * lines] for q in range(4))
            weight = jnp.where(order == 0, 1.0, 2.0) * modes ** (-0.5)
            ratio = order.astype(F32) * (1.0 / modes)
            blocks.append(s0 * weight)
            blocks.append((cos * s2 - s3) * inv_sin * weight)
            blocks.append(turn(s1) * ratio * inv_sin * weight)
        row = iota((wide - 6 * lines, s_ref.shape[2]), 0)
        low, high = (small % LANES).astype(F32), (small // LANES).astype(F32)
        blocks.append(jnp.where(row == 0, low, jnp.where(row == 1, high, 0.0)))
    fourier = jnp.concatenate(blocks, axis=0).astype(BF16)
    out = dot(cycle_of_slot, fourier, NT).astype(BF16)
    near_ref[...] = out[: cycles // 2].reshape(near_ref.shape)
    far_ref[...] = out[cycles // 2 :].reshape(far_ref.shape)


def synth(tbar_alm, twf_alm, table, m_slots, cycle_order, colatitude):
    pairs, sims, _, rows = tbar_alm.shape
    modes = rows - 1
    cycles = table.shape[2]
    lines = 2 * sims
    wide = 8 * lines
    steps = 4
    vmem = pl.BlockSpec(memory_space=pltpu.VMEM)
    hbm = pl.BlockSpec(memory_space=pltpu.HBM)
    return pl.pallas_call(
        synth_kernel,
        in_specs=[hbm] * 6,
        out_specs=[vmem] * 5,
        out_shape=[
            pltpu.VMEM((cycles // 2, pairs * wide // LANES, LANES), BF16),
            pltpu.VMEM((cycles // 2, pairs * wide // LANES, LANES), BF16),
            pltpu.VMEM((pairs, modes, cycles), BF16),
            pltpu.VMEM((pairs, cycles), F32),
            pltpu.VMEM((pairs, LANES), F32),
        ],
        scratch_shapes=[
            pltpu.SMEM(m_slots.shape, jnp.int32),
            pltpu.VMEM((1, cycles), jnp.int32),
            pltpu.VMEM((1, cycles), F32),
            pltpu.VMEM(tbar_alm.shape, BF16),
            pltpu.VMEM(twf_alm.shape, BF16),
            pltpu.VMEM((1, pairs, cycles), BF16),
            pltpu.VMEM((pairs, modes // LANES, 8 * lines, LANES), BF16),
            pltpu.VMEM((pairs, 8 * lines, cycles), F32),
            pltpu.VMEM((pairs, modes), F32),
            pltpu.VMEM((pairs, modes), F32),
            pltpu.VMEM((pairs, modes), F32),
            pltpu.VMEM((pairs, LANES), F32),
            pltpu.VMEM((pairs, 4 * lines, cycles), F32),
            pltpu.VMEM((modes // steps * STRIDE, cycles), F32),
            pltpu.SemaphoreType.DMA((steps + 6,)),
        ]
        + [pltpu.VMEM((modes // steps, pairs, cycles), BF16)] * steps,
        compiler_params=pltpu.CompilerParams(vmem_limit_bytes=GRANT),
        name="synth",
    )(*(pltpu.with_memory_space_constraint(x, pltpu.HBM) for x in (
        m_slots, cycle_order.reshape(1, -1), colatitude.reshape(1, -1), tbar_alm, twf_alm, table
    )))


def angles(left, right, period):
    return 2.0 * np.pi * (np.outer(left, right) % period) / period


def split(table):
    high = table.astype(np.float32).astype(jnp.bfloat16)
    return high, (table - high.astype(np.float64)).astype(np.float32).astype(jnp.bfloat16)


def sky_tables(modes, pixels):
    small = pixels // LANES
    m1, j2, m2 = np.arange(LANES), np.arange(small), np.arange(modes // LANES)
    j1 = np.arange(LANES).reshape(-1, LANES // small).T.reshape(-1)
    th = angles(j2, m2, small).reshape(small, 2, -1)
    c, s = np.cos(th), np.sin(th)
    first = np.stack([np.stack([c, -s], 2), np.stack([s, c], 2)], 0).reshape(2 * small, -1)
    th = angles(j2, m1, pixels)
    twist = np.stack([np.cos(th), np.sin(th)])
    th = angles(m1, j1, LANES)
    second = np.concatenate([np.cos(th), -np.sin(th)], 0)
    third = np.concatenate([np.cos(th.T), -np.sin(th.T)], 1)
    th = angles(m2, j2, small).reshape(2, -1, small)
    c, s = np.cos(th), np.sin(th)
    fourth = np.stack([np.concatenate([c, s], 2), np.concatenate([-s, c], 2)], 1)
    fourth = fourth.reshape(2 * modes // LANES, -1)
    return (
        np.concatenate(split(first), 1), twist.astype(np.float32), np.concatenate(split(second), 0),
        np.concatenate(split(third), 0), np.concatenate(split(fourth), 1),
    )


def near_then_far(ref):
    chips, parts, lanes = ref.shape
    halves = (ref[:, : parts // 2], ref[:, parts // 2 :])
    return jnp.concatenate([h.reshape(chips, parts // 2 * lanes) for h in halves], axis=0)


def sky_kernel(
    pairs, sims, x_ref, mask_ref, first_ref, twist_ref, second_ref, third_ref, fourth_ref, near_ref, far_ref,
    xt_ref, lhs_ref, hot_ref,
):
    devices = 2 * x_ref.shape[0]
    wide = x_ref.shape[1] * x_ref.shape[2] // 2 // pairs
    lines = 2 * sims
    small = twist_ref.shape[1]
    pixels = small * LANES
    tall = fourth_ref.shape[0] // 4
    xt_ref[...] = near_then_far(x_ref).astype(F32).T

    n = 2 * tall
    groups = 3 * sims
    sorted_halves, places = [], []
    for half in range(2):
        place = []
        for p in range(pairs):
            at = p * wide + 6 * lines
            low, high = (xt_ref[at + i : at + i + 1, :].astype(jnp.int32) for i in range(2))
            if half:
                low, high = LANES - 1 - low, tall - 1 - high
            place.append(iota((tall, devices), 0) == high)
            hot_ref[half, p] = jnp.where(iota((LANES, devices), 0) == low, 1.0, 0.0).astype(BF16)
            parts = []
            for row in range(3 * lines):
                at = p * wide + half * 3 * lines + row
                parts.append(jnp.where(place[p], xt_ref[at : at + 1, :], 0.0))
            lhs_ref[p] = jnp.concatenate(parts, axis=0).astype(BF16)
        places.append(place)
        left, right = (across(ref[p] for p in range(pairs)) for ref in (lhs_ref, hot_ref.at[half]))
        sorted_halves.append(dot(left, right, NT).astype(BF16))

    spread = jnp.concatenate(
        [
            jnp.concatenate([s[g * n : (g + 1) * n] for s in sorted_halves], axis=0)
            for g in range(groups)
        ],
        axis=1,
    )
    stage = dot(first_ref[...], jnp.concatenate([spread, spread], axis=0))
    cos, sin = twist_ref[0], twist_ref[1]
    twisted = []
    for g in range(groups):
        re, im = (stage[i * small : (i + 1) * small, g * LANES : (g + 1) * LANES] for i in range(2))
        twisted.append(jnp.concatenate([re * cos - im * sin, re * sin + im * cos], axis=1))
    twisted = jnp.concatenate(twisted, axis=0).astype(BF16)
    maps = dot(twisted, second_ref[: 2 * LANES]) + dot(twisted, second_ref[2 * LANES :])

    mask = mask_ref[...].astype(F32).T
    mask = jnp.concatenate([mask[i * small : (i + 1) * small] for i in range(LANES // small)], axis=1)
    products = []
    for q in range(1, 3):
        for s in range(sims):
            at = (q * sims + s) * small
            products.append(mask * maps[s * small : (s + 1) * small] * maps[at : at + small])
    products = jnp.concatenate(products, axis=0).astype(BF16)
    stage = dot(products, third_ref[:LANES]) + dot(products, third_ref[LANES:])
    groups = 2 * sims
    twisted = []
    for g in range(groups):
        re, im = (stage[g * small : (g + 1) * small, i * LANES : (i + 1) * LANES] for i in range(2))
        twisted.append(jnp.concatenate([re * cos + im * sin, im * cos - re * sin], axis=0))
    twisted = jnp.concatenate(twisted, axis=1).astype(BF16)
    spectra = dot(fourth_ref[...], jnp.concatenate([twisted, twisted], axis=0)) * pixels ** (-0.5)
    spectra = spectra.astype(BF16)

    rows, columns = 2 * groups, 2 * groups * tall
    add = jnp.where(iota((rows, columns), 1) // tall == iota((rows, columns), 0), 1.0, 0.0).astype(BF16)
    found = []
    for half in range(2):
        stacked = jnp.concatenate(
            [spectra[half * n : (half + 1) * n, g * LANES : (g + 1) * LANES] for g in range(groups)], axis=0
        )
        values = dot(stacked, across(hot_ref[half, p] for p in range(pairs)))
        for p in range(pairs):
            tile = slice(p * devices, (p + 1) * devices)
            keep = jnp.concatenate([places[half][p]] * rows, axis=0)
            lhs_ref[p, :columns] = jnp.where(keep, values[:, tile], 0.0).astype(BF16)
        found.append(dot(add, across(lhs_ref[p, :columns] for p in range(pairs))))
    blocks = [found[half][:, p * devices : (p + 1) * devices] for p in range(pairs) for half in range(2)]
    out = jnp.concatenate(blocks, axis=0).T.astype(BF16)
    near_ref[...] = out[: devices // 2].reshape(near_ref.shape)
    far_ref[...] = out[devices // 2 :].reshape(far_ref.shape)


def sky(received, pixel_mask, pairs, sims, modes):
    devices = 2 * received.shape[0]
    pixels = pixel_mask.shape[1]
    tables = sky_tables(modes, pixels)
    vmem = pl.BlockSpec(memory_space=pltpu.VMEM)
    tall = modes // LANES // 2
    return pl.pallas_call(
        functools.partial(sky_kernel, pairs, sims),
        in_specs=[vmem] * 7,
        out_specs=[vmem] * 2,
        out_shape=[pltpu.VMEM((devices // 2, pairs * 8 * sims // LANES, LANES), BF16)] * 2,
        scratch_shapes=[
            pltpu.VMEM((received.shape[1] // 2 * LANES, devices), F32),
            pltpu.VMEM((pairs, 6 * sims * tall, devices), BF16),
            pltpu.VMEM((2, pairs, LANES, devices), BF16),
        ],
        compiler_params=pltpu.CompilerParams(vmem_limit_bytes=GRANT),
        name="sky",
    )(received, pixel_mask.reshape(-1, LANES), *(jnp.asarray(t) for t in tables))


def rows_kernel(
    small_ref, order_ref, colat_ref, weight_ref, table_ref, _, row_ref, end_ref, hot_ref, with_ref, flip_ref
):
    pairs, modes, cycles = row_ref.shape[1], row_ref.shape[3], end_ref.shape[2]
    small = small_ref[:, :1].astype(jnp.int32)
    main, last = layout_rows(small, modes)
    for i, ref in enumerate((row_ref, end_ref)):
        degree, orders, eps = (main, last)[i]
        scale = (modes / cycles) ** 0.5 / jnp.sqrt(jnp.maximum(degree * (degree + 1.0), 1.0))
        for j, values in enumerate((degree * scale, eps * scale, orders * scale)):
            if i:
                ref[j] = jnp.broadcast_to(values, ref.shape[1:])
            else:
                for p in range(pairs):
                    ref[j, p] = jnp.broadcast_to(values[p : p + 1], ref.shape[2:])
    late = flip_ref.shape[0]
    for p in range(late):
        for t in range(modes // LANES):
            flip_ref[p, t] = table_ref[pairs - late + p, t * LANES : (t + 1) * LANES].T
    hot_ref[...] = slot_of_cycle(order_ref).astype(BF16)
    theta, weight = colat_ref[...], weight_ref[...]
    with_ref[0] = jnp.broadcast_to(weight * jnp.cos(theta) / jnp.sin(theta), with_ref.shape[1:])
    with_ref[1] = jnp.broadcast_to(weight / jnp.sin(theta), with_ref.shape[1:])


def layout(small, cycle_order, colatitude, cycle_weight, table, late, after, lines, modes):
    pairs = small.shape[0]
    cycles = cycle_order.shape[0]
    vmem = pl.BlockSpec(memory_space=pltpu.VMEM)
    return pl.pallas_call(
        rows_kernel,
        in_specs=[vmem] * 6,
        out_specs=[vmem] * 5,
        out_shape=[
            pltpu.VMEM((3, pairs, lines, modes), F32), pltpu.VMEM((3, pairs, cycles), F32),
            pltpu.VMEM((cycles, cycles), BF16), pltpu.VMEM((2, lines, cycles), F32),
            pltpu.VMEM((late, modes // LANES, cycles, LANES), BF16),
        ],
        compiler_params=pltpu.CompilerParams(vmem_limit_bytes=GRANT),
        cost_estimate=pl.CostEstimate(flops=10**9, bytes_accessed=10**6, transcendentals=10**5),
        name="layout",
    )(small, cycle_order.reshape(1, -1), colatitude.reshape(1, -1), cycle_weight.reshape(1, -1), table, after)


def flip_kernel(table_ref, _, out_ref):
    for p in range(out_ref.shape[0]):
        for t in range(out_ref.shape[1]):
            out_ref[p, t] = table_ref[p, t * LANES : (t + 1) * LANES].T


def flip(table, pairs, after):
    _, modes, cycles = table.shape
    vmem = pl.BlockSpec(memory_space=pltpu.VMEM)
    return pl.pallas_call(
        flip_kernel,
        in_specs=[vmem] * 2,
        out_specs=vmem,
        out_shape=pltpu.VMEM((pairs, modes // LANES, cycles, LANES), BF16),
        compiler_params=pltpu.CompilerParams(vmem_limit_bytes=GRANT),
        cost_estimate=pl.CostEstimate(flops=10**9, bytes_accessed=10**6, transcendentals=0),
        name="flip",
    )(table, after)


def analyse_kernel(
    small_ref, r_ref, l_ref, l2_ref, tail_ref, row_ref, end_ref, hot_ref, with_ref, grad_hbm, curl_hbm,
    w_ref, grad_ref, curl_ref, sems,
):
    pairs, lines, modes = row_ref.shape[1:]
    cycles = l_ref.shape[2]
    sims = lines // 2
    high = 6 * lines

    spectra = dot(near_then_far(r_ref).astype(F32).T.astype(BF16), hot_ref[...], NT)
    with_cos, with_sin = with_ref[0], with_ref[1]
    for i in range(pairs):
        for half in range(2):
            at = (i * 2 + half) * 2 * lines
            parts, turned = [], []
            for values in (spectra[at : at + lines], spectra[at + lines : at + 2 * lines]):
                parts += [values * with_cos, values * with_sin]
                turned.append(turn(parts[-1]))
            parts = jnp.concatenate(parts + turned, axis=0)
            w_ref[i, half * high : (half + 1) * high] = parts.astype(BF16)

    k = iota((lines, modes), 1)
    starts = k == 0

    def previous(values):
        return jnp.where(starts, 0.0, pltpu.roll(values, 1, 1))

    copies = []
    for p in range(pairs):
        odd = p % 2
        if not odd:
            ref, at = (l_ref, p) if p < l_ref.shape[0] else (l2_ref, p - l_ref.shape[0])
            tables = across(
                jnp.concatenate([ref[at, t], ref[at + 1, t]], axis=0) for t in range(ref.shape[1])
            )
            blank = jnp.zeros((2 * high, cycles), BF16)
            left = [jnp.concatenate([w_ref[p], blank], axis=0), jnp.concatenate([blank, w_ref[p + 1]], axis=0)]
            both = dot(across(left), tables)
        sums = both[odd * 2 * high : (odd + 1) * 2 * high]
        upper = k >= modes - small_ref[p : p + 1, :1].astype(jnp.int32)
        a0, a1, a2, a3, t1, t3 = (
            jnp.where(upper, sums[high + q * lines : high + (q + 1) * lines], sums[q * lines : (q + 1) * lines])
            for q in range(6)
        )
        level, raised, azimuth = (row_ref[i, p] for i in range(3))
        grad = level * a0 - raised * previous(a1) - azimuth * t3
        curl = level * a2 - raised * previous(a3) + azimuth * t1
        last = jnp.sum(w_ref[p, high:].astype(F32) * tail_ref[p : p + 1, :], axis=1, keepdims=True)
        level, raised, azimuth = (end_ref[i, p : p + 1, :1] for i in range(3))
        b0, b1, b2, b3, u1, u3 = (last[q * lines : (q + 1) * lines] for q in range(6))
        last_grad = level * b0 - raised * a1[:, modes - 1 :] - azimuth * u3
        last_curl = level * b2 - raised * a3[:, modes - 1 :] + azimuth * u1
        for ref, hbm, main, last in ((grad_ref, grad_hbm, grad, last_grad), (curl_ref, curl_hbm, curl, last_curl)):
            ref[p, :, :, :modes] = main.reshape(sims, 2, modes)
            ref[p, :, :, modes:] = last.reshape(sims, 2, 1)
            copies.append(pltpu.make_async_copy(ref.at[p], hbm.at[p], sems.at[len(copies)]))
            copies[-1].start()
    for copy in copies:
        copy.wait()


def analyse(returned, tables, tail, small, rows, ends, hot, weights):
    _, pairs, lines, modes = rows.shape
    cycles = hot.shape[0]
    vmem = pl.BlockSpec(memory_space=pltpu.VMEM)
    hbm = pl.BlockSpec(memory_space=pltpu.HBM)
    shape = (pairs, lines // 2, 2, modes + 1)
    out = jax.ShapeDtypeStruct(shape, F32)
    return pl.pallas_call(
        analyse_kernel,
        in_specs=[vmem] * 9,
        out_specs=[hbm, hbm],
        out_shape=[out, out],
        scratch_shapes=[
            pltpu.VMEM((pairs, 12 * lines, cycles), BF16),
            pltpu.VMEM(shape, F32),
            pltpu.VMEM(shape, F32),
            pltpu.SemaphoreType.DMA((2 * pairs,)),
        ],
        compiler_params=pltpu.CompilerParams(vmem_limit_bytes=GRANT),
        name="analyse",
    )(small, returned, *tables, tail, rows, ends, hot, weights)


def merge_kernel(near_ref, far_ref, *refs):
    out_ref = refs[-1]
    parts = near_ref.shape[1]
    out_ref[:, :parts] = near_ref[...]
    out_ref[:, parts:] = far_ref[...]


def exchange(near, far, *beside):
    vmem = pl.BlockSpec(memory_space=pltpu.VMEM)
    swapped = lax.ppermute(far, CORE, [(0, 1), (1, 0)])
    chips, parts, lanes = near.shape
    both = pl.pallas_call(
        merge_kernel,
        in_specs=[vmem] * (2 + len(beside)),
        out_specs=vmem,
        out_shape=pltpu.VMEM((chips, 2 * parts, lanes), near.dtype),
        compiler_params=pltpu.CompilerParams(vmem_limit_bytes=GRANT),
        name="merge",
    )(near, swapped, *beside)
    return lax.all_to_all(both, CHIP, 0, 0, tiled=True)


def shards(tbar_alm, twf_alm, legendre, m_slots, cycle_order, colatitude, cycle_weight, pixel_mask):
    pairs, sims, _, rows = tbar_alm.shape
    by_row = jnp.transpose(legendre, (1, 0, 2))
    near, far, table, tail, small = synth(tbar_alm, twf_alm, by_row, m_slots, cycle_order, colatitude)
    early = pairs // 4 * 3
    flipped = flip(table, early, near)
    near, far = sky(exchange(near, far, flipped), pixel_mask, pairs, sims, rows - 1)
    factors, ends, hot, weights, others = layout(
        small, cycle_order, colatitude, cycle_weight, table, pairs - early, near, 2 * sims, rows - 1
    )
    returned = exchange(near, far, ends)
    return analyse(returned, (flipped, others), tail, small, factors, ends, hot, weights)


def solution(mesh):
    devices = mesh.devices.reshape(mesh.shape["grp"], -1, 2)
    finer = Mesh(devices, ("grp", CHIP, CORE))
    ma = (CHIP, CORE)
    coefficients = P(ma, "grp", None, None)
    return jax.shard_map(
        shards,
        mesh=finer,
        in_specs=(coefficients, coefficients, P(ma, None, None), P(), P(), P(), P(), P(ma, None)),
        out_specs=(coefficients, coefficients),
        check_vma=False,
    )
```

```python
import functools
import math

import jax
import jax.numpy as jnp
import numpy as np
from jax import lax
from jax.experimental import pallas as pl
from jax.experimental.pallas import tpu as pltpu
from jax.sharding import Mesh
from jax.sharding import PartitionSpec as P

F32 = jnp.float32
BF16 = jnp.bfloat16
LANES = 128
GRANT = 24 * 2**20
STRIDE = 9
CUTS = 4
CHIP, CORE = "chip", "core"
NT = (((1,), (1,)), ((), ()))
NN = (((1,), (0,)), ((), ()))


def dot(a, b, dims=NN):
    return lax.dot_general(a, b, dims, preferred_element_type=F32)


def iota(shape, dim):
    return lax.broadcasted_iota(jnp.int32, shape, dim)


def across(tiles):
    return jnp.concatenate(list(tiles), axis=1)


def small_column(m_ref, first, pairs):
    row = iota((pairs, 1), 0)
    column = jnp.zeros((pairs, 1), jnp.int32)
    for p in range(pairs):
        column = jnp.where(row == p, m_ref[first + p], column)
    return column


def layout_rows(small, modes):
    k = iota((small.shape[0], modes), 1)
    upper = k >= modes - small
    degree = jnp.where(upper, k - 1, small + k).astype(F32)
    orders = jnp.where(upper, modes - 1 - small, small).astype(F32)
    last_degree = jnp.full(small.shape, modes - 1, F32)
    last_orders = (modes - 1 - small).astype(F32)
    return (
        (degree, orders, raising(degree, orders)),
        (last_degree, last_orders, raising(last_degree, last_orders)),
    )


def raising(degree, orders):
    square = (
        (degree * degree - orders * orders)
        * (2.0 * degree + 1.0)
        / jnp.maximum(2.0 * degree - 1.0, 1.0)
    )
    return jnp.where(degree > orders, jnp.sqrt(jnp.where(degree > orders, square, 0.0)), 0.0)


def slot_of_cycle(order_ref):
    n = order_ref.shape[1]
    core = lax.axis_index(CORE)
    place = iota((n, n), 1)
    near = place < n // 2
    slot = 2 * (place % (n // 2)) + jnp.where(near, core, 1 - core)
    pick = jnp.where(iota((n, n), 0) == slot, 1.0, 0.0).astype(BF16)
    order = jnp.broadcast_to(order_ref[...].astype(F32), (8, n)).astype(BF16)
    return jnp.where(iota((n, n), 0).astype(F32) == dot(order, pick)[:1], 1.0, 0.0)


def first_pair(pairs):
    return (lax.axis_index(CHIP) * lax.axis_size(CORE) + lax.axis_index(CORE)) * pairs


def swap_rows(values):
    rows = values.shape[0]
    real = iota(values.shape, 0) % 2 == 0
    return jnp.where(real, pltpu.roll(values, rows - 1, 0), pltpu.roll(values, 1, 0))


def turn(values):
    rows = values.shape[0]
    real = iota(values.shape, 0) % 2 == 0
    return jnp.where(real, -pltpu.roll(values, rows - 1, 0), pltpu.roll(values, 1, 0))


def synth_kernel(
    m_hbm, order_hbm, colat_hbm, t_hbm, w_hbm, l_hbm, near_ref, far_ref, lr_ref, ltail_ref, small_ref,
    m_ref, order_ref, colat_ref, t_ref, w_ref, last_ref, c_ref, s_ref, deg_ref, eps_ref, up_ref, end_ref, lasts_ref, f_ref, sems, *l_refs,
):
    pairs, sims = t_ref.shape[0], t_ref.shape[1]
    modes = t_ref.shape[3] - 1
    lines = 2 * sims
    steps = len(l_refs)
    chunk = modes // steps
    first = first_pair(pairs)
    wide = near_ref.shape[1] * near_ref.shape[2] // pairs
    cycles = last_ref.shape[2]

    pieces = [(m_hbm, m_ref), (order_hbm, order_ref), (colat_hbm, colat_ref), (w_hbm, w_ref), (t_hbm, t_ref)]
    pieces.append((l_hbm.at[pl.ds(modes, 1)], last_ref))
    pieces += [(l_hbm.at[pl.ds(j * chunk, chunk)], l_refs[j]) for j in range(steps)]
    copies = [pltpu.make_async_copy(*piece, sems.at[i]) for i, piece in enumerate(pieces)]
    for copy in copies:
        copy.start()
    for copy in copies[:3]:
        copy.wait()

    small = small_column(m_ref, first, pairs)
    (degree, _, eps), (_, _, last_eps) = layout_rows(small, modes)
    small_ref[...] = jnp.broadcast_to(small.astype(F32), small_ref.shape)
    deg_ref[...] = degree * (1.0 / modes)
    eps_ref[...] = eps * (1.0 / modes)
    last_eps = last_eps * (1.0 / modes)
    theta = colat_ref[...]
    cos, inv_sin = jnp.cos(theta), 1.0 / jnp.sin(theta)
    cycle_of_slot = slot_of_cycle(order_ref).T.astype(BF16)
    up_ref[...] = jnp.where(iota((pairs, modes), 1) >= modes - small, 1.0, 0.0)
    ends = iota((lines, modes), 1) == modes - 1

    copies[3].wait()
    copies[4].wait()
    def coefficients(p, _):
        tbar = t_ref[p].reshape(lines, modes + 1)
        wiener = w_ref[p].reshape(lines, modes + 1)
        main, last = wiener[:, :modes].astype(F32), wiener[:, modes:].astype(F32)
        raised = pltpu.roll(eps_ref[pl.ds(p, 1), :] * main, modes - 1, 1)
        raised = jnp.where(ends, end_ref[pl.ds(p, 1), :][:, :1] * last, raised)
        raised = jnp.concatenate([deg_ref[pl.ds(p, 1), :] * main, raised], axis=0).astype(BF16)
        upper = jnp.broadcast_to(up_ref[pl.ds(p, 1), :], (2 * lines, modes)).astype(BF16)
        for i, sets in enumerate((jnp.concatenate([tbar[:, :modes], wiener[:, :modes]], axis=0), raised)):
            above = sets * upper
            for t in range(modes // LANES):
                tile = slice(t * LANES, (t + 1) * LANES)
                c_ref[p, t, 2 * i * lines : 2 * (i + 1) * lines] = sets[:, tile]
                c_ref[p, t, 2 * (i + 2) * lines : 2 * (i + 3) * lines] = above[:, tile]
        lasts = jnp.concatenate(
            [tbar[:, modes:].astype(F32), last, ((modes - 1.0) / modes) * last, 0.0 * last], axis=0
        )
        lasts_ref[p] = jnp.broadcast_to(lasts.astype(BF16).astype(F32), lasts_ref.shape[1:])
        return 0

    end_ref[...] = jnp.broadcast_to(last_eps, end_ref.shape)
    lax.fori_loop(0, pairs, coefficients, 0, unroll=2)

    copies[5].wait()
    tail_rows = last_ref[0].astype(F32)
    ltail_ref[...] = tail_rows
    for j in range(steps):
        copies[6 + j].wait()
        at = slice(j * chunk, (j + 1) * chunk)
        for row in range(chunk):
            f_ref[row * STRIDE : row * STRIDE + pairs, :] = l_refs[j][row].astype(F32)
        for p in range(0, pairs, 2):
            tables = [f_ref[pl.ds(p + i, chunk, stride=STRIDE), :].astype(BF16) for i in range(2)]
            both = across(
                jnp.concatenate([c_ref[p, t], c_ref[p + 1, t]], axis=0)
                for t in range(j * chunk // LANES, (j + 1) * chunk // LANES)
            )
            sums = dot(both, jnp.concatenate(tables, axis=1))
            for i in range(2):
                lr_ref[p + i, at, :] = tables[i]
                part = sums[i * 8 * lines : (i + 1) * 8 * lines, i * cycles : (i + 1) * cycles]
                s_ref[p + i] = part if j == 0 else s_ref[p + i] + part

    blocks = []
    for p in range(pairs):
        small = m_ref[first + p]
        for half, order in enumerate((small, modes - 1 - small)):
            above = s_ref[p, 4 * lines :, :]
            sums = above + lasts_ref[p] * tail_rows[p : p + 1, :] if half else s_ref[p, : 4 * lines, :] - above
            s0, s1, s2, s3 = (sums[q * lines : (q + 1) * lines] for q in range(4))
            weight = jnp.where(order == 0, 1.0, 2.0) * modes ** (-0.5)
            ratio = order.astype(F32) * (1.0 / modes)
            blocks.append(s0 * weight)
            blocks.append((cos * s2 - s3) * inv_sin * weight)
            blocks.append(turn(s1) * ratio * inv_sin * weight)
        row = iota((wide - 6 * lines, s_ref.shape[2]), 0)
        low, high = (small % LANES).astype(F32), (small // LANES).astype(F32)
        blocks.append(jnp.where(row == 0, low, jnp.where(row == 1, high, 0.0)))
    fourier = jnp.concatenate(blocks, axis=0).astype(BF16)
    out = dot(cycle_of_slot, fourier, NT).astype(BF16)
    near_ref[...] = out[: cycles // 2].reshape(near_ref.shape)
    far_ref[...] = out[cycles // 2 :].reshape(far_ref.shape)


def synth(tbar_alm, twf_alm, table, m_slots, cycle_order, colatitude):
    pairs, sims, _, rows = tbar_alm.shape
    modes = rows - 1
    cycles = table.shape[2]
    lines = 2 * sims
    wide = 8 * lines
    steps = 4
    vmem = pl.BlockSpec(memory_space=pltpu.VMEM)
    hbm = pl.BlockSpec(memory_space=pltpu.HBM)
    return pl.pallas_call(
        synth_kernel,
        in_specs=[hbm] * 6,
        out_specs=[vmem] * 5,
        out_shape=[
            pltpu.VMEM((cycles // 2, pairs * wide // LANES, LANES), BF16),
            pltpu.VMEM((cycles // 2, pairs * wide // LANES, LANES), BF16),
            pltpu.VMEM((pairs, modes, cycles), BF16),
            pltpu.VMEM((pairs, cycles), F32),
            pltpu.VMEM((pairs, LANES), F32),
        ],
        scratch_shapes=[
            pltpu.SMEM(m_slots.shape, jnp.int32),
            pltpu.VMEM((1, cycles), jnp.int32),
            pltpu.VMEM((1, cycles), F32),
            pltpu.VMEM(tbar_alm.shape, BF16),
            pltpu.VMEM(twf_alm.shape, BF16),
            pltpu.VMEM((1, pairs, cycles), BF16),
            pltpu.VMEM((pairs, modes // LANES, 8 * lines, LANES), BF16),
            pltpu.VMEM((pairs, 8 * lines, cycles), F32),
            pltpu.VMEM((pairs, modes), F32),
            pltpu.VMEM((pairs, modes), F32),
            pltpu.VMEM((pairs, modes), F32),
            pltpu.VMEM((pairs, LANES), F32),
            pltpu.VMEM((pairs, 4 * lines, cycles), F32),
            pltpu.VMEM((modes // steps * STRIDE, cycles), F32),
            pltpu.SemaphoreType.DMA((steps + 6,)),
        ]
        + [pltpu.VMEM((modes // steps, pairs, cycles), BF16)] * steps,
        compiler_params=pltpu.CompilerParams(vmem_limit_bytes=GRANT),
        name="synth",
    )(*(pltpu.with_memory_space_constraint(x, pltpu.HBM) for x in (
        m_slots, cycle_order.reshape(1, -1), colatitude.reshape(1, -1), tbar_alm, twf_alm, table
    )))


def angles(left, right, period):
    return 2.0 * np.pi * (np.outer(left, right) % period) / period


def split(table):
    high = table.astype(np.float32).astype(jnp.bfloat16)
    return high, (table - high.astype(np.float64)).astype(np.float32).astype(jnp.bfloat16)


def sky_tables(modes, pixels):
    small = pixels // LANES
    m1, j2, m2 = np.arange(LANES), np.arange(small), np.arange(modes // LANES)
    j1 = np.arange(LANES).reshape(-1, LANES // small).T.reshape(-1)
    th = angles(j2, m2, small).reshape(small, 2, -1)
    c, s = np.cos(th), np.sin(th)
    first = np.stack([np.stack([c, -s], 2), np.stack([s, c], 2)], 0).reshape(2 * small, -1)
    th = angles(j2, m1, pixels)
    twist = np.stack([np.cos(th), np.sin(th)])
    th = angles(m1, j1, LANES)
    second = np.concatenate([np.cos(th), -np.sin(th)], 0)
    third = np.concatenate([np.cos(th.T), -np.sin(th.T)], 1)
    th = angles(m2, j2, small).reshape(2, -1, small)
    c, s = np.cos(th), np.sin(th)
    fourth = np.stack([np.concatenate([c, s], 2), np.concatenate([-s, c], 2)], 1)
    fourth = fourth.reshape(2 * modes // LANES, -1)
    return (
        np.concatenate(split(first), 1), twist.astype(np.float32), np.concatenate(split(second), 0),
        np.concatenate(split(third), 0), np.concatenate(split(fourth), 1),
    )


def near_then_far(ref):
    chips, parts, lanes = ref.shape
    halves = (ref[:, : parts // 2], ref[:, parts // 2 :])
    return jnp.concatenate([h.reshape(chips, parts // 2 * lanes) for h in halves], axis=0)


def sky_kernel(
    pairs, sims, x_ref, mask_ref, first_ref, twist_ref, second_ref, third_ref, fourth_ref, near_ref, far_ref,
    xt_ref, lhs_ref, hot_ref,
):
    devices = 2 * x_ref.shape[0]
    wide = x_ref.shape[1] * x_ref.shape[2] // 2 // pairs
    lines = 2 * sims
    small = twist_ref.shape[1]
    pixels = small * LANES
    tall = fourth_ref.shape[0] // 4
    xt_ref[...] = near_then_far(x_ref).astype(F32).T

    n = 2 * tall
    groups = 3 * sims
    sorted_halves, places = [], []
    for half in range(2):
        place = []
        for p in range(pairs):
            at = p * wide + 6 * lines
            low, high = (xt_ref[at + i : at + i + 1, :].astype(jnp.int32) for i in range(2))
            if half:
                low, high = LANES - 1 - low, tall - 1 - high
            place.append(iota((tall, devices), 0) == high)
            hot_ref[half, p] = jnp.where(iota((LANES, devices), 0) == low, 1.0, 0.0).astype(BF16)
            parts = []
            for row in range(3 * lines):
                at = p * wide + half * 3 * lines + row
                parts.append(jnp.where(place[p], xt_ref[at : at + 1, :], 0.0))
            lhs_ref[p] = jnp.concatenate(parts, axis=0).astype(BF16)
        places.append(place)
        left, right = (across(ref[p] for p in range(pairs)) for ref in (lhs_ref, hot_ref.at[half]))
        sorted_halves.append(dot(left, right, NT).astype(BF16))

    spread = jnp.concatenate(
        [
            jnp.concatenate([s[g * n : (g + 1) * n] for s in sorted_halves], axis=0)
            for g in range(groups)
        ],
        axis=1,
    )
    stage = dot(first_ref[...], jnp.concatenate([spread, spread], axis=0))
    cos, sin = twist_ref[0], twist_ref[1]
    twisted = []
    for g in range(groups):
        re, im = (stage[i * small : (i + 1) * small, g * LANES : (g + 1) * LANES] for i in range(2))
        twisted.append(jnp.concatenate([re * cos - im * sin, re * sin + im * cos], axis=1))
    twisted = jnp.concatenate(twisted, axis=0).astype(BF16)
    maps = dot(twisted, second_ref[: 2 * LANES]) + dot(twisted, second_ref[2 * LANES :])

    mask = mask_ref[...].astype(F32).T
    mask = jnp.concatenate([mask[i * small : (i + 1) * small] for i in range(LANES // small)], axis=1)
    products = []
    for q in range(1, 3):
        for s in range(sims):
            at = (q * sims + s) * small
            products.append(mask * maps[s * small : (s + 1) * small] * maps[at : at + small])
    products = jnp.concatenate(products, axis=0).astype(BF16)
    stage = dot(products, third_ref[:LANES]) + dot(products, third_ref[LANES:])
    groups = 2 * sims
    twisted = []
    for g in range(groups):
        re, im = (stage[g * small : (g + 1) * small, i * LANES : (i + 1) * LANES] for i in range(2))
        twisted.append(jnp.concatenate([re * cos + im * sin, im * cos - re * sin], axis=0))
    twisted = jnp.concatenate(twisted, axis=1).astype(BF16)
    spectra = dot(fourth_ref[...], jnp.concatenate([twisted, twisted], axis=0)) * pixels ** (-0.5)
    spectra = spectra.astype(BF16)

    rows, columns = 2 * groups, 2 * groups * tall
    add = jnp.where(iota((rows, columns), 1) // tall == iota((rows, columns), 0), 1.0, 0.0).astype(BF16)
    found = []
    for half in range(2):
        stacked = jnp.concatenate(
            [spectra[half * n : (half + 1) * n, g * LANES : (g + 1) * LANES] for g in range(groups)], axis=0
        )
        values = dot(stacked, across(hot_ref[half, p] for p in range(pairs)))
        for p in range(pairs):
            tile = slice(p * devices, (p + 1) * devices)
            keep = jnp.concatenate([places[half][p]] * rows, axis=0)
            lhs_ref[p, :columns] = jnp.where(keep, values[:, tile], 0.0).astype(BF16)
        found.append(dot(add, across(lhs_ref[p, :columns] for p in range(pairs))))
    blocks = [found[half][:, p * devices : (p + 1) * devices] for p in range(pairs) for half in range(2)]
    out = jnp.concatenate(blocks, axis=0).T.astype(BF16)
    near_ref[...] = out[: devices // 2].reshape(near_ref.shape)
    far_ref[...] = out[devices // 2 :].reshape(far_ref.shape)


def sky(received, pixel_mask, pairs, sims, modes):
    devices = 2 * received.shape[0]
    pixels = pixel_mask.shape[1]
    tables = sky_tables(modes, pixels)
    vmem = pl.BlockSpec(memory_space=pltpu.VMEM)
    tall = modes // LANES // 2
    return pl.pallas_call(
        functools.partial(sky_kernel, pairs, sims),
        in_specs=[vmem] * 7,
        out_specs=[vmem] * 2,
        out_shape=[pltpu.VMEM((devices // 2, pairs * 8 * sims // LANES, LANES), BF16)] * 2,
        scratch_shapes=[
            pltpu.VMEM((received.shape[1] // 2 * LANES, devices), F32),
            pltpu.VMEM((pairs, 6 * sims * tall, devices), BF16),
            pltpu.VMEM((2, pairs, LANES, devices), BF16),
        ],
        compiler_params=pltpu.CompilerParams(vmem_limit_bytes=GRANT),
        name="sky",
    )(received, pixel_mask.reshape(-1, LANES), *(jnp.asarray(t) for t in tables))


def rows_kernel(
    small_ref, order_ref, colat_ref, weight_ref, table_ref, _, row_ref, end_ref, hot_ref, with_ref, flip_ref
):
    pairs, modes, cycles = row_ref.shape[1], row_ref.shape[3], end_ref.shape[2]
    small = small_ref[:, :1].astype(jnp.int32)
    main, last = layout_rows(small, modes)
    for i, ref in enumerate((row_ref, end_ref)):
        degree, orders, eps = (main, last)[i]
        scale = (modes / cycles) ** 0.5 / jnp.sqrt(jnp.maximum(degree * (degree + 1.0), 1.0))
        for j, values in enumerate((degree * scale, eps * scale, orders * scale)):
            if i:
                ref[j] = jnp.broadcast_to(values, ref.shape[1:])
            else:
                for p in range(pairs):
                    row = jnp.broadcast_to(values[p : p + 1], ref.shape[2:])
                    ref[j, p] = jnp.where(iota(row.shape, 0) % 2 == 0, -row, row) if j == 2 else row
    late = flip_ref.shape[0]
    for p in range(late):
        for t in range(modes // LANES):
            flip_ref[p, t] = table_ref[pairs - late + p, t * LANES : (t + 1) * LANES].T
    hot_ref[...] = slot_of_cycle(order_ref).astype(BF16)
    theta, weight = colat_ref[...], weight_ref[...]
    with_ref[0] = jnp.broadcast_to(weight * jnp.cos(theta) / jnp.sin(theta), with_ref.shape[1:])
    with_ref[1] = jnp.broadcast_to(weight / jnp.sin(theta), with_ref.shape[1:])


def layout(small, cycle_order, colatitude, cycle_weight, table, late, after, lines, modes):
    pairs = small.shape[0]
    cycles = cycle_order.shape[0]
    vmem = pl.BlockSpec(memory_space=pltpu.VMEM)
    return pl.pallas_call(
        rows_kernel,
        in_specs=[vmem] * 6,
        out_specs=[vmem] * 5,
        out_shape=[
            pltpu.VMEM((3, pairs, lines, modes), F32), pltpu.VMEM((3, pairs, cycles), F32),
            pltpu.VMEM((cycles, cycles), BF16), pltpu.VMEM((2, lines, cycles), F32),
            pltpu.VMEM((late, modes // LANES, cycles, LANES), BF16),
        ],
        compiler_params=pltpu.CompilerParams(vmem_limit_bytes=GRANT),
        cost_estimate=pl.CostEstimate(flops=10**9, bytes_accessed=10**6, transcendentals=10**5),
        name="layout",
    )(small, cycle_order.reshape(1, -1), colatitude.reshape(1, -1), cycle_weight.reshape(1, -1), table, after)


def flip_kernel(table_ref, _, out_ref):
    for p in range(out_ref.shape[0]):
        for t in range(out_ref.shape[1]):
            out_ref[p, t] = table_ref[p, t * LANES : (t + 1) * LANES].T


def flip(table, pairs, after):
    _, modes, cycles = table.shape
    vmem = pl.BlockSpec(memory_space=pltpu.VMEM)
    return pl.pallas_call(
        flip_kernel,
        in_specs=[vmem] * 2,
        out_specs=vmem,
        out_shape=pltpu.VMEM((pairs, modes // LANES, cycles, LANES), BF16),
        compiler_params=pltpu.CompilerParams(vmem_limit_bytes=GRANT),
        cost_estimate=pl.CostEstimate(flops=10**9, bytes_accessed=10**6, transcendentals=0),
        name="flip",
    )(table, after)


def analyse_kernel(
    small_ref, r_ref, l_ref, l2_ref, tail_ref, row_ref, end_ref, hot_ref, with_ref, grad_hbm, curl_hbm,
    w_ref, grad_ref, curl_ref, sems,
):
    pairs, lines, modes = row_ref.shape[1:]
    cycles = l_ref.shape[2]
    sims = lines // 2
    high = 4 * lines

    spectra = dot(near_then_far(r_ref).astype(F32).T.astype(BF16), hot_ref[...], NT)
    with_cos, with_sin = with_ref[0], with_ref[1]
    for i in range(pairs):
        for half in range(2):
            at = (i * 2 + half) * 2 * lines
            parts = []
            for values in (spectra[at : at + lines], spectra[at + lines : at + 2 * lines]):
                parts += [values * with_cos, values * with_sin]
            parts = jnp.concatenate(parts, axis=0)
            w_ref[i, half * high : (half + 1) * high] = parts.astype(BF16)

    chunk = modes // CUTS
    k = iota((lines, chunk), 1)
    copies = []
    for p in range(pairs):
        ref, at = (l_ref, p) if p < l_ref.shape[0] else (l2_ref, p - l_ref.shape[0])
        before = [jnp.zeros((lines, LANES), F32)] * 2
        bound = modes - small_ref[p : p + 1, :1].astype(jnp.int32)
        for cut in range(CUTS):
            columns = slice(cut * chunk, (cut + 1) * chunk)
            sums = dot(w_ref[p], across(ref[at, t] for t in range(cut * chunk // LANES, (cut + 1) * chunk // LANES)))
            upper = k >= bound - cut * chunk
            a0, a1, a2, a3 = (
                jnp.where(upper, sums[high + q * lines : high + (q + 1) * lines], sums[q * lines : (q + 1) * lines])
                for q in range(4)
            )
            level, raised, azimuth = (row_ref[i, p, :, columns] for i in range(3))
            shifted = [
                pltpu.roll(across((tile, values)), 1, 1)[:, LANES:] for tile, values in zip(before, (a1, a3))
            ]
            before = [a1[:, chunk - LANES :], a3[:, chunk - LANES :]]
            grad = level * a0 - raised * shifted[0] - azimuth * swap_rows(a3)
            curl = level * a2 - raised * shifted[1] + azimuth * swap_rows(a1)
            grad_ref[p, :, :, columns] = grad.reshape(sims, 2, chunk)
            curl_ref[p, :, :, columns] = curl.reshape(sims, 2, chunk)
        last = jnp.sum(w_ref[p, high:].astype(F32) * tail_ref[p : p + 1, :], axis=1, keepdims=True)
        level, raised, azimuth = (end_ref[i, p : p + 1, :1] for i in range(3))
        b0, b1, b2, b3 = (last[q * lines : (q + 1) * lines] for q in range(4))
        a1, a3 = (values[:, LANES - 1 :] for values in before)
        last_grad = level * b0 - raised * a1 - azimuth * turn(b3)
        last_curl = level * b2 - raised * a3 + azimuth * turn(b1)
        for out, hbm, last in ((grad_ref, grad_hbm, last_grad), (curl_ref, curl_hbm, last_curl)):
            out[p, :, :, modes:] = last.reshape(sims, 2, 1)
            copies.append(pltpu.make_async_copy(out.at[p], hbm.at[p], sems.at[len(copies)]))
            copies[-1].start()
    for copy in copies:
        copy.wait()


def analyse(returned, tables, tail, small, rows, ends, hot, weights):
    _, pairs, lines, modes = rows.shape
    cycles = hot.shape[0]
    vmem = pl.BlockSpec(memory_space=pltpu.VMEM)
    hbm = pl.BlockSpec(memory_space=pltpu.HBM)
    shape = (pairs, lines // 2, 2, modes + 1)
    out = jax.ShapeDtypeStruct(shape, F32)
    return pl.pallas_call(
        analyse_kernel,
        in_specs=[vmem] * 9,
        out_specs=[hbm, hbm],
        out_shape=[out, out],
        scratch_shapes=[
            pltpu.VMEM((pairs, 8 * lines, cycles), BF16),
            pltpu.VMEM(shape, F32),
            pltpu.VMEM(shape, F32),
            pltpu.SemaphoreType.DMA((2 * pairs,)),
        ],
        compiler_params=pltpu.CompilerParams(vmem_limit_bytes=GRANT),
        name="analyse",
    )(small, returned, *tables, tail, rows, ends, hot, weights)


def merge_kernel(near_ref, far_ref, *refs):
    out_ref = refs[-1]
    parts = near_ref.shape[1]
    out_ref[:, :parts] = near_ref[...]
    out_ref[:, parts:] = far_ref[...]


def exchange(near, far, *beside):
    vmem = pl.BlockSpec(memory_space=pltpu.VMEM)
    swapped = lax.ppermute(far, CORE, [(0, 1), (1, 0)])
    chips, parts, lanes = near.shape
    both = pl.pallas_call(
        merge_kernel,
        in_specs=[vmem] * (2 + len(beside)),
        out_specs=vmem,
        out_shape=pltpu.VMEM((chips, 2 * parts, lanes), near.dtype),
        compiler_params=pltpu.CompilerParams(vmem_limit_bytes=GRANT),
        name="merge",
    )(near, swapped, *beside)
    return lax.all_to_all(both, CHIP, 0, 0, tiled=True)


def shards(tbar_alm, twf_alm, legendre, m_slots, cycle_order, colatitude, cycle_weight, pixel_mask):
    pairs, sims, _, rows = tbar_alm.shape
    by_row = jnp.transpose(legendre, (1, 0, 2))
    near, far, table, tail, small = synth(tbar_alm, twf_alm, by_row, m_slots, cycle_order, colatitude)
    early = pairs // 4 * 3
    flipped = flip(table, early, near)
    near, far = sky(exchange(near, far, flipped), pixel_mask, pairs, sims, rows - 1)
    factors, ends, hot, weights, others = layout(
        small, cycle_order, colatitude, cycle_weight, table, pairs - early, near, 2 * sims, rows - 1
    )
    returned = exchange(near, far, ends)
    return analyse(returned, (flipped, others), tail, small, factors, ends, hot, weights)


def solution(mesh):
    devices = mesh.devices.reshape(mesh.shape["grp"], -1, 2)
    finer = Mesh(devices, ("grp", CHIP, CORE))
    ma = (CHIP, CORE)
    coefficients = P(ma, "grp", None, None)
    return jax.shard_map(
        shards,
        mesh=finer,
        in_specs=(coefficients, coefficients, P(ma, None, None), P(), P(), P(), P(), P(ma, None)),
        out_specs=(coefficients, coefficients),
        check_vma=False,
    )
```

```python
import functools
import math

import jax
import jax.numpy as jnp
import numpy as np
from jax import lax
from jax.experimental import pallas as pl
from jax.experimental.pallas import tpu as pltpu
from jax.sharding import Mesh
from jax.sharding import PartitionSpec as P

F32 = jnp.float32
BF16 = jnp.bfloat16
LANES = 128
GRANT = 24 * 2**20
STRIDE = 9
CUTS = 4
CHIP, CORE = "chip", "core"
NT = (((1,), (1,)), ((), ()))
NN = (((1,), (0,)), ((), ()))


def dot(a, b, dims=NN):
    return lax.dot_general(a, b, dims, preferred_element_type=F32)


def iota(shape, dim):
    return lax.broadcasted_iota(jnp.int32, shape, dim)


def across(tiles):
    return jnp.concatenate(list(tiles), axis=1)


def small_column(m_ref, first, pairs):
    row = iota((pairs, 1), 0)
    column = jnp.zeros((pairs, 1), jnp.int32)
    for p in range(pairs):
        column = jnp.where(row == p, m_ref[first + p], column)
    return column


def layout_rows(small, modes):
    k = iota((small.shape[0], modes), 1)
    upper = k >= modes - small
    degree = jnp.where(upper, k - 1, small + k).astype(F32)
    orders = jnp.where(upper, modes - 1 - small, small).astype(F32)
    last_degree = jnp.full(small.shape, modes - 1, F32)
    last_orders = (modes - 1 - small).astype(F32)
    return (
        (degree, orders, raising(degree, orders)),
        (last_degree, last_orders, raising(last_degree, last_orders)),
    )


def raising(degree, orders):
    square = (
        (degree * degree - orders * orders)
        * (2.0 * degree + 1.0)
        / jnp.maximum(2.0 * degree - 1.0, 1.0)
    )
    return jnp.where(degree > orders, jnp.sqrt(jnp.where(degree > orders, square, 0.0)), 0.0)


def slot_of_cycle(order_ref):
    n = order_ref.shape[1]
    core = lax.axis_index(CORE)
    place = iota((n, n), 1)
    near = place < n // 2
    slot = 2 * (place % (n // 2)) + jnp.where(near, core, 1 - core)
    pick = jnp.where(iota((n, n), 0) == slot, 1.0, 0.0).astype(BF16)
    order = jnp.broadcast_to(order_ref[...].astype(F32), (8, n)).astype(BF16)
    return jnp.where(iota((n, n), 0).astype(F32) == dot(order, pick)[:1], 1.0, 0.0)


def first_pair(pairs):
    return (lax.axis_index(CHIP) * lax.axis_size(CORE) + lax.axis_index(CORE)) * pairs


def swap_rows(values):
    rows = values.shape[0]
    real = iota(values.shape, 0) % 2 == 0
    return jnp.where(real, pltpu.roll(values, rows - 1, 0), pltpu.roll(values, 1, 0))


def turn(values):
    rows = values.shape[0]
    real = iota(values.shape, 0) % 2 == 0
    return jnp.where(real, -pltpu.roll(values, rows - 1, 0), pltpu.roll(values, 1, 0))


def synth_kernel(
    m_hbm, order_hbm, colat_hbm, t_hbm, w_hbm, l_hbm, near_ref, far_ref, lr_ref, ltail_ref, small_ref,
    m_ref, order_ref, colat_ref, t_ref, w_ref, last_ref, c_ref, s_ref, deg_ref, eps_ref, up_ref, end_ref, lasts_ref, f_ref, sems, *l_refs,
):
    pairs, sims = t_ref.shape[0], t_ref.shape[1]
    modes = t_ref.shape[3] - 1
    lines = 2 * sims
    steps = len(l_refs)
    chunk = modes // steps
    first = first_pair(pairs)
    wide = near_ref.shape[1] * near_ref.shape[2] // pairs
    cycles = last_ref.shape[2]

    pieces = [(m_hbm, m_ref), (order_hbm, order_ref), (colat_hbm, colat_ref), (w_hbm, w_ref), (t_hbm, t_ref)]
    pieces.append((l_hbm.at[pl.ds(modes, 1)], last_ref))
    pieces += [(l_hbm.at[pl.ds(j * chunk, chunk)], l_refs[j]) for j in range(steps)]
    copies = [pltpu.make_async_copy(*piece, sems.at[i]) for i, piece in enumerate(pieces)]
    for copy in copies:
        copy.start()
    for copy in copies[:3]:
        copy.wait()

    small = small_column(m_ref, first, pairs)
    (degree, _, eps), (_, _, last_eps) = layout_rows(small, modes)
    small_ref[...] = jnp.broadcast_to(small.astype(F32), small_ref.shape)
    deg_ref[...] = degree * (1.0 / modes)
    eps_ref[...] = eps * (1.0 / modes)
    last_eps = last_eps * (1.0 / modes)
    theta = colat_ref[...]
    cos, inv_sin = jnp.cos(theta), 1.0 / jnp.sin(theta)
    cycle_of_slot = slot_of_cycle(order_ref).T.astype(BF16)
    up_ref[...] = jnp.where(iota((pairs, modes), 1) >= modes - small, 1.0, 0.0)
    ends = iota((lines, modes), 1) == modes - 1

    copies[3].wait()
    copies[4].wait()
    def coefficients(p, _):
        tbar = t_ref[p].reshape(lines, modes + 1)
        wiener = w_ref[p].reshape(lines, modes + 1)
        main, last = wiener[:, :modes].astype(F32), wiener[:, modes:].astype(F32)
        raised = pltpu.roll(eps_ref[pl.ds(p, 1), :] * main, modes - 1, 1)
        raised = jnp.where(ends, end_ref[pl.ds(p, 1), :][:, :1] * last, raised)
        raised = jnp.concatenate([deg_ref[pl.ds(p, 1), :] * main, raised], axis=0).astype(BF16)
        upper = jnp.broadcast_to(up_ref[pl.ds(p, 1), :], (2 * lines, modes)).astype(BF16)
        for i, sets in enumerate((jnp.concatenate([tbar[:, :modes], wiener[:, :modes]], axis=0), raised)):
            above = sets * upper
            for t in range(modes // LANES):
                tile = slice(t * LANES, (t + 1) * LANES)
                c_ref[p, t, 2 * i * lines : 2 * (i + 1) * lines] = sets[:, tile]
                c_ref[p, t, 2 * (i + 2) * lines : 2 * (i + 3) * lines] = above[:, tile]
        lasts = jnp.concatenate(
            [tbar[:, modes:].astype(F32), last, ((modes - 1.0) / modes) * last, 0.0 * last], axis=0
        )
        lasts_ref[p] = jnp.broadcast_to(lasts.astype(BF16).astype(F32), lasts_ref.shape[1:])
        return 0

    end_ref[...] = jnp.broadcast_to(last_eps, end_ref.shape)
    lax.fori_loop(0, pairs, coefficients, 0, unroll=2)

    copies[5].wait()
    tail_rows = last_ref[0].astype(F32)
    ltail_ref[...] = tail_rows
    for j in range(steps):
        copies[6 + j].wait()
        at = slice(j * chunk, (j + 1) * chunk)
        for row in range(chunk):
            f_ref[row * STRIDE : row * STRIDE + pairs, :] = l_refs[j][row].astype(F32)
        for p in range(0, pairs, 2):
            tables = [f_ref[pl.ds(p + i, chunk, stride=STRIDE), :].astype(BF16) for i in range(2)]
            both = across(
                jnp.concatenate([c_ref[p, t], c_ref[p + 1, t]], axis=0)
                for t in range(j * chunk // LANES, (j + 1) * chunk // LANES)
            )
            sums = dot(both, jnp.concatenate(tables, axis=1))
            for i in range(2):
                lr_ref[p + i, at, :] = tables[i]
                part = sums[i * 8 * lines : (i + 1) * 8 * lines, i * cycles : (i + 1) * cycles]
                s_ref[p + i] = part if j == 0 else s_ref[p + i] + part

    blocks = []
    for p in range(pairs):
        small = m_ref[first + p]
        for half, order in enumerate((small, modes - 1 - small)):
            above = s_ref[p, 4 * lines :, :]
            sums = above + lasts_ref[p] * tail_rows[p : p + 1, :] if half else s_ref[p, : 4 * lines, :] - above
            s0, s1, s2, s3 = (sums[q * lines : (q + 1) * lines] for q in range(4))
            weight = jnp.where(order == 0, 1.0, 2.0) * modes ** (-0.5)
            ratio = order.astype(F32) * (1.0 / modes)
            blocks.append(s0 * weight)
            blocks.append((cos * s2 - s3) * inv_sin * weight)
            blocks.append(turn(s1) * ratio * inv_sin * weight)
        row = iota((wide - 6 * lines, s_ref.shape[2]), 0)
        low, high = (small % LANES).astype(F32), (small // LANES).astype(F32)
        blocks.append(jnp.where(row == 0, low, jnp.where(row == 1, high, 0.0)))
    fourier = jnp.concatenate(blocks, axis=0).astype(BF16)
    out = dot(cycle_of_slot, fourier, NT).astype(BF16)
    near_ref[...] = out[: cycles // 2].reshape(near_ref.shape)
    far_ref[...] = out[cycles // 2 :].reshape(far_ref.shape)


def synth(tbar_alm, twf_alm, table, m_slots, cycle_order, colatitude):
    pairs, sims, _, rows = tbar_alm.shape
    modes = rows - 1
    cycles = table.shape[2]
    lines = 2 * sims
    wide = 8 * lines
    steps = 4
    vmem = pl.BlockSpec(memory_space=pltpu.VMEM)
    hbm = pl.BlockSpec(memory_space=pltpu.HBM)
    return pl.pallas_call(
        synth_kernel,
        in_specs=[hbm] * 6,
        out_specs=[vmem] * 5,
        out_shape=[
            pltpu.VMEM((cycles // 2, pairs * wide // LANES, LANES), BF16),
            pltpu.VMEM((cycles // 2, pairs * wide // LANES, LANES), BF16),
            pltpu.VMEM((pairs, modes, cycles), BF16),
            pltpu.VMEM((pairs, cycles), F32),
            pltpu.VMEM((pairs, LANES), F32),
        ],
        scratch_shapes=[
            pltpu.SMEM(m_slots.shape, jnp.int32),
            pltpu.VMEM((1, cycles), jnp.int32),
            pltpu.VMEM((1, cycles), F32),
            pltpu.VMEM(tbar_alm.shape, BF16),
            pltpu.VMEM(twf_alm.shape, BF16),
            pltpu.VMEM((1, pairs, cycles), BF16),
            pltpu.VMEM((pairs, modes // LANES, 8 * lines, LANES), BF16),
            pltpu.VMEM((pairs, 8 * lines, cycles), F32),
            pltpu.VMEM((pairs, modes), F32),
            pltpu.VMEM((pairs, modes), F32),
            pltpu.VMEM((pairs, modes), F32),
            pltpu.VMEM((pairs, LANES), F32),
            pltpu.VMEM((pairs, 4 * lines, cycles), F32),
            pltpu.VMEM((modes // steps * STRIDE, cycles), F32),
            pltpu.SemaphoreType.DMA((steps + 6,)),
        ]
        + [pltpu.VMEM((modes // steps, pairs, cycles), BF16)] * steps,
        compiler_params=pltpu.CompilerParams(vmem_limit_bytes=GRANT),
        name="synth",
    )(*(pltpu.with_memory_space_constraint(x, pltpu.HBM) for x in (
        m_slots, cycle_order.reshape(1, -1), colatitude.reshape(1, -1), tbar_alm, twf_alm, table
    )))


def angles(left, right, period):
    return 2.0 * np.pi * (np.outer(left, right) % period) / period


def split(table):
    high = table.astype(np.float32).astype(jnp.bfloat16)
    return high, (table - high.astype(np.float64)).astype(np.float32).astype(jnp.bfloat16)


def sky_tables(modes, pixels):
    small = pixels // LANES
    m1, j2, m2 = np.arange(LANES), np.arange(small), np.arange(modes // LANES)
    j1 = np.arange(LANES).reshape(-1, LANES // small).T.reshape(-1)
    th = angles(j2, m2, small).reshape(small, 2, -1)
    c, s = np.cos(th), np.sin(th)
    first = np.stack([np.stack([c, -s], 2), np.stack([s, c], 2)], 0).reshape(2 * small, -1)
    th = angles(j2, m1, pixels)
    twist = np.stack([np.cos(th), np.sin(th)])
    th = angles(m1, j1, LANES)
    second = np.concatenate([np.cos(th), -np.sin(th)], 0)
    third = np.concatenate([np.cos(th.T), -np.sin(th.T)], 1)
    th = angles(m2, j2, small).reshape(2, -1, small)
    c, s = np.cos(th), np.sin(th)
    fourth = np.stack([np.concatenate([c, s], 2), np.concatenate([-s, c], 2)], 1)
    fourth = fourth.reshape(2 * modes // LANES, -1)
    return (
        np.concatenate(split(first), 1), twist.astype(np.float32), split(second)[0],
        np.concatenate(split(third), 0), np.concatenate(split(fourth), 1),
    )


def near_then_far(ref):
    chips, parts, lanes = ref.shape
    halves = (ref[:, : parts // 2], ref[:, parts // 2 :])
    return jnp.concatenate([h.reshape(chips, parts // 2 * lanes) for h in halves], axis=0)


def sky_kernel(
    pairs, sims, x_ref, mask_ref, first_ref, twist_ref, second_ref, third_ref, fourth_ref, near_ref, far_ref,
    xt_ref, lhs_ref, hot_ref,
):
    devices = 2 * x_ref.shape[0]
    wide = x_ref.shape[1] * x_ref.shape[2] // 2 // pairs
    lines = 2 * sims
    small = twist_ref.shape[1]
    pixels = small * LANES
    tall = fourth_ref.shape[0] // 4
    xt_ref[...] = near_then_far(x_ref).astype(F32).T

    n = 2 * tall
    groups = 3 * sims
    sorted_halves, places = [], []
    for half in range(2):
        place = []
        for p in range(pairs):
            at = p * wide + 6 * lines
            low, high = (xt_ref[at + i : at + i + 1, :].astype(jnp.int32) for i in range(2))
            if half:
                low, high = LANES - 1 - low, tall - 1 - high
            place.append(iota((tall, devices), 0) == high)
            hot_ref[half, p] = jnp.where(iota((LANES, devices), 0) == low, 1.0, 0.0).astype(BF16)
            parts = []
            for row in range(3 * lines):
                at = p * wide + half * 3 * lines + row
                parts.append(jnp.where(place[p], xt_ref[at : at + 1, :], 0.0))
            lhs_ref[p] = jnp.concatenate(parts, axis=0).astype(BF16)
        places.append(place)
        left, right = (across(ref[p] for p in range(pairs)) for ref in (lhs_ref, hot_ref.at[half]))
        sorted_halves.append(dot(left, right, NT).astype(BF16))

    spread = jnp.concatenate(
        [
            jnp.concatenate([s[g * n : (g + 1) * n] for s in sorted_halves], axis=0)
            for g in range(groups)
        ],
        axis=1,
    )
    stage = dot(first_ref[...], jnp.concatenate([spread, spread], axis=0))
    cos, sin = twist_ref[0], twist_ref[1]
    twisted = []
    for g in range(groups):
        re, im = (stage[i * small : (i + 1) * small, g * LANES : (g + 1) * LANES] for i in range(2))
        twisted.append(jnp.concatenate([re * cos - im * sin, re * sin + im * cos], axis=1))
    twisted = jnp.concatenate(twisted, axis=0).astype(BF16)
    maps = dot(twisted, second_ref[...])

    mask = mask_ref[...].astype(F32).T
    mask = jnp.concatenate([mask[i * small : (i + 1) * small] for i in range(LANES // small)], axis=1)
    products = []
    for q in range(1, 3):
        for s in range(sims):
            at = (q * sims + s) * small
            products.append(mask * maps[s * small : (s + 1) * small] * maps[at : at + small])
    products = jnp.concatenate(products, axis=0).astype(BF16)
    stage = dot(across((products, products)), third_ref[...])
    groups = 2 * sims
    twisted = []
    for g in range(groups):
        re, im = (stage[g * small : (g + 1) * small, i * LANES : (i + 1) * LANES] for i in range(2))
        twisted.append(jnp.concatenate([re * cos + im * sin, im * cos - re * sin], axis=0))
    twisted = jnp.concatenate(twisted, axis=1).astype(BF16)
    spectra = dot(fourth_ref[...], jnp.concatenate([twisted, twisted], axis=0)) * pixels ** (-0.5)
    spectra = spectra.astype(BF16)

    rows, columns = 2 * groups, 2 * groups * tall
    add = jnp.where(iota((rows, columns), 1) // tall == iota((rows, columns), 0), 1.0, 0.0).astype(BF16)
    found = []
    for half in range(2):
        stacked = jnp.concatenate(
            [spectra[half * n : (half + 1) * n, g * LANES : (g + 1) * LANES] for g in range(groups)], axis=0
        )
        values = dot(stacked, across(hot_ref[half, p] for p in range(pairs)))
        for p in range(pairs):
            tile = slice(p * devices, (p + 1) * devices)
            keep = jnp.concatenate([places[half][p]] * rows, axis=0)
            lhs_ref[p, :columns] = jnp.where(keep, values[:, tile], 0.0).astype(BF16)
        found.append(dot(add, across(lhs_ref[p, :columns] for p in range(pairs))))
    blocks = [found[half][:, p * devices : (p + 1) * devices] for p in range(pairs) for half in range(2)]
    out = jnp.concatenate(blocks, axis=0).T.astype(BF16)
    near_ref[...] = out[: devices // 2].reshape(near_ref.shape)
    far_ref[...] = out[devices // 2 :].reshape(far_ref.shape)


def sky(received, pixel_mask, pairs, sims, modes):
    devices = 2 * received.shape[0]
    pixels = pixel_mask.shape[1]
    tables = sky_tables(modes, pixels)
    vmem = pl.BlockSpec(memory_space=pltpu.VMEM)
    tall = modes // LANES // 2
    return pl.pallas_call(
        functools.partial(sky_kernel, pairs, sims),
        in_specs=[vmem] * 7,
        out_specs=[vmem] * 2,
        out_shape=[pltpu.VMEM((devices // 2, pairs * 8 * sims // LANES, LANES), BF16)] * 2,
        scratch_shapes=[
            pltpu.VMEM((received.shape[1] // 2 * LANES, devices), F32),
            pltpu.VMEM((pairs, 6 * sims * tall, devices), BF16),
            pltpu.VMEM((2, pairs, LANES, devices), BF16),
        ],
        compiler_params=pltpu.CompilerParams(vmem_limit_bytes=GRANT),
        name="sky",
    )(received, pixel_mask.reshape(-1, LANES), *(jnp.asarray(t) for t in tables))


def rows_kernel(
    small_ref, order_ref, colat_ref, weight_ref, table_ref, _, row_ref, end_ref, hot_ref, with_ref, flip_ref
):
    pairs, modes, cycles = row_ref.shape[1], row_ref.shape[3], end_ref.shape[2]
    small = small_ref[:, :1].astype(jnp.int32)
    main, last = layout_rows(small, modes)
    for i, ref in enumerate((row_ref, end_ref)):
        degree, orders, eps = (main, last)[i]
        scale = (modes / cycles) ** 0.5 / jnp.sqrt(jnp.maximum(degree * (degree + 1.0), 1.0))
        for j, values in enumerate((degree * scale, eps * scale, orders * scale)):
            if i:
                ref[j] = jnp.broadcast_to(values, ref.shape[1:])
            else:
                for p in range(pairs):
                    row = jnp.broadcast_to(values[p : p + 1], ref.shape[2:])
                    ref[j, p] = jnp.where(iota(row.shape, 0) % 2 == 0, -row, row) if j == 2 else row
    late = flip_ref.shape[0]
    for p in range(late):
        for t in range(modes // LANES):
            flip_ref[p, t] = table_ref[pairs - late + p, t * LANES : (t + 1) * LANES].T
    hot_ref[...] = slot_of_cycle(order_ref).astype(BF16)
    theta, weight = colat_ref[...], weight_ref[...]
    with_ref[0] = jnp.broadcast_to(weight * jnp.cos(theta) / jnp.sin(theta), with_ref.shape[1:])
    with_ref[1] = jnp.broadcast_to(weight / jnp.sin(theta), with_ref.shape[1:])


def layout(small, cycle_order, colatitude, cycle_weight, table, late, after, lines, modes):
    pairs = small.shape[0]
    cycles = cycle_order.shape[0]
    vmem = pl.BlockSpec(memory_space=pltpu.VMEM)
    return pl.pallas_call(
        rows_kernel,
        in_specs=[vmem] * 6,
        out_specs=[vmem] * 5,
        out_shape=[
            pltpu.VMEM((3, pairs, lines, modes), F32), pltpu.VMEM((3, pairs, cycles), F32),
            pltpu.VMEM((cycles, cycles), BF16), pltpu.VMEM((2, lines, cycles), F32),
            pltpu.VMEM((late, modes // LANES, cycles, LANES), BF16),
        ],
        compiler_params=pltpu.CompilerParams(vmem_limit_bytes=GRANT),
        cost_estimate=pl.CostEstimate(flops=10**9, bytes_accessed=10**6, transcendentals=10**5),
        name="layout",
    )(small, cycle_order.reshape(1, -1), colatitude.reshape(1, -1), cycle_weight.reshape(1, -1), table, after)


def flip_kernel(table_ref, _, out_ref):
    for p in range(out_ref.shape[0]):
        for t in range(out_ref.shape[1]):
            out_ref[p, t] = table_ref[p, t * LANES : (t + 1) * LANES].T


def flip(table, pairs, after):
    _, modes, cycles = table.shape
    vmem = pl.BlockSpec(memory_space=pltpu.VMEM)
    return pl.pallas_call(
        flip_kernel,
        in_specs=[vmem] * 2,
        out_specs=vmem,
        out_shape=pltpu.VMEM((pairs, modes // LANES, cycles, LANES), BF16),
        compiler_params=pltpu.CompilerParams(vmem_limit_bytes=GRANT),
        cost_estimate=pl.CostEstimate(flops=10**9, bytes_accessed=10**6, transcendentals=0),
        name="flip",
    )(table, after)


def analyse_kernel(
    small_ref, r_ref, l_ref, l2_ref, tail_ref, row_ref, end_ref, hot_ref, with_ref, grad_hbm, curl_hbm,
    w_ref, grad_ref, curl_ref, sems,
):
    pairs, lines, modes = row_ref.shape[1:]
    cycles = l_ref.shape[2]
    sims = lines // 2
    high = 4 * lines

    spectra = dot(near_then_far(r_ref).astype(F32).T.astype(BF16), hot_ref[...], NT)
    with_cos, with_sin = with_ref[0], with_ref[1]
    for i in range(pairs):
        for half in range(2):
            at = (i * 2 + half) * 2 * lines
            parts = []
            for values in (spectra[at : at + lines], spectra[at + lines : at + 2 * lines]):
                parts += [values * with_cos, values * with_sin]
            parts = jnp.concatenate(parts, axis=0)
            w_ref[i, half * high : (half + 1) * high] = parts.astype(BF16)

    chunk = modes // CUTS
    k = iota((lines, chunk), 1)
    copies = []
    for p in range(pairs):
        ref, at = (l_ref, p) if p < l_ref.shape[0] else (l2_ref, p - l_ref.shape[0])
        before = [jnp.zeros((lines, LANES), F32)] * 2
        bound = modes - small_ref[p : p + 1, :1].astype(jnp.int32)
        for cut in range(CUTS):
            columns = slice(cut * chunk, (cut + 1) * chunk)
            sums = dot(w_ref[p], across(ref[at, t] for t in range(cut * chunk // LANES, (cut + 1) * chunk // LANES)))
            upper = k >= bound - cut * chunk
            a0, a1, a2, a3 = (
                jnp.where(upper, sums[high + q * lines : high + (q + 1) * lines], sums[q * lines : (q + 1) * lines])
                for q in range(4)
            )
            level, raised, azimuth = (row_ref[i, p, :, columns] for i in range(3))
            shifted = [
                pltpu.roll(across((tile, values)), 1, 1)[:, LANES:] for tile, values in zip(before, (a1, a3))
            ]
            before = [a1[:, chunk - LANES :], a3[:, chunk - LANES :]]
            grad = level * a0 - raised * shifted[0] - azimuth * swap_rows(a3)
            curl = level * a2 - raised * shifted[1] + azimuth * swap_rows(a1)
            grad_ref[p, :, :, columns] = grad.reshape(sims, 2, chunk)
            curl_ref[p, :, :, columns] = curl.reshape(sims, 2, chunk)
        last = jnp.sum(w_ref[p, high:].astype(F32) * tail_ref[p : p + 1, :], axis=1, keepdims=True)
        level, raised, azimuth = (end_ref[i, p : p + 1, :1] for i in range(3))
        b0, b1, b2, b3 = (last[q * lines : (q + 1) * lines] for q in range(4))
        a1, a3 = (values[:, LANES - 1 :] for values in before)
        last_grad = level * b0 - raised * a1 - azimuth * turn(b3)
        last_curl = level * b2 - raised * a3 + azimuth * turn(b1)
        for out, hbm, last in ((grad_ref, grad_hbm, last_grad), (curl_ref, curl_hbm, last_curl)):
            out[p, :, :, modes:] = last.reshape(sims, 2, 1)
            copies.append(pltpu.make_async_copy(out.at[p], hbm.at[p], sems.at[len(copies)]))
            copies[-1].start()
    for copy in copies:
        copy.wait()


def analyse(returned, tables, tail, small, rows, ends, hot, weights):
    _, pairs, lines, modes = rows.shape
    cycles = hot.shape[0]
    vmem = pl.BlockSpec(memory_space=pltpu.VMEM)
    hbm = pl.BlockSpec(memory_space=pltpu.HBM)
    shape = (pairs, lines // 2, 2, modes + 1)
    out = jax.ShapeDtypeStruct(shape, F32)
    return pl.pallas_call(
        analyse_kernel,
        in_specs=[vmem] * 9,
        out_specs=[hbm, hbm],
        out_shape=[out, out],
        scratch_shapes=[
            pltpu.VMEM((pairs, 8 * lines, cycles), BF16),
            pltpu.VMEM(shape, F32),
            pltpu.VMEM(shape, F32),
            pltpu.SemaphoreType.DMA((2 * pairs,)),
        ],
        compiler_params=pltpu.CompilerParams(vmem_limit_bytes=GRANT),
        name="analyse",
    )(small, returned, *tables, tail, rows, ends, hot, weights)


def merge_kernel(near_ref, far_ref, *refs):
    out_ref = refs[-1]
    parts = near_ref.shape[1]
    out_ref[:, :parts] = near_ref[...]
    out_ref[:, parts:] = far_ref[...]


def exchange(near, far, *beside):
    vmem = pl.BlockSpec(memory_space=pltpu.VMEM)
    swapped = lax.ppermute(far, CORE, [(0, 1), (1, 0)])
    chips, parts, lanes = near.shape
    both = pl.pallas_call(
        merge_kernel,
        in_specs=[vmem] * (2 + len(beside)),
        out_specs=vmem,
        out_shape=pltpu.VMEM((chips, 2 * parts, lanes), near.dtype),
        compiler_params=pltpu.CompilerParams(vmem_limit_bytes=GRANT),
        name="merge",
    )(near, swapped, *beside)
    return lax.all_to_all(both, CHIP, 0, 0, tiled=True)


def shards(tbar_alm, twf_alm, legendre, m_slots, cycle_order, colatitude, cycle_weight, pixel_mask):
    pairs, sims, _, rows = tbar_alm.shape
    by_row = jnp.transpose(legendre, (1, 0, 2))
    near, far, table, tail, small = synth(tbar_alm, twf_alm, by_row, m_slots, cycle_order, colatitude)
    early = pairs // 4 * 3
    flipped = flip(table, early, near)
    near, far = sky(exchange(near, far, flipped), pixel_mask, pairs, sims, rows - 1)
    factors, ends, hot, weights, others = layout(
        small, cycle_order, colatitude, cycle_weight, table, pairs - early, near, 2 * sims, rows - 1
    )
    returned = exchange(near, far, ends)
    return analyse(returned, (flipped, others), tail, small, factors, ends, hot, weights)


def solution(mesh):
    devices = mesh.devices.reshape(mesh.shape["grp"], -1, 2)
    finer = Mesh(devices, ("grp", CHIP, CORE))
    ma = (CHIP, CORE)
    coefficients = P(ma, "grp", None, None)
    return jax.shard_map(
        shards,
        mesh=finer,
        in_specs=(coefficients, coefficients, P(ma, None, None), P(), P(), P(), P(), P(ma, None)),
        out_specs=(coefficients, coefficients),
        check_vma=False,
    )
```
